32 devices in a mesh: groups: 2 (over x), traces: 16 (over z, y, core).
Axes of the slice: x: 2, y: 2, z: 4, core: 2. Of those that a mesh axis runs over, the one named last changes fastest.
Arguments:
- raw_traces: float32 [8192, 8192], P(('groups', 'traces')), parts along dimension 0, may hold values from -6 to 6
- filter_index: int32 [8192], P(('groups', 'traces')), parts along dimension 0, may hold values from 0 to 255
- channel_order: int32 [512], P('groups'), parts along dimension 0, may hold values from 0 to 255, each once
- wavelets: float32 [256, 256], P('traces'), may hold values from -0.375 to 0.375
- damping: float32 [256], P('traces'), may hold values from 0.02 to 0.5
Outputs:
- deconvolved: float32 [8192, 8192], P(('groups', 'traces')), parts along dimension 0
The draws below stay inside these ranges and needn't reach their ends.
There are 2 independent parts, one for each index of `groups`. The reference program is written for one: setup_inputs(seed, part) draws one part's arguments, and reference() takes and returns one part's arrays. A program takes and returns all parts, laid end to end along the dimension named above; an argument that names none is the same for every part. Nothing has to cross between parts.
Inputs may be any that keep to these rules, and one draw needn't show every extreme that they name: `channel_order`: each of 0 to 255 appears once.
All inputs are finite; a program needn't handle non-finite values.
Results may differ from the reference program's by a relative error of at most 0.00021.
Values sent between devices are 32-bit elements; how exact they have to be, the bound alone decides.
A program may use at most 192 MiB of HBM per device.

```python
import math
import jax
import jax.numpy as jnp
from jax import lax

L = 8192
FILTERS = 256
FLEN = 256
TR_DEV = 256
TRACES = 4096
N_TRACES = 16


def plant(drawn, own_key, smallest, largest):
    longest = drawn.shape.index(max(drawn.shape))
    spots = []
    for shift in (0, 1):
        where = [jax.random.randint(jax.random.fold_in(own_key, axis), (), 0, length) for axis, length in enumerate(drawn.shape)]
        where[longest] = (where[longest] + shift) % drawn.shape[longest]
        spots.append(tuple(where))
    return drawn.at[spots[0]].set(smallest).at[spots[1]].set(largest)


def block_scale(key, shape, pieces, least, largest):
    factor_of, own = 1.0, jax.random.fold_in(key, 6)
    for dim, blocks in pieces:
        steps = jnp.exp(jax.random.uniform(jax.random.fold_in(own, dim), (blocks,), jnp.float32, least / len(pieces), largest / len(pieces)))
        factor_of = factor_of * jnp.repeat(steps, shape[dim] // blocks).reshape([-1 if axis == dim else 1 for axis in range(len(shape))])
    return factor_of


def centred(key, dims, deviation, bound, pieces=(), kind=jnp.bfloat16):
    loudness = block_scale(key, dims, pieces, -0.22, 0.18) if pieces else 1.0
    array = jax.random.normal(key, dims, jnp.float32) * deviation * loudness
    return jnp.minimum(jnp.maximum(array, -bound), bound).astype(kind)


def setup_inputs(seed: int = 0, part: int = 0) -> dict:
    streams_of = jax.random.split(jax.random.key(seed), 6)
    part_keys = jax.random.split(jax.random.fold_in(streams_of[5], part), 6)
    return {
        "raw_traces": centred(part_keys[0], (TRACES, L), 1.0, 6.0, ((0, 16),), jnp.float32),
        "filter_index": plant(jax.random.randint(part_keys[1], (TRACES,), 0, FILTERS), jax.random.fold_in(part_keys[1], 1), 0, FILTERS - 1).astype(jnp.int32),
        "channel_order": jax.random.permutation(part_keys[2], TR_DEV).astype(jnp.int32),
        "wavelets": centred(streams_of[3], (FILTERS, FLEN), FLEN ** -0.5, 0.375, ((0, 16),), jnp.float32),
        "damping": jnp.clip(jnp.exp(math.log(0.5) - 3.218876 * jax.random.uniform(streams_of[4], (FILTERS,), jnp.float32) ** block_scale(streams_of[4], (FILTERS,), ((0, 16),), -0.2, 0.2)), 0.02, 0.5),
    }


def filter_gains(wavelets, damping):
    padded = jnp.pad(wavelets, ((0, 0), (0, L - FLEN)))
    spectrum = jnp.fft.fft(padded, axis=1)
    spec_re = jnp.real(spectrum)
    spec_im = jnp.imag(spectrum)
    power = spec_re * spec_re + spec_im * spec_im
    level = jnp.mean(power, axis=1, keepdims=True)
    denom = power + damping[:, None] * (level + 1e-6)
    return spec_re / denom, -spec_im / denom


def reference(raw_traces, filter_index, channel_order, wavelets, damping):
    gain_re, gain_im = filter_gains(wavelets, damping)
    blocks = raw_traces.reshape(N_TRACES, TR_DEV, L)
    picks = filter_index.reshape(N_TRACES, TR_DEV)

    def one_block(pair):
        rows, index = pair
        spectrum = jnp.fft.fft(rows, axis=1)
        spec_re = jnp.real(spectrum)
        spec_im = jnp.imag(spectrum)
        pick_re = jnp.take(gain_re, index, axis=0)
        pick_im = jnp.take(gain_im, index, axis=0)
        out_re = spec_re * pick_re - spec_im * pick_im
        out_im = spec_re * pick_im + spec_im * pick_re
        return jnp.real(jnp.fft.ifft(lax.complex(out_re, out_im), axis=1))

    results = lax.map(one_block, (blocks, picks)).reshape(TRACES, L)
    out_rows = jnp.arange(TRACES, dtype=jnp.int32)
    position = (out_rows // TR_DEV) * TR_DEV + jnp.take(channel_order, out_rows % TR_DEV).astype(jnp.int32)
    source = ((position % N_TRACES) * TR_DEV + position // N_TRACES).astype(jnp.int32)
    return jnp.take(results, source, axis=0)
```

```python
import functools
import math

import jax
import jax.numpy as jnp
import numpy as np
from jax import lax
from jax.experimental import pallas as pl
from jax.experimental.pallas import tpu as pltpu
from jax.sharding import PartitionSpec as P

LANES = 128
RADIX = 8
ROWS = 16
SUBLANES = 8

KEPT = (
    [RADIX * b for b in range(RADIX // 2 + 1)]
    + [a + RADIX * b for a in range(1, RADIX // 2) for b in range(RADIX)]
    + [RADIX // 2 + RADIX * b for b in range(RADIX // 2)]
)
SLOT = {k: s for s, k in enumerate(KEPT)}
KEEP = len(KEPT)


def lane_matrix(sign, scale):
    ids = np.arange(LANES)
    angle = 2.0 * np.pi * (np.outer(ids, ids) % LANES) / LANES
    c, s = np.cos(angle) * scale, sign * np.sin(angle) * scale
    full = np.block([[c, s], [-s, c]])
    import ml_dtypes

    high = full.astype(np.float32).astype(ml_dtypes.bfloat16)
    low = (full.astype(np.float32) - high.astype(np.float32)).astype(ml_dtypes.bfloat16)
    return np.concatenate([high, high, low], axis=0)


def twiddles(length, taps):
    m = np.arange(LANES)
    rows = []
    for k in KEPT:
        angle = 2.0 * np.pi * k * m / length
        row = [np.cos(angle), -np.sin(angle)]
        weight = 1.0 if k in (0, RADIX * RADIX // 2) else 2.0
        row += [weight * np.cos(angle), weight * np.sin(angle)]
        for piece in range(taps // LANES):
            shifted = 2.0 * np.pi * k * (m + LANES * piece) / length
            row += [np.cos(shifted), -np.sin(shifted)]
        rows.append(np.stack(row))
    return np.stack(rows).astype(np.float32)


def cadd(a, b):
    return (a[0] + b[0], a[1] + b[1])


def csub(a, b):
    return (a[0] - b[0], a[1] - b[1])


def turn(a, num, den):
    num %= den
    if num == 0:
        return a
    if 4 * num == den:
        return (-a[1], a[0])
    if 2 * num == den:
        return (-a[0], -a[1])
    if 4 * num == 3 * den:
        return (a[1], -a[0])
    c, s = math.cos(2 * math.pi * num / den), math.sin(2 * math.pi * num / den)
    return (a[0] * c - a[1] * s, a[0] * s + a[1] * c)


def fourier(items, sign):
    n = len(items)
    if n == 1:
        return items
    even, odd = fourier(items[0::2], sign), fourier(items[1::2], sign)
    turned = [turn(o, sign * k, n) for k, o in enumerate(odd)]
    return [cadd(e, t) for e, t in zip(even, turned)] + [csub(e, t) for e, t in zip(even, turned)]


def real_eight(v):
    h = math.sqrt(0.5)
    s0, d0, s1, d1 = v[0] + v[4], v[0] - v[4], v[1] + v[5], v[1] - v[5]
    s2, d2, s3, d3 = v[2] + v[6], v[2] - v[6], v[3] + v[7], v[3] - v[7]
    p, q = s0 + s2, s1 + s3
    r, t = (d1 - d3) * h, (d1 + d3) * h
    return [p + q, (d0 + r, -(d2 + t)), (s0 - s2, s3 - s1), (d0 - r, d2 - t), p - q]


def eight_real(u0, u1, u2, u3, u4):
    h = math.sqrt(0.5)
    p, q = u0 + u4, u0 - u4
    e = [p + u2[0], q - u2[1], p - u2[0], q + u2[1]]
    f, g = u1[0] - u3[0], u1[1] + u3[1]
    o = [u1[0] + u3[0], (f - g) * h, u3[1] - u1[1], -(f + g) * h]
    return [a + b for a, b in zip(e, o)] + [a - b for a, b in zip(e, o)]


def put_split(ref, base, re, im):
    rows = pl.ds(base, ROWS)
    for part, value in enumerate((re, im)):
        high = value.astype(jnp.bfloat16)
        low = (value - high.astype(jnp.float32)).astype(jnp.bfloat16)
        at = part * LANES
        ref[rows, at : at + LANES] = high
        ref[rows, 2 * LANES + at : 2 * LANES + at + LANES] = low
        ref[rows, 4 * LANES + at : 4 * LANES + at + LANES] = high


def deconvolve(read, write, wave, floor, fwd_ref, inv_ref, tw_ref, mid_ref, cut_ref, spec_ref):
    half, wide = RADIX // 2, RADIX * RADIX
    for j2 in range(RADIX):
        out = real_eight([read(RADIX * j1 + j2) for j1 in range(RADIX)])
        mid_ref[2 * j2] = out[0]
        mid_ref[2 * j2 + 1] = out[half]
        for a in range(1, half):
            mid_ref[2 * RADIX * a + 2 * j2] = out[a][0]
            mid_ref[2 * RADIX * a + 2 * j2 + 1] = out[a][1]

    def emit(k, value):
        s = SLOT[k]
        c, n = tw_ref[s, 0:1, :], tw_ref[s, 1:2, :]
        put_split(cut_ref, s * ROWS, value[0] * c - value[1] * n, value[0] * n + value[1] * c)

    zero = real_eight([mid_ref[2 * j2] for j2 in range(RADIX)])
    c, n = tw_ref[0, 0:1, :], tw_ref[0, 1:2, :]
    for b in range(half + 1):
        s = SLOT[RADIX * b]
        c, n = tw_ref[s, 0:1, :], tw_ref[s, 1:2, :]
        if b in (0, half):
            put_split(cut_ref, s * ROWS, zero[b] * c, zero[b] * n)
        else:
            emit(RADIX * b, zero[b])
    for a in range(1, half):
        base = 2 * RADIX * a
        items = [turn((mid_ref[base + 2 * j2], mid_ref[base + 2 * j2 + 1]), -a * j2, wide) for j2 in range(RADIX)]
        for b, value in enumerate(fourier(items, -1)):
            emit(a + RADIX * b, value)
    four = [mid_ref[2 * j2 + 1] for j2 in range(RADIX)]
    for b in range(half):
        k = half + RADIX * b
        re, im = four[0], None
        for j2 in range(1, RADIX):
            angle = 2 * math.pi * (k * j2 % wide) / wide
            re = re + four[j2] * math.cos(angle)
            term = four[j2] * -math.sin(angle)
            im = term if im is None else im + term
        emit(k, (re, im))

    for s in range(KEEP):
        re = im = None
        for piece, taps in enumerate(wave):
            c, n = tw_ref[s, 4 + 2 * piece : 5 + 2 * piece, :], tw_ref[s, 5 + 2 * piece : 6 + 2 * piece, :]
            re = taps * c if re is None else re + taps * c
            im = taps * n if im is None else im + taps * n
        put_split(cut_ref, (KEEP + s) * ROWS, re, im)

    spec_ref[...] = jnp.dot(cut_ref[...], fwd_ref[...], preferred_element_type=jnp.float32)

    def apply(s, carry):
        at = pl.multiple_of(s * ROWS, ROWS)
        other = pl.multiple_of((KEEP + s) * ROWS, ROWS)
        xr, xi = spec_ref[pl.ds(at, ROWS), 0:LANES], spec_ref[pl.ds(at, ROWS), LANES:]
        hr, hi = spec_ref[pl.ds(other, ROWS), 0:LANES], spec_ref[pl.ds(other, ROWS), LANES:]
        scale = 1.0 / (hr * hr + hi * hi + floor)
        put_split(cut_ref, at, (xr * hr + xi * hi) * scale, (xi * hr - xr * hi) * scale)
        return carry

    lax.fori_loop(0, KEEP, apply, 0, unroll=3)
    rows = KEEP * ROWS
    spec_ref[0:rows] = jnp.dot(cut_ref[0:rows], inv_ref[...], preferred_element_type=jnp.float32)

    def fetch(k):
        s = SLOT[k]
        re, im = spec_ref[s * ROWS : (s + 1) * ROWS, 0:LANES], spec_ref[s * ROWS : (s + 1) * ROWS, LANES:]
        c, n = tw_ref[s, 2:3, :], tw_ref[s, 3:4, :]
        if k in (0, wide // 2):
            return re * c - im * n
        return (re * c - im * n, re * n + im * c)

    for a in range(1, half):
        base = 2 * RADIX * a
        for j2, value in enumerate(fourier([fetch(a + RADIX * b) for b in range(RADIX)], 1)):
            value = turn(value, a * j2, wide)
            mid_ref[base + 2 * j2] = value[0]
            mid_ref[base + 2 * j2 + 1] = value[1]
    for j2, value in enumerate(eight_real(*[fetch(RADIX * b) for b in range(half + 1)])):
        mid_ref[2 * j2] = value
    four = [fetch(half + RADIX * b) for b in range(half)]
    for j2 in range(RADIX):
        total = None
        for b, value in enumerate(four):
            angle = 2 * math.pi * ((half + RADIX * b) * j2 % wide) / wide
            term = value[0] * math.cos(angle)
            if j2:
                term = term - value[1] * math.sin(angle)
            total = term if total is None else total + term
        mid_ref[2 * j2 + 1] = total
    for j2 in range(RADIX):
        parts = [mid_ref[2 * j2]]
        for a in range(1, half):
            base = 2 * RADIX * a
            parts.append((mid_ref[base + 2 * j2], mid_ref[base + 2 * j2 + 1]))
        parts.append(mid_ref[2 * j2 + 1])
        for j1, value in enumerate(eight_real(*parts)):
            write(RADIX * j1 + j2, value)


def slabs(ref, lead):
    def at(j):
        return lead + (slice(None), slice(j * LANES, (j + 1) * LANES))

    def read(j):
        value = ref[at(j)]
        return value.reshape(ROWS, LANES)

    def write(j, value):
        ref[at(j)] = value.reshape(ref[at(j)].shape)

    return read, write


def block_kernel(taps, lead, x_ref, w_ref, fwd_ref, inv_ref, tw_ref, o_ref, mid_ref, cut_ref, spec_ref):
    read, _ = slabs(x_ref, lead)
    _, write = slabs(o_ref, (slice(None),) * (len(o_ref.shape) - 2))
    wave = [w_ref[:, p * LANES : (p + 1) * LANES] for p in range(taps // LANES)]
    deconvolve(read, write, wave, w_ref[:, taps : taps + LANES], fwd_ref, inv_ref, tw_ref, mid_ref, cut_ref, spec_ref)


def split_count(n):
    inner = 1
    while inner * inner < n:
        inner *= 2
    return (n // inner, inner) if n % inner == 0 else (1, n)


def exchange_kernel(
    n,
    taps,
    x_ref,
    pick_ref,
    wave_ref,
    damp_ref,
    fwd_hbm,
    inv_hbm,
    tw_hbm,
    buf_ref,
    mid_ref,
    cut_ref,
    spec_ref,
    fwd_ref,
    inv_ref,
    tw_ref,
    bank_ref,
    rows_ref,
    pick_smem,
    damp_smem,
    load_sems,
    near_sems,
    raw_sems,
    pick_sems,
    bank_sends,
    bank_recvs,
    sends,
    recvs,
):
    me = lax.axis_index("traces")
    own, each = wave_ref.shape[0], x_ref.shape[0] // n
    half = n // 2
    partner = lax.rem(me + half, n)
    outer, inner = split_count(n)
    far, near = lax.div(me, inner), lax.rem(me, inner)
    halves, pieces = own // SUBLANES, taps // LANES
    last = halves * pieces

    def remote(src, dst, send_sem, recv_sem, device):
        return pltpu.make_async_remote_copy(
            src_ref=src,
            dst_ref=dst,
            send_sem=send_sem,
            recv_sem=recv_sem,
            device_id={"traces": device},
            device_id_type=pl.DeviceIdType.MESH,
        )

    def block_of(e):
        return x_ref.at[pl.ds(pl.multiple_of(e * each, each), each)]

    barrier = pltpu.get_barrier_semaphore()

    def greet(k, carry):
        other = lax.rem(me + k, n)
        pl.semaphore_signal(barrier, inc=1, device_id={"traces": other}, device_id_type=pl.DeviceIdType.MESH)
        return carry

    lax.fori_loop(1, n, greet, 0)

    damp_in = pltpu.make_async_copy(damp_ref, damp_smem, near_sems.at[0])
    pick_in = pltpu.make_async_copy(pick_ref, pick_smem.at[0], near_sems.at[1])
    tables_in = [
        pltpu.make_async_copy(there, here, near_sems.at[2 + i])
        for i, (there, here) in enumerate(((fwd_hbm, fwd_ref), (inv_hbm, inv_ref), (tw_hbm, tw_ref)))
    ]
    tiles_in = [
        pltpu.make_async_copy(
            wave_ref.at[pl.ds(h * SUBLANES, SUBLANES), pl.ds(p * LANES, LANES)],
            bank_ref.at[me, h * pieces + p],
            near_sems.at[5 + h * pieces + p],
        )
        for h in range(halves)
        for p in range(pieces)
    ]
    for copy in [damp_in] + tiles_in + [pick_in] + tables_in:
        copy.start()

    def load(e):
        return pltpu.make_async_copy(block_of(e), buf_ref.at[n + e], load_sems.at[e])

    def load_start(k, carry):
        @pl.when(k != half)
        def _():
            load(lax.rem(me + k, n)).start()

        return carry

    lax.fori_loop(1, n + 1, load_start, 0)

    damp_in.wait()
    lane = lax.broadcasted_iota(jnp.int32, (SUBLANES, LANES), 1)
    levels = jnp.zeros((SUBLANES, LANES), jnp.float32)
    for f in range(own):
        levels = jnp.where(lane == f, damp_smem[f], levels)
    bank_ref[me, last] = levels
    for copy in tiles_in:
        copy.wait()
    pl.semaphore_wait(barrier, n - 1)

    def far_copy(t):
        there = lax.rem(far + t, outer) * inner + near
        return remote(bank_ref.at[me], bank_ref.at[me], bank_sends.at[t - 1], bank_recvs.at[me], there)

    def near_copy(t, d):
        block = lax.rem(far + t, outer) * inner + near
        there = far * inner + lax.rem(near + d, inner)
        slot = outer - 1 + (d - 1) * outer + t
        return remote(bank_ref.at[block], bank_ref.at[block], bank_sends.at[slot], bank_recvs.at[block], there)

    def bank_came(block):
        return remote(bank_ref.at[block], bank_ref.at[block], bank_sends.at[0], bank_recvs.at[block], partner)

    for t in range(1, outer):
        far_copy(t).start()
    raw_out = remote(block_of(partner), buf_ref.at[n + me], raw_sems.at[0], raw_sems.at[1], partner)
    raw_came = remote(block_of(partner), buf_ref.at[n + partner], raw_sems.at[0], raw_sems.at[1], partner)
    picks_out = remote(pick_ref, pick_smem.at[1], pick_sems.at[0], pick_sems.at[1], partner)
    raw_out.start()
    picks_out.start()
    for d in range(1, inner):
        near_copy(0, d).start()
    for t in range(1, outer):
        bank_came(lax.rem(far + t, outer) * inner + near).wait_recv()
        for d in range(1, inner):
            near_copy(t, d).start()
    for d in range(1, inner):
        for t in range(outer):
            bank_came(lax.rem(far + t, outer) * inner + lax.rem(near + d, inner)).wait_recv()
    pick_in.wait()
    for copy in tables_in:
        copy.wait()

    def turn_of(s):
        return jnp.where(s < half - 1, s + 1, jnp.where(s < n - 2, s + 2, jnp.where(s == n - 2, half, 0)))

    def send(e):
        return remote(buf_ref.at[n + e], buf_ref.at[me], sends.at[e], recvs.at[me], e)

    row_lane = lax.broadcasted_iota(jnp.int32, (1, LANES), 1)

    def step(s, carry):
        e = lax.rem(me + turn_of(s), n)
        theirs = s == n - 2

        @pl.when(theirs)
        def _():
            raw_came.wait_recv()
            picks_out.wait_recv()

        @pl.when(jnp.logical_not(theirs))
        def _():
            load(e).wait()

        table = jnp.where(theirs, 1, 0)
        base = jnp.where(theirs, me, e) * each
        for r in range(ROWS):
            pick = pick_smem[table, base + r]
            block, inside = lax.div(pick, own), lax.rem(pick, own)
            tile, sub = lax.div(inside, SUBLANES) * pieces, lax.rem(inside, SUBLANES)
            for p in range(pieces):
                rows_ref[r : r + 1, p * LANES : (p + 1) * LANES] = bank_ref[block, tile + p, pl.ds(sub, 1), :]
            level = bank_ref[block, last, 0:1, :]
            rows_ref[r : r + 1, taps : taps + LANES] = jnp.where(row_lane == inside, level, 0.0)

        @pl.when(jnp.logical_and(s >= 1, s <= n - 2))
        def _():
            send(lax.rem(me + turn_of(s - 1), n)).start()

        slot = jnp.where(s >= n - 2, e, n + e)
        wave = [rows_ref[:, p * LANES : (p + 1) * LANES] for p in range(pieces)]
        power = sum(jnp.sum(w * w, axis=1, keepdims=True) for w in wave)
        damp = jnp.sum(rows_ref[:, taps : taps + LANES], axis=1, keepdims=True)
        floor = jnp.broadcast_to(damp * (power + 1e-6), (ROWS, LANES))

        def read(j):
            return buf_ref[n + e, :, j * LANES : (j + 1) * LANES]

        def write(j, value):
            buf_ref[slot, :, j * LANES : (j + 1) * LANES] = value

        deconvolve(read, write, wave, floor, fwd_ref, inv_ref, tw_ref, mid_ref, cut_ref, spec_ref)
        return carry

    lax.fori_loop(0, n, step, 0)

    raw_out.wait_send()
    picks_out.wait_send()
    for t in range(1, outer):
        far_copy(t).wait_send()
    for d in range(1, inner):
        for t in range(outer):
            near_copy(t, d).wait_send()

    def finish(k, carry):
        @pl.when(k != half)
        def _():
            e = lax.rem(me + k, n)
            send(e).wait_send()
            remote(buf_ref.at[e], buf_ref.at[e], sends.at[e], recvs.at[e], e).wait_recv()

        return carry

    lax.fori_loop(1, n, finish, 0)


def settle_kernel(n, order_ref, came_ref, o_ref, sems):
    rows = o_ref.shape[0]
    each = rows // n

    def put(d, carry):
        for r in range(each):
            q = d * each + r
            place = order_ref[q]
            came = came_ref.at[lax.rem(place, n), pl.ds(lax.div(place, n), 1)]
            pltpu.make_async_copy(came, o_ref.at[pl.ds(q, 1)], sems.at[d]).start()
        return carry

    lax.fori_loop(0, n, put, 0)

    def finish(d, carry):
        part = o_ref.at[pl.ds(pl.multiple_of(d * each, each), each)]
        pltpu.make_async_copy(came_ref.at[0], part, sems.at[d]).wait()
        return carry

    lax.fori_loop(0, n, finish, 0)


def tables(length, taps):
    return (
        jnp.asarray(lane_matrix(-1.0, 1.0)),
        jnp.asarray(lane_matrix(1.0, 1.0 / length)),
        jnp.asarray(twiddles(length, taps)),
    )


def scratch():
    return [
        pltpu.VMEM((RADIX * RADIX, ROWS, LANES), jnp.float32),
        pltpu.VMEM((2 * KEEP * ROWS, 6 * LANES), jnp.bfloat16),
        pltpu.VMEM((2 * KEEP * ROWS, 2 * LANES), jnp.float32),
    ]


def gathered(raw_traces, filter_index, channel_order, wavelets, damping):
    rows, length = raw_traces.shape
    own, taps = wavelets.shape
    n = lax.axis_size("traces")
    me = lax.axis_index("traces")
    each = rows // n
    floor = damping * (jnp.sum(wavelets * wavelets, axis=1) + 1e-6)
    picks = filter_index.reshape(own, rows // own).astype(jnp.float32)
    packed = lax.all_gather(jnp.concatenate([wavelets, floor[:, None], picks], axis=1), "traces", axis=0, tiled=True)
    all_picks = packed[:, taps + 1 :].reshape(n, n, each).astype(jnp.int32)
    came_picks = lax.dynamic_index_in_dim(all_picks, me, 1, keepdims=False)
    bank = jnp.concatenate([packed[:, :taps], jnp.broadcast_to(packed[:, taps : taps + 1], (own * n, LANES))], axis=1)
    fwd, inv, tw = tables(length, taps)
    whole = lambda a: pl.BlockSpec(a.shape, lambda i, *_: (0,) * a.ndim)
    fixed = [pl.BlockSpec((ROWS, taps + LANES), lambda i, *_: (i, 0)), whole(fwd), whole(inv), whole(tw)]
    came = lax.all_to_all(raw_traces.reshape(n, each, length), "traces", 0, 0, tiled=True).reshape(rows, length)
    result = pl.pallas_call(
        functools.partial(block_kernel, taps, ()),
        grid=(rows // ROWS,),
        out_shape=jax.ShapeDtypeStruct((rows, length), jnp.float32),
        in_specs=[pl.BlockSpec((ROWS, length), lambda i: (i, 0))] + fixed,
        out_specs=pl.BlockSpec((ROWS, length), lambda i: (i, 0)),
        scratch_shapes=scratch(),
        compiler_params=pltpu.CompilerParams(vmem_limit_bytes=48 * 1024 * 1024),
    )(came, jnp.take(bank, came_picks.reshape(-1), axis=0), fwd, inv, tw)
    return jnp.take(result, (channel_order % n) * each + channel_order // n, axis=0)


def local(raw_traces, filter_index, channel_order, wavelets, damping):
    rows, length = raw_traces.shape
    own, taps = wavelets.shape
    n = lax.axis_size("traces")
    if n % 2 or rows != n * ROWS or own % SUBLANES or own > LANES or taps % LANES:
        return gathered(raw_traces, filter_index, channel_order, wavelets, damping)

    fwd, inv, tw = tables(length, taps)
    tiles = own // SUBLANES * (taps // LANES)
    dma = pltpu.SemaphoreType.DMA
    came = pl.pallas_call(
        functools.partial(exchange_kernel, n, taps),
        in_specs=[pl.BlockSpec(memory_space=pltpu.HBM)] * 7,
        out_specs=pl.BlockSpec(memory_space=pltpu.VMEM),
        out_shape=pltpu.VMEM((2 * n, ROWS, length), jnp.float32),
        scratch_shapes=scratch()
        + [pltpu.VMEM(a.shape, a.dtype) for a in (fwd, inv, tw)]
        + [
            pltpu.VMEM((n, tiles + 1, SUBLANES, LANES), jnp.float32),
            pltpu.VMEM((ROWS, taps + LANES), jnp.float32),
            pltpu.SMEM((2, rows), jnp.int32),
            pltpu.SMEM((own,), jnp.float32),
            dma((n,)),
            dma((5 + tiles,)),
            dma((2,)),
            dma((2,)),
            dma((n,)),
            dma((n,)),
            dma((n,)),
            dma((n,)),
        ],
        compiler_params=pltpu.CompilerParams(
            collective_id=0, has_side_effects=True, vmem_limit_bytes=40 * 1024 * 1024
        ),
        cost_estimate=pl.CostEstimate(flops=rows * length * 1500, bytes_accessed=8 * rows * length, transcendentals=0),
    )(raw_traces, filter_index, wavelets, damping, fwd, inv, tw)
    came = pltpu.with_memory_space_constraint(came, pltpu.VMEM)
    return pl.pallas_call(
        functools.partial(settle_kernel, n),
        in_specs=[pl.BlockSpec(memory_space=pltpu.SMEM), pl.BlockSpec(memory_space=pltpu.VMEM)],
        out_specs=pl.BlockSpec(memory_space=pltpu.HBM),
        out_shape=jax.ShapeDtypeStruct((rows, length), jnp.float32),
        scratch_shapes=[dma((n,))],
        compiler_params=pltpu.CompilerParams(vmem_limit_bytes=20 * 1024 * 1024),
    )(channel_order, came)


def solution(mesh):
    placed = (
        P(("groups", "traces"), None),
        P(("groups", "traces")),
        P("groups"),
        P("traces", None),
        P("traces"),
    )
    return jax.shard_map(
        local, mesh=mesh, in_specs=placed, out_specs=P(("groups", "traces"), None), check_vma=False
    )
```

```python
import functools
import math

import jax
import jax.numpy as jnp
import numpy as np
from jax import lax
from jax.experimental import pallas as pl
from jax.experimental.pallas import tpu as pltpu
from jax.sharding import PartitionSpec as P

LANES = 128
RADIX = 8
ROWS = 16
SUBLANES = 8

KEPT = (
    [RADIX * b for b in range(RADIX // 2 + 1)]
    + [a + RADIX * b for a in range(1, RADIX // 2) for b in range(RADIX)]
    + [RADIX // 2 + RADIX * b for b in range(RADIX // 2)]
)
SLOT = {k: s for s, k in enumerate(KEPT)}
KEEP = len(KEPT)


def lane_matrix(sign, scale):
    ids = np.arange(LANES)
    angle = 2.0 * np.pi * (np.outer(ids, ids) % LANES) / LANES
    c, s = np.cos(angle) * scale, sign * np.sin(angle) * scale
    full = np.block([[c, s], [-s, c]])
    import ml_dtypes

    high = full.astype(np.float32).astype(ml_dtypes.bfloat16)
    low = (full.astype(np.float32) - high.astype(np.float32)).astype(ml_dtypes.bfloat16)
    return np.concatenate([high, high, low], axis=0)


def twiddles(length, taps):
    m = np.arange(LANES)
    rows = []
    for k in KEPT:
        angle = 2.0 * np.pi * k * m / length
        row = [np.cos(angle), -np.sin(angle)]
        weight = 1.0 if k in (0, RADIX * RADIX // 2) else 2.0
        row += [weight * np.cos(angle), weight * np.sin(angle)]
        for piece in range(taps // LANES):
            shifted = 2.0 * np.pi * k * (m + LANES * piece) / length
            row += [np.cos(shifted), -np.sin(shifted)]
        rows.append(np.stack(row))
    return np.stack(rows).astype(np.float32)


def cadd(a, b):
    return (a[0] + b[0], a[1] + b[1])


def csub(a, b):
    return (a[0] - b[0], a[1] - b[1])


def turn(a, num, den):
    num %= den
    if num == 0:
        return a
    if 4 * num == den:
        return (-a[1], a[0])
    if 2 * num == den:
        return (-a[0], -a[1])
    if 4 * num == 3 * den:
        return (a[1], -a[0])
    c, s = math.cos(2 * math.pi * num / den), math.sin(2 * math.pi * num / den)
    return (a[0] * c - a[1] * s, a[0] * s + a[1] * c)


def fourier(items, sign):
    n = len(items)
    if n == 1:
        return items
    even, odd = fourier(items[0::2], sign), fourier(items[1::2], sign)
    turned = [turn(o, sign * k, n) for k, o in enumerate(odd)]
    return [cadd(e, t) for e, t in zip(even, turned)] + [csub(e, t) for e, t in zip(even, turned)]


def real_eight(v):
    h = math.sqrt(0.5)
    s0, d0, s1, d1 = v[0] + v[4], v[0] - v[4], v[1] + v[5], v[1] - v[5]
    s2, d2, s3, d3 = v[2] + v[6], v[2] - v[6], v[3] + v[7], v[3] - v[7]
    p, q = s0 + s2, s1 + s3
    r, t = (d1 - d3) * h, (d1 + d3) * h
    return [p + q, (d0 + r, -(d2 + t)), (s0 - s2, s3 - s1), (d0 - r, d2 - t), p - q]


def eight_real(u0, u1, u2, u3, u4):
    h = math.sqrt(0.5)
    p, q = u0 + u4, u0 - u4
    e = [p + u2[0], q - u2[1], p - u2[0], q + u2[1]]
    f, g = u1[0] - u3[0], u1[1] + u3[1]
    o = [u1[0] + u3[0], (f - g) * h, u3[1] - u1[1], -(f + g) * h]
    return [a + b for a, b in zip(e, o)] + [a - b for a, b in zip(e, o)]


def put_split(ref, base, re, im):
    rows = pl.ds(base, ROWS)
    for part, value in enumerate((re, im)):
        high = value.astype(jnp.bfloat16)
        low = (value - high.astype(jnp.float32)).astype(jnp.bfloat16)
        at = part * LANES
        ref[rows, at : at + LANES] = high
        ref[rows, 2 * LANES + at : 2 * LANES + at + LANES] = low
        ref[rows, 4 * LANES + at : 4 * LANES + at + LANES] = high


def deconvolve(read, write, wave, floor, fwd_ref, inv_ref, tw_ref, mid_ref, cut_ref, spec_ref):
    half, wide = RADIX // 2, RADIX * RADIX
    for j2 in range(RADIX):
        out = real_eight([read(RADIX * j1 + j2) for j1 in range(RADIX)])
        mid_ref[2 * j2] = out[0]
        mid_ref[2 * j2 + 1] = out[half]
        for a in range(1, half):
            mid_ref[2 * RADIX * a + 2 * j2] = out[a][0]
            mid_ref[2 * RADIX * a + 2 * j2 + 1] = out[a][1]

    def emit(k, value):
        s = SLOT[k]
        c, n = tw_ref[s, 0:1, :], tw_ref[s, 1:2, :]
        put_split(cut_ref, s * ROWS, value[0] * c - value[1] * n, value[0] * n + value[1] * c)

    zero = real_eight([mid_ref[2 * j2] for j2 in range(RADIX)])
    c, n = tw_ref[0, 0:1, :], tw_ref[0, 1:2, :]
    for b in range(half + 1):
        s = SLOT[RADIX * b]
        c, n = tw_ref[s, 0:1, :], tw_ref[s, 1:2, :]
        if b in (0, half):
            put_split(cut_ref, s * ROWS, zero[b] * c, zero[b] * n)
        else:
            emit(RADIX * b, zero[b])
    for a in range(1, half):
        base = 2 * RADIX * a
        items = [turn((mid_ref[base + 2 * j2], mid_ref[base + 2 * j2 + 1]), -a * j2, wide) for j2 in range(RADIX)]
        for b, value in enumerate(fourier(items, -1)):
            emit(a + RADIX * b, value)
    four = [mid_ref[2 * j2 + 1] for j2 in range(RADIX)]
    for b in range(half):
        k = half + RADIX * b
        re, im = four[0], None
        for j2 in range(1, RADIX):
            angle = 2 * math.pi * (k * j2 % wide) / wide
            re = re + four[j2] * math.cos(angle)
            term = four[j2] * -math.sin(angle)
            im = term if im is None else im + term
        emit(k, (re, im))

    for s in range(KEEP):
        re = im = None
        for piece, taps in enumerate(wave):
            c, n = tw_ref[s, 4 + 2 * piece : 5 + 2 * piece, :], tw_ref[s, 5 + 2 * piece : 6 + 2 * piece, :]
            re = taps * c if re is None else re + taps * c
            im = taps * n if im is None else im + taps * n
        put_split(cut_ref, (KEEP + s) * ROWS, re, im)

    spec_ref[...] = jnp.dot(cut_ref[...], fwd_ref[...], preferred_element_type=jnp.float32)

    def apply(s, carry):
        at = pl.multiple_of(s * ROWS, ROWS)
        other = pl.multiple_of((KEEP + s) * ROWS, ROWS)
        xr, xi = spec_ref[pl.ds(at, ROWS), 0:LANES], spec_ref[pl.ds(at, ROWS), LANES:]
        hr, hi = spec_ref[pl.ds(other, ROWS), 0:LANES], spec_ref[pl.ds(other, ROWS), LANES:]
        scale = 1.0 / (hr * hr + hi * hi + floor)
        put_split(cut_ref, at, (xr * hr + xi * hi) * scale, (xi * hr - xr * hi) * scale)
        return carry

    lax.fori_loop(0, KEEP, apply, 0, unroll=3)
    rows = KEEP * ROWS
    spec_ref[0:rows] = jnp.dot(cut_ref[0:rows], inv_ref[...], preferred_element_type=jnp.float32)

    def fetch(k):
        s = SLOT[k]
        re, im = spec_ref[s * ROWS : (s + 1) * ROWS, 0:LANES], spec_ref[s * ROWS : (s + 1) * ROWS, LANES:]
        c, n = tw_ref[s, 2:3, :], tw_ref[s, 3:4, :]
        if k in (0, wide // 2):
            return re * c - im * n
        return (re * c - im * n, re * n + im * c)

    for a in range(1, half):
        base = 2 * RADIX * a
        for j2, value in enumerate(fourier([fetch(a + RADIX * b) for b in range(RADIX)], 1)):
            value = turn(value, a * j2, wide)
            mid_ref[base + 2 * j2] = value[0]
            mid_ref[base + 2 * j2 + 1] = value[1]
    for j2, value in enumerate(eight_real(*[fetch(RADIX * b) for b in range(half + 1)])):
        mid_ref[2 * j2] = value
    four = [fetch(half + RADIX * b) for b in range(half)]
    for j2 in range(RADIX):
        total = None
        for b, value in enumerate(four):
            angle = 2 * math.pi * ((half + RADIX * b) * j2 % wide) / wide
            term = value[0] * math.cos(angle)
            if j2:
                term = term - value[1] * math.sin(angle)
            total = term if total is None else total + term
        mid_ref[2 * j2 + 1] = total
    for j2 in range(RADIX):
        parts = [mid_ref[2 * j2]]
        for a in range(1, half):
            base = 2 * RADIX * a
            parts.append((mid_ref[base + 2 * j2], mid_ref[base + 2 * j2 + 1]))
        parts.append(mid_ref[2 * j2 + 1])
        for j1, value in enumerate(eight_real(*parts)):
            write(RADIX * j1 + j2, value)


def slabs(ref, lead):
    def at(j):
        return lead + (slice(None), slice(j * LANES, (j + 1) * LANES))

    def read(j):
        value = ref[at(j)]
        return value.reshape(ROWS, LANES)

    def write(j, value):
        ref[at(j)] = value.reshape(ref[at(j)].shape)

    return read, write


def block_kernel(taps, lead, x_ref, w_ref, fwd_ref, inv_ref, tw_ref, o_ref, mid_ref, cut_ref, spec_ref):
    read, _ = slabs(x_ref, lead)
    _, write = slabs(o_ref, (slice(None),) * (len(o_ref.shape) - 2))
    wave = [w_ref[:, p * LANES : (p + 1) * LANES] for p in range(taps // LANES)]
    deconvolve(read, write, wave, w_ref[:, taps : taps + LANES], fwd_ref, inv_ref, tw_ref, mid_ref, cut_ref, spec_ref)


def split_count(n):
    inner = 1
    while inner * inner < n:
        inner *= 2
    return (n // inner, inner) if n % inner == 0 else (1, n)


def block_order(n):
    inner = split_count(n)[1]
    raws = [n - inner, (n - inner) ^ 1]
    near = sorted(range(1, n // 2), key=lambda k: (k < inner, k))
    cross = [k for k in range(n // 2, n) if k not in raws]
    lead, rest = cross[:inner], cross[inner:]
    mixed = lead[:1] + [k for pair in zip(lead[1:], near) for k in pair]
    return mixed + near[max(len(lead) - 1, 0) :] + rest + raws + [0], raws


def exchange_kernel(
    n,
    taps,
    x_ref,
    pick_ref,
    wave_ref,
    damp_ref,
    fwd_hbm,
    inv_hbm,
    tw_hbm,
    buf_ref,
    mid_ref,
    cut_ref,
    spec_ref,
    fwd_ref,
    inv_ref,
    tw_ref,
    bank_ref,
    rows_ref,
    pick_smem,
    damp_smem,
    load_sems,
    near_sems,
    raw_sems,
    pick_sems,
    bank_sends,
    bank_recvs,
    ready_sems,
    sends,
    recvs,
):
    me = lax.axis_index("traces")
    own, each = wave_ref.shape[0], x_ref.shape[0] // n
    outer, inner = split_count(n)
    partner = me ^ (n - inner)
    far, near = lax.div(me, inner), lax.rem(me, inner)
    halves, pieces = own // SUBLANES, taps // LANES
    last = halves * pieces

    def remote(src, dst, send_sem, recv_sem, device):
        return pltpu.make_async_remote_copy(
            src_ref=src,
            dst_ref=dst,
            send_sem=send_sem,
            recv_sem=recv_sem,
            device_id={"traces": device},
            device_id_type=pl.DeviceIdType.MESH,
        )

    def block_of(e):
        return x_ref.at[pl.ds(pl.multiple_of(e * each, each), each)]

    turns, raws = block_order(n)
    made = n - 1 - len(raws)

    def turn_of(s):
        k = 0
        for i, turn in enumerate(turns):
            k = jnp.where(s == i, turn, k)
        return k

    barrier = pltpu.get_barrier_semaphore()

    def tell(sem, other):
        pl.semaphore_signal(sem, inc=1, device_id={"traces": other}, device_id_type=pl.DeviceIdType.MESH)

    def greet(other, carry):
        tell(barrier, other)
        return carry

    def answer(other, carry):
        @pl.when(other != partner)
        def _():
            tell(ready_sems.at[me], other)

        return carry

    def meet(other, carry):
        @pl.when(other != partner)
        def _():
            pl.semaphore_wait(ready_sems.at[other], 1)

        return carry

    lax.fori_loop(me + 1, n, greet, 0)

    damp_in = pltpu.make_async_copy(damp_ref, damp_smem, near_sems.at[0])
    pick_in = pltpu.make_async_copy(pick_ref, pick_smem.at[pl.ds(0, n * each)], near_sems.at[1])
    tables_in = [
        pltpu.make_async_copy(there, here, near_sems.at[2 + i])
        for i, (there, here) in enumerate(((fwd_hbm, fwd_ref), (inv_hbm, inv_ref), (tw_hbm, tw_ref)))
    ]
    tiles_in = [
        pltpu.make_async_copy(
            wave_ref.at[pl.ds(h * SUBLANES, SUBLANES), pl.ds(p * LANES, LANES)],
            bank_ref.at[me, h * pieces + p],
            near_sems.at[5 + h * pieces + p],
        )
        for h in range(halves)
        for p in range(pieces)
    ]
    for copy in [damp_in] + tiles_in + [pick_in] + tables_in:
        copy.start()

    def load(e):
        return pltpu.make_async_copy(block_of(e), buf_ref.at[n + e], load_sems.at[e])

    def load_start(s, carry):
        @pl.when(jnp.logical_or(s < made, s == n - 1))
        def _():
            load(me ^ turn_of(s)).start()

        return carry

    def raw(i, part, here):
        first, count, other = part * (each // 2), each // 2, me ^ raws[i]
        rows = x_ref.at[pl.ds(pl.multiple_of(other * each + first, count), count)]
        there = buf_ref.at[n + jnp.where(here, other, me), pl.ds(first, count)]
        return remote(rows, there, raw_sems.at[0, i, part], raw_sems.at[1, i, part], other)

    def picks(i):
        count = n * each
        there = pick_smem.at[pl.ds((1 + i) * count, count)]
        return remote(pick_ref, there, pick_sems.at[0, i], pick_sems.at[1, i], me ^ raws[i])

    @pl.when(me > 0)
    def _():
        pl.semaphore_wait(barrier, me)

    @pl.when(partner < me)
    def _():
        tell(ready_sems.at[me], partner)

    @pl.when(partner > me)
    def _():
        pl.semaphore_wait(ready_sems.at[partner], 1)

    raw(0, 0, False).start()
    lax.fori_loop(0, me, answer, 0)
    damp_in.wait()
    lane = lax.broadcasted_iota(jnp.int32, (SUBLANES, LANES), 1)
    levels = jnp.zeros((SUBLANES, LANES), jnp.float32)
    for f in range(own):
        levels = jnp.where(lane == f, damp_smem[f], levels)
    bank_ref[me, last] = levels
    lax.fori_loop(me + 1, n, meet, 0)
    for copy in tiles_in:
        copy.wait()

    def bank_copy(block, slot, there):
        return remote(bank_ref.at[block], bank_ref.at[block], bank_sends.at[slot], bank_recvs.at[block], there)

    def block_at(f):
        return f * inner + near

    middle = outer // 2
    upper = far >= middle
    gate = jnp.where(upper, middle, middle - 1)

    def across(t, act):
        there = lax.rem(far + t, outer)
        direct = jnp.logical_or((there >= middle) == upper, there == outer - 1 - gate)

        @pl.when(direct)
        def _():
            act(bank_copy(me, t - 1, block_at(there)))

    def onward(t, act):
        block = lax.rem(far + t, outer)
        for there in range(outer):
            slot = outer - 1 + (t - 1) * outer + there
            near_side = (there >= middle) == upper
            foreign = (block >= middle) != upper
            go = jnp.logical_and(jnp.logical_and(far == gate, far != there), jnp.logical_and(near_side, foreign))

            @pl.when(go)
            def _():
                act(bank_copy(block_at(block), slot, block_at(there)))

    def spread(f, act):
        for d in range(1, inner):
            slot = outer * outer - 1 + f * (inner - 1) + d - 1
            act(bank_copy(block_at(f), slot, far * inner + (near ^ d)))

    def bank_came(block):
        bank_copy(block, 0, partner).wait_recv()

    start, sent = (lambda copy: copy.start()), (lambda copy: copy.wait_send())
    for t in range(1, outer):
        across(t, start)
    spread(far, start)
    raw(0, 1, False).start()
    for i in range(1, len(raws)):
        raw(i, 0, False).start()
        raw(i, 1, False).start()
    for i in range(len(raws)):
        picks(i).start()
    lax.fori_loop(0, n, load_start, 0)
    for t in range(1, outer):
        block = lax.rem(far + t, outer)
        bank_came(block_at(block))
        onward(t, start)
        spread(block, start)
    for f in range(outer):
        for d in range(1, inner):
            bank_came(f * inner + (near ^ d))
    pick_in.wait()
    for copy in tables_in:
        copy.wait()

    def send(e):
        return remote(buf_ref.at[n + e], buf_ref.at[me], sends.at[e], recvs.at[me], e)

    row_lane = lax.broadcasted_iota(jnp.int32, (1, LANES), 1)

    def step(s, carry):
        e = me ^ turn_of(s)
        theirs = jnp.logical_and(s >= made, s < n - 1)
        for i in range(len(raws)):

            @pl.when(s == made + i)
            def _():
                raw(i, 0, True).wait_recv()
                raw(i, 1, True).wait_recv()
                picks(i).wait_recv()

        @pl.when(jnp.logical_not(theirs))
        def _():
            load(e).wait()

        table = jnp.where(theirs, s - made + 1, 0)
        base = (table * n + jnp.where(theirs, me, e)) * each
        for r in range(ROWS):
            pick = pick_smem[base + r]
            block, inside = lax.div(pick, own), lax.rem(pick, own)
            tile, sub = lax.div(inside, SUBLANES) * pieces, lax.rem(inside, SUBLANES)
            for p in range(pieces):
                rows_ref[r : r + 1, p * LANES : (p + 1) * LANES] = bank_ref[block, tile + p, pl.ds(sub, 1), :]
            level = bank_ref[block, last, 0:1, :]
            rows_ref[r : r + 1, taps : taps + LANES] = jnp.where(row_lane == inside, level, 0.0)

        @pl.when(jnp.logical_and(s >= 1, s <= made))
        def _():
            send(me ^ turn_of(s - 1)).start()

        slot = jnp.where(s >= made, e, n + e)
        wave = [rows_ref[:, p * LANES : (p + 1) * LANES] for p in range(pieces)]
        power = sum(jnp.sum(w * w, axis=1, keepdims=True) for w in wave)
        damp = jnp.sum(rows_ref[:, taps : taps + LANES], axis=1, keepdims=True)
        floor = jnp.broadcast_to(damp * (power + 1e-6), (ROWS, LANES))

        def read(j):
            return buf_ref[n + e, :, j * LANES : (j + 1) * LANES]

        def write(j, value):
            buf_ref[slot, :, j * LANES : (j + 1) * LANES] = value

        deconvolve(read, write, wave, floor, fwd_ref, inv_ref, tw_ref, mid_ref, cut_ref, spec_ref)
        return carry

    lax.fori_loop(0, n, step, 0)

    for i in range(len(raws)):
        raw(i, 0, False).wait_send()
        raw(i, 1, False).wait_send()
        picks(i).wait_send()
    for t in range(1, outer):
        across(t, sent)
        onward(t, sent)
    for f in range(outer):
        spread(f, sent)

    def finish(s, carry):
        e = me ^ turn_of(s)
        send(e).wait_send()
        remote(buf_ref.at[e], buf_ref.at[e], sends.at[e], recvs.at[e], e).wait_recv()
        return carry

    lax.fori_loop(0, made, finish, 0)


def settle_kernel(n, order_ref, came_ref, o_ref, sems):
    each = o_ref.shape[0] // n
    shift = n.bit_length() - 1

    def put(d, carry):
        for r in range(each):
            q = d * each + r
            place = order_ref[q]
            came = came_ref.at[place & (n - 1), pl.ds(place >> shift, 1)]
            pltpu.make_async_copy(came, o_ref.at[pl.ds(q, 1)], sems.at[d]).start()
        return carry

    lax.fori_loop(0, n, put, 0)

    def finish(d, carry):
        part = o_ref.at[pl.ds(pl.multiple_of(d * each, each), each)]
        pltpu.make_async_copy(came_ref.at[0], part, sems.at[d]).wait()
        return carry

    lax.fori_loop(0, n, finish, 0)


def tables(length, taps):
    return (
        jnp.asarray(lane_matrix(-1.0, 1.0)),
        jnp.asarray(lane_matrix(1.0, 1.0 / length)),
        jnp.asarray(twiddles(length, taps)),
    )


def scratch():
    return [
        pltpu.VMEM((RADIX * RADIX, ROWS, LANES), jnp.float32),
        pltpu.VMEM((2 * KEEP * ROWS, 6 * LANES), jnp.bfloat16),
        pltpu.VMEM((2 * KEEP * ROWS, 2 * LANES), jnp.float32),
    ]


def gathered(raw_traces, filter_index, channel_order, wavelets, damping):
    rows, length = raw_traces.shape
    own, taps = wavelets.shape
    n = lax.axis_size("traces")
    me = lax.axis_index("traces")
    each = rows // n
    floor = damping * (jnp.sum(wavelets * wavelets, axis=1) + 1e-6)
    picks = filter_index.reshape(own, rows // own).astype(jnp.float32)
    packed = lax.all_gather(jnp.concatenate([wavelets, floor[:, None], picks], axis=1), "traces", axis=0, tiled=True)
    all_picks = packed[:, taps + 1 :].reshape(n, n, each).astype(jnp.int32)
    came_picks = lax.dynamic_index_in_dim(all_picks, me, 1, keepdims=False)
    bank = jnp.concatenate([packed[:, :taps], jnp.broadcast_to(packed[:, taps : taps + 1], (own * n, LANES))], axis=1)
    fwd, inv, tw = tables(length, taps)
    whole = lambda a: pl.BlockSpec(a.shape, lambda i, *_: (0,) * a.ndim)
    fixed = [pl.BlockSpec((ROWS, taps + LANES), lambda i, *_: (i, 0)), whole(fwd), whole(inv), whole(tw)]
    came = lax.all_to_all(raw_traces.reshape(n, each, length), "traces", 0, 0, tiled=True).reshape(rows, length)
    result = pl.pallas_call(
        functools.partial(block_kernel, taps, ()),
        grid=(rows // ROWS,),
        out_shape=jax.ShapeDtypeStruct((rows, length), jnp.float32),
        in_specs=[pl.BlockSpec((ROWS, length), lambda i: (i, 0))] + fixed,
        out_specs=pl.BlockSpec((ROWS, length), lambda i: (i, 0)),
        scratch_shapes=scratch(),
        compiler_params=pltpu.CompilerParams(vmem_limit_bytes=48 * 1024 * 1024),
    )(came, jnp.take(bank, came_picks.reshape(-1), axis=0), fwd, inv, tw)
    return jnp.take(result, (channel_order % n) * each + channel_order // n, axis=0)


def local(raw_traces, filter_index, channel_order, wavelets, damping):
    rows, length = raw_traces.shape
    own, taps = wavelets.shape
    n = lax.axis_size("traces")
    if n < 4 or n & (n - 1) or rows != n * ROWS or own % SUBLANES or own > LANES or taps % LANES:
        return gathered(raw_traces, filter_index, channel_order, wavelets, damping)

    fwd, inv, tw = tables(length, taps)
    tiles = own // SUBLANES * (taps // LANES)
    outer = split_count(n)[0]
    raws = len(block_order(n)[1])
    dma = pltpu.SemaphoreType.DMA
    came = pl.pallas_call(
        functools.partial(exchange_kernel, n, taps),
        in_specs=[pl.BlockSpec(memory_space=pltpu.HBM)] * 7,
        out_specs=pl.BlockSpec(memory_space=pltpu.VMEM),
        out_shape=pltpu.VMEM((2 * n, ROWS, length), jnp.float32),
        scratch_shapes=scratch()
        + [pltpu.VMEM(a.shape, a.dtype) for a in (fwd, inv, tw)]
        + [
            pltpu.VMEM((n, tiles + 1, SUBLANES, LANES), jnp.float32),
            pltpu.VMEM((ROWS, taps + LANES), jnp.float32),
            pltpu.SMEM(((1 + raws) * rows,), jnp.int32),
            pltpu.SMEM((own,), jnp.float32),
            dma((n,)),
            dma((5 + tiles,)),
            dma((2, raws, 2)),
            dma((2, raws)),
            dma((outer * outer - 1 + n - outer,)),
            dma((n,)),
            pltpu.SemaphoreType.REGULAR((n,)),
            dma((n,)),
            dma((n,)),
        ],
        compiler_params=pltpu.CompilerParams(
            collective_id=0, has_side_effects=True, vmem_limit_bytes=40 * 1024 * 1024
        ),
        cost_estimate=pl.CostEstimate(flops=rows * length * 1500, bytes_accessed=8 * rows * length, transcendentals=0),
    )(raw_traces, filter_index, wavelets, damping, fwd, inv, tw)
    came = pltpu.with_memory_space_constraint(came, pltpu.VMEM)
    return pl.pallas_call(
        functools.partial(settle_kernel, n),
        in_specs=[pl.BlockSpec(memory_space=pltpu.SMEM), pl.BlockSpec(memory_space=pltpu.VMEM)],
        out_specs=pl.BlockSpec(memory_space=pltpu.HBM),
        out_shape=jax.ShapeDtypeStruct((rows, length), jnp.float32),
        scratch_shapes=[dma((n,))],
        compiler_params=pltpu.CompilerParams(vmem_limit_bytes=20 * 1024 * 1024),
    )(channel_order, came)


def solution(mesh):
    placed = (
        P(("groups", "traces"), None),
        P(("groups", "traces")),
        P("groups"),
        P("traces", None),
        P("traces"),
    )
    return jax.shard_map(
        local, mesh=mesh, in_specs=placed, out_specs=P(("groups", "traces"), None), check_vma=False
    )
```

```python
import functools
import math

import jax
import jax.numpy as jnp
import numpy as np
from jax import lax
from jax.experimental import pallas as pl
from jax.experimental.pallas import tpu as pltpu
from jax.sharding import PartitionSpec as P

LANES = 128
RADIX = 8
ROWS = 16
SUBLANES = 8

KEPT = (
    [RADIX * b for b in range(RADIX // 2 + 1)]
    + [a + RADIX * b for a in range(1, RADIX // 2) for b in range(RADIX)]
    + [RADIX // 2 + RADIX * b for b in range(RADIX // 2)]
)
SLOT = {k: s for s, k in enumerate(KEPT)}
KEEP = len(KEPT)


def lane_matrix(sign, scale):
    ids = np.arange(LANES)
    angle = 2.0 * np.pi * (np.outer(ids, ids) % LANES) / LANES
    c, s = np.cos(angle) * scale, sign * np.sin(angle) * scale
    full = np.block([[c, s], [-s, c]])
    import ml_dtypes

    high = full.astype(np.float32).astype(ml_dtypes.bfloat16)
    low = (full.astype(np.float32) - high.astype(np.float32)).astype(ml_dtypes.bfloat16)
    return np.concatenate([high, high, low], axis=0)


def twiddles(length, taps):
    m = np.arange(LANES)
    rows = []
    for k in KEPT:
        angle = 2.0 * np.pi * k * m / length
        row = [np.cos(angle), -np.sin(angle)]
        weight = 1.0 if k in (0, RADIX * RADIX // 2) else 2.0
        row += [weight * np.cos(angle), weight * np.sin(angle)]
        for piece in range(taps // LANES):
            shifted = 2.0 * np.pi * k * (m + LANES * piece) / length
            row += [np.cos(shifted), -np.sin(shifted)]
        rows.append(np.stack(row))
    return np.stack(rows).astype(np.float32)


def cadd(a, b):
    return (a[0] + b[0], a[1] + b[1])


def csub(a, b):
    return (a[0] - b[0], a[1] - b[1])


def turn(a, num, den):
    num %= den
    if num == 0:
        return a
    if 4 * num == den:
        return (-a[1], a[0])
    if 2 * num == den:
        return (-a[0], -a[1])
    if 4 * num == 3 * den:
        return (a[1], -a[0])
    c, s = math.cos(2 * math.pi * num / den), math.sin(2 * math.pi * num / den)
    return (a[0] * c - a[1] * s, a[0] * s + a[1] * c)


def fourier(items, sign):
    n = len(items)
    if n == 1:
        return items
    even, odd = fourier(items[0::2], sign), fourier(items[1::2], sign)
    turned = [turn(o, sign * k, n) for k, o in enumerate(odd)]
    return [cadd(e, t) for e, t in zip(even, turned)] + [csub(e, t) for e, t in zip(even, turned)]


def real_eight(v):
    h = math.sqrt(0.5)
    s0, d0, s1, d1 = v[0] + v[4], v[0] - v[4], v[1] + v[5], v[1] - v[5]
    s2, d2, s3, d3 = v[2] + v[6], v[2] - v[6], v[3] + v[7], v[3] - v[7]
    p, q = s0 + s2, s1 + s3
    r, t = (d1 - d3) * h, (d1 + d3) * h
    return [p + q, (d0 + r, -(d2 + t)), (s0 - s2, s3 - s1), (d0 - r, d2 - t), p - q]


def eight_real(u0, u1, u2, u3, u4):
    h = math.sqrt(0.5)
    p, q = u0 + u4, u0 - u4
    e = [p + u2[0], q - u2[1], p - u2[0], q + u2[1]]
    f, g = u1[0] - u3[0], u1[1] + u3[1]
    o = [u1[0] + u3[0], (f - g) * h, u3[1] - u1[1], -(f + g) * h]
    return [a + b for a, b in zip(e, o)] + [a - b for a, b in zip(e, o)]


def put_split(ref, base, re, im):
    rows = pl.ds(base, ROWS)
    for part, value in enumerate((re, im)):
        high = value.astype(jnp.bfloat16)
        low = (value - high.astype(jnp.float32)).astype(jnp.bfloat16)
        at = part * LANES
        ref[rows, at : at + LANES] = high
        ref[rows, 2 * LANES + at : 2 * LANES + at + LANES] = low
        ref[rows, 4 * LANES + at : 4 * LANES + at + LANES] = high


def deconvolve(read, write, wave, floor, fwd_ref, inv_ref, tw_ref, mid_ref, cut_ref, spec_ref):
    half, wide = RADIX // 2, RADIX * RADIX
    for j2 in range(RADIX):
        out = real_eight([read(RADIX * j1 + j2) for j1 in range(RADIX)])
        mid_ref[2 * j2] = out[0]
        mid_ref[2 * j2 + 1] = out[half]
        for a in range(1, half):
            mid_ref[2 * RADIX * a + 2 * j2] = out[a][0]
            mid_ref[2 * RADIX * a + 2 * j2 + 1] = out[a][1]

    def emit(k, value):
        s = SLOT[k]
        c, n = tw_ref[s, 0:1, :], tw_ref[s, 1:2, :]
        put_split(cut_ref, s * ROWS, value[0] * c - value[1] * n, value[0] * n + value[1] * c)

    zero = real_eight([mid_ref[2 * j2] for j2 in range(RADIX)])
    c, n = tw_ref[0, 0:1, :], tw_ref[0, 1:2, :]
    for b in range(half + 1):
        s = SLOT[RADIX * b]
        c, n = tw_ref[s, 0:1, :], tw_ref[s, 1:2, :]
        if b in (0, half):
            put_split(cut_ref, s * ROWS, zero[b] * c, zero[b] * n)
        else:
            emit(RADIX * b, zero[b])
    for a in range(1, half):
        base = 2 * RADIX * a
        items = [turn((mid_ref[base + 2 * j2], mid_ref[base + 2 * j2 + 1]), -a * j2, wide) for j2 in range(RADIX)]
        for b, value in enumerate(fourier(items, -1)):
            emit(a + RADIX * b, value)
    four = [mid_ref[2 * j2 + 1] for j2 in range(RADIX)]
    for b in range(half):
        k = half + RADIX * b
        re, im = four[0], None
        for j2 in range(1, RADIX):
            angle = 2 * math.pi * (k * j2 % wide) / wide
            re = re + four[j2] * math.cos(angle)
            term = four[j2] * -math.sin(angle)
            im = term if im is None else im + term
        emit(k, (re, im))

    for s in range(KEEP):
        re = im = None
        for piece, taps in enumerate(wave):
            c, n = tw_ref[s, 4 + 2 * piece : 5 + 2 * piece, :], tw_ref[s, 5 + 2 * piece : 6 + 2 * piece, :]
            re = taps * c if re is None else re + taps * c
            im = taps * n if im is None else im + taps * n
        put_split(cut_ref, (KEEP + s) * ROWS, re, im)

    spec_ref[...] = jnp.dot(cut_ref[...], fwd_ref[...], preferred_element_type=jnp.float32)

    def apply(s, carry):
        at = pl.multiple_of(s * ROWS, ROWS)
        other = pl.multiple_of((KEEP + s) * ROWS, ROWS)
        xr, xi = spec_ref[pl.ds(at, ROWS), 0:LANES], spec_ref[pl.ds(at, ROWS), LANES:]
        hr, hi = spec_ref[pl.ds(other, ROWS), 0:LANES], spec_ref[pl.ds(other, ROWS), LANES:]
        scale = 1.0 / (hr * hr + hi * hi + floor)
        put_split(cut_ref, at, (xr * hr + xi * hi) * scale, (xi * hr - xr * hi) * scale)
        return carry

    lax.fori_loop(0, KEEP, apply, 0, unroll=3)
    rows = KEEP * ROWS
    spec_ref[0:rows] = jnp.dot(cut_ref[0:rows], inv_ref[...], preferred_element_type=jnp.float32)

    def fetch(k):
        s = SLOT[k]
        re, im = spec_ref[s * ROWS : (s + 1) * ROWS, 0:LANES], spec_ref[s * ROWS : (s + 1) * ROWS, LANES:]
        c, n = tw_ref[s, 2:3, :], tw_ref[s, 3:4, :]
        if k in (0, wide // 2):
            return re * c - im * n
        return (re * c - im * n, re * n + im * c)

    for a in range(1, half):
        base = 2 * RADIX * a
        for j2, value in enumerate(fourier([fetch(a + RADIX * b) for b in range(RADIX)], 1)):
            value = turn(value, a * j2, wide)
            mid_ref[base + 2 * j2] = value[0]
            mid_ref[base + 2 * j2 + 1] = value[1]
    for j2, value in enumerate(eight_real(*[fetch(RADIX * b) for b in range(half + 1)])):
        mid_ref[2 * j2] = value
    four = [fetch(half + RADIX * b) for b in range(half)]
    for j2 in range(RADIX):
        total = None
        for b, value in enumerate(four):
            angle = 2 * math.pi * ((half + RADIX * b) * j2 % wide) / wide
            term = value[0] * math.cos(angle)
            if j2:
                term = term - value[1] * math.sin(angle)
            total = term if total is None else total + term
        mid_ref[2 * j2 + 1] = total
    for j2 in range(RADIX):
        parts = [mid_ref[2 * j2]]
        for a in range(1, half):
            base = 2 * RADIX * a
            parts.append((mid_ref[base + 2 * j2], mid_ref[base + 2 * j2 + 1]))
        parts.append(mid_ref[2 * j2 + 1])
        for j1, value in enumerate(eight_real(*parts)):
            write(RADIX * j1 + j2, value)


def slabs(ref, lead):
    def at(j):
        return lead + (slice(None), slice(j * LANES, (j + 1) * LANES))

    def read(j):
        value = ref[at(j)]
        return value.reshape(ROWS, LANES)

    def write(j, value):
        ref[at(j)] = value.reshape(ref[at(j)].shape)

    return read, write


def block_kernel(taps, lead, x_ref, w_ref, fwd_ref, inv_ref, tw_ref, o_ref, mid_ref, cut_ref, spec_ref):
    read, _ = slabs(x_ref, lead)
    _, write = slabs(o_ref, (slice(None),) * (len(o_ref.shape) - 2))
    wave = [w_ref[:, p * LANES : (p + 1) * LANES] for p in range(taps // LANES)]
    deconvolve(read, write, wave, w_ref[:, taps : taps + LANES], fwd_ref, inv_ref, tw_ref, mid_ref, cut_ref, spec_ref)


def split_count(n):
    inner = 1
    while inner * inner < n:
        inner *= 2
    return (n // inner, inner) if n % inner == 0 else (1, n)


def block_order(n):
    inner = split_count(n)[1]
    raws = list(range(n - inner + 1, n, 2))[:2]
    kept = list(range(n - inner, n, 2))[:2]
    near = sorted(range(1, n // 2), key=lambda k: (k < inner, k))
    cross = [k for k in range(n // 2, n) if k not in raws + kept]
    lead, rest = cross[:inner], cross[inner:]
    mixed = lead[:1] + [k for pair in zip(lead[1:], near) for k in pair]
    return mixed + near[max(len(lead) - 1, 0) :] + rest + kept + raws + [0], raws, kept


def keeps_blocks(me, n):
    outer, inner = split_count(n)
    far = lax.div(me, inner)
    return jnp.logical_and(me % 2 == 0, jnp.logical_or(far == outer // 2 - 1, far == outer // 2))


def exchange_kernel(
    n,
    taps,
    x_ref,
    pick_ref,
    wave_ref,
    damp_ref,
    fwd_hbm,
    inv_hbm,
    tw_hbm,
    buf_ref,
    mid_ref,
    cut_ref,
    spec_ref,
    fwd_ref,
    inv_ref,
    tw_ref,
    bank_ref,
    rows_ref,
    pick_smem,
    damp_smem,
    load_sems,
    near_sems,
    raw_sems,
    pick_sems,
    bank_sends,
    bank_recvs,
    ready_sems,
    sends,
    recvs,
):
    me = lax.axis_index("traces")
    own, each = wave_ref.shape[0], x_ref.shape[0] // n
    outer, inner = split_count(n)
    far, near = lax.div(me, inner), lax.rem(me, inner)
    halves, pieces = own // SUBLANES, taps // LANES
    last = halves * pieces

    def remote(src, dst, send_sem, recv_sem, device):
        return pltpu.make_async_remote_copy(
            src_ref=src,
            dst_ref=dst,
            send_sem=send_sem,
            recv_sem=recv_sem,
            device_id={"traces": device},
            device_id_type=pl.DeviceIdType.MESH,
        )

    def block_of(e):
        return x_ref.at[pl.ds(pl.multiple_of(e * each, each), each)]

    turns, raws, kept = block_order(n)
    partner = me ^ raws[0]
    made = n - 1 - len(raws)
    sent_here = made - jnp.where(keeps_blocks(me, n), len(kept), 0)

    def turn_of(s):
        k = 0
        for i, turn in enumerate(turns):
            k = jnp.where(s == i, turn, k)
        return k

    barrier = pltpu.get_barrier_semaphore()

    def tell(sem, other):
        pl.semaphore_signal(sem, inc=1, device_id={"traces": other}, device_id_type=pl.DeviceIdType.MESH)

    def greet(other, carry):
        tell(barrier, other)
        return carry

    def answer(other, carry):
        @pl.when(other != partner)
        def _():
            tell(ready_sems.at[me], other)

        return carry

    def meet(other, carry):
        @pl.when(other != partner)
        def _():
            pl.semaphore_wait(ready_sems.at[other], 1)

        return carry

    lax.fori_loop(me + 1, n, greet, 0)

    damp_in = pltpu.make_async_copy(damp_ref, damp_smem, near_sems.at[0])
    pick_in = pltpu.make_async_copy(pick_ref, pick_smem.at[pl.ds(0, n * each)], near_sems.at[1])
    tables_in = [
        pltpu.make_async_copy(there, here, near_sems.at[2 + i])
        for i, (there, here) in enumerate(((fwd_hbm, fwd_ref), (inv_hbm, inv_ref), (tw_hbm, tw_ref)))
    ]
    tiles_in = [
        pltpu.make_async_copy(
            wave_ref.at[pl.ds(h * SUBLANES, SUBLANES), pl.ds(p * LANES, LANES)],
            bank_ref.at[me, h * pieces + p],
            near_sems.at[5 + h * pieces + p],
        )
        for h in range(halves)
        for p in range(pieces)
    ]
    for copy in [damp_in] + tiles_in + [pick_in] + tables_in:
        copy.start()

    def load(e):
        return pltpu.make_async_copy(block_of(e), buf_ref.at[n + e], load_sems.at[e])

    def load_start(s, carry):
        @pl.when(jnp.logical_or(s < made, s == n - 1))
        def _():
            load(me ^ turn_of(s)).start()

        return carry

    def raw(i, part, here):
        first, count, other = part * (each // 2), each // 2, me ^ raws[i]
        rows = x_ref.at[pl.ds(pl.multiple_of(other * each + first, count), count)]
        there = buf_ref.at[n + jnp.where(here, other, me), pl.ds(first, count)]
        return remote(rows, there, raw_sems.at[0, i, part], raw_sems.at[1, i, part], other)

    def picks(i):
        count = n * each
        there = pick_smem.at[pl.ds((1 + i) * count, count)]
        return remote(pick_ref, there, pick_sems.at[0, i], pick_sems.at[1, i], me ^ raws[i])

    @pl.when(me > 0)
    def _():
        pl.semaphore_wait(barrier, me)

    @pl.when(partner < me)
    def _():
        tell(ready_sems.at[me], partner)

    @pl.when(partner > me)
    def _():
        pl.semaphore_wait(ready_sems.at[partner], 1)

    raw(0, 0, False).start()
    lax.fori_loop(0, me, answer, 0)
    damp_in.wait()
    lane = lax.broadcasted_iota(jnp.int32, (SUBLANES, LANES), 1)
    levels = jnp.zeros((SUBLANES, LANES), jnp.float32)
    for f in range(own):
        levels = jnp.where(lane == f, damp_smem[f], levels)
    bank_ref[me, last] = levels
    lax.fori_loop(me + 1, n, meet, 0)
    for copy in tiles_in:
        copy.wait()

    def bank_copy(block, slot, there):
        return remote(bank_ref.at[block], bank_ref.at[block], bank_sends.at[slot], bank_recvs.at[block], there)

    def block_at(f):
        return f * inner + near

    middle = outer // 2
    upper = far >= middle
    gate = jnp.where(upper, middle, middle - 1)

    def across(t, act):
        there = lax.rem(far + t, outer)
        direct = jnp.logical_or((there >= middle) == upper, there == outer - 1 - gate)

        @pl.when(direct)
        def _():
            act(bank_copy(me, t - 1, block_at(there)))

    def onward(t, act):
        block = lax.rem(far + t, outer)
        for there in range(outer):
            slot = outer - 1 + (t - 1) * outer + there
            near_side = (there >= middle) == upper
            foreign = (block >= middle) != upper
            go = jnp.logical_and(jnp.logical_and(far == gate, far != there), jnp.logical_and(near_side, foreign))

            @pl.when(go)
            def _():
                act(bank_copy(block_at(block), slot, block_at(there)))

    def spread(f, act):
        for d in range(1, inner):
            slot = outer * outer - 1 + f * (inner - 1) + d - 1
            act(bank_copy(block_at(f), slot, far * inner + (near ^ d)))

    def bank_came(block):
        bank_copy(block, 0, partner).wait_recv()

    start, sent = (lambda copy: copy.start()), (lambda copy: copy.wait_send())
    for t in range(1, outer):
        across(t, start)
    spread(far, start)
    raw(0, 1, False).start()
    for i in range(1, len(raws)):
        raw(i, 0, False).start()
        raw(i, 1, False).start()
    for i in range(len(raws)):
        picks(i).start()
    lax.fori_loop(0, n, load_start, 0)
    for t in range(1, outer):
        block = lax.rem(far + t, outer)
        bank_came(block_at(block))
        onward(t, start)
        spread(block, start)
    for f in range(outer):
        for d in range(1, inner):
            bank_came(f * inner + (near ^ d))
    pick_in.wait()
    for copy in tables_in:
        copy.wait()

    def send(e):
        return remote(buf_ref.at[n + e], buf_ref.at[me], sends.at[e], recvs.at[me], e)

    row_lane = lax.broadcasted_iota(jnp.int32, (1, LANES), 1)

    def step(s, carry):
        e = me ^ turn_of(s)
        theirs = jnp.logical_and(s >= made, s < n - 1)
        for i in range(len(raws)):

            @pl.when(s == made + i)
            def _():
                raw(i, 0, True).wait_recv()
                raw(i, 1, True).wait_recv()
                picks(i).wait_recv()

        @pl.when(jnp.logical_not(theirs))
        def _():
            load(e).wait()

        table = jnp.where(theirs, s - made + 1, 0)
        base = (table * n + jnp.where(theirs, me, e)) * each
        for r in range(ROWS):
            pick = pick_smem[base + r]
            block, inside = lax.div(pick, own), lax.rem(pick, own)
            tile, sub = lax.div(inside, SUBLANES) * pieces, lax.rem(inside, SUBLANES)
            for p in range(pieces):
                rows_ref[r : r + 1, p * LANES : (p + 1) * LANES] = bank_ref[block, tile + p, pl.ds(sub, 1), :]
            level = bank_ref[block, last, 0:1, :]
            rows_ref[r : r + 1, taps : taps + LANES] = jnp.where(row_lane == inside, level, 0.0)

        @pl.when(jnp.logical_and(s >= 1, s <= sent_here))
        def _():
            send(me ^ turn_of(s - 1)).start()

        slot = jnp.where(s >= made, e, n + e)
        wave = [rows_ref[:, p * LANES : (p + 1) * LANES] for p in range(pieces)]
        power = sum(jnp.sum(w * w, axis=1, keepdims=True) for w in wave)
        damp = jnp.sum(rows_ref[:, taps : taps + LANES], axis=1, keepdims=True)
        floor = jnp.broadcast_to(damp * (power + 1e-6), (ROWS, LANES))

        def read(j):
            return buf_ref[n + e, :, j * LANES : (j + 1) * LANES]

        def write(j, value):
            buf_ref[slot, :, j * LANES : (j + 1) * LANES] = value

        deconvolve(read, write, wave, floor, fwd_ref, inv_ref, tw_ref, mid_ref, cut_ref, spec_ref)
        return carry

    lax.fori_loop(0, n, step, 0)

    for i in range(len(raws)):
        raw(i, 0, False).wait_send()
        raw(i, 1, False).wait_send()
        picks(i).wait_send()
    for t in range(1, outer):
        across(t, sent)
        onward(t, sent)
    for f in range(outer):
        spread(f, sent)

    def finish(s, carry):
        e = me ^ turn_of(s)
        send(e).wait_send()
        remote(buf_ref.at[e], buf_ref.at[e], sends.at[e], recvs.at[e], e).wait_recv()
        return carry

    lax.fori_loop(0, sent_here, finish, 0)


def late_kernel(n, buf_ref, after_ref, late_ref, sends, recvs):
    del after_ref
    me = lax.axis_index("traces")
    kept = block_order(n)[2]

    @pl.when(keeps_blocks(me, n))
    def _():
        barrier = pltpu.get_barrier_semaphore()
        for k in kept:
            pl.semaphore_signal(barrier, inc=1, device_id={"traces": me ^ k}, device_id_type=pl.DeviceIdType.MESH)
        pl.semaphore_wait(barrier, len(kept))
        copies = [
            pltpu.make_async_remote_copy(
                src_ref=buf_ref.at[n + (me ^ k)],
                dst_ref=late_ref.at[i],
                send_sem=sends.at[i],
                recv_sem=recvs.at[i],
                device_id={"traces": me ^ k},
                device_id_type=pl.DeviceIdType.MESH,
            )
            for i, k in enumerate(kept)
        ]
        for copy in copies:
            copy.start()
        for copy in copies:
            copy.wait()


def settle_kernel(n, order_ref, came_ref, o_ref, late_rows_ref, sem):
    rows = o_ref.shape[0]
    each = rows // n
    shift = n.bit_length() - 1
    me = lax.axis_index("traces")
    kept = block_order(n)[2]
    keeps = keeps_blocks(me, n)

    def put(d, carry):
        for r in range(each):
            q = d * each + r
            place = order_ref[q]
            source, row = place & (n - 1), place >> shift
            turn = source ^ me
            late = jnp.logical_and(keeps, functools.reduce(jnp.logical_or, [turn == k for k in kept]))

            @pl.when(late)
            def _():
                index = functools.reduce(lambda at, ik: jnp.where(turn == ik[1], ik[0], at), enumerate(kept), 0)
                late_rows_ref[index * each + row] = q

            @pl.when(jnp.logical_not(late))
            def _():
                pltpu.make_async_copy(came_ref.at[source, pl.ds(row, 1)], o_ref.at[pl.ds(q, 1)], sem).start()

        return carry

    lax.fori_loop(0, n, put, 0)

    def finish(count):
        pltpu.make_async_copy(o_ref.at[pl.ds(0, count)], o_ref.at[pl.ds(0, count)], sem).wait()

    @pl.when(keeps)
    def _():
        finish(rows - len(kept) * each)

    @pl.when(jnp.logical_not(keeps))
    def _():
        finish(rows)


def last_kernel(n, late_rows_ref, late_ref, settled_ref, o_ref, sem):
    del settled_ref
    count, each, _ = late_ref.shape

    @pl.when(keeps_blocks(lax.axis_index("traces"), n))
    def _():
        for i in range(count):
            for r in range(each):
                q = late_rows_ref[i * each + r]
                pltpu.make_async_copy(late_ref.at[i, pl.ds(r, 1)], o_ref.at[pl.ds(q, 1)], sem).start()
        part = o_ref.at[pl.ds(0, count * each)]
        pltpu.make_async_copy(part, part, sem).wait()


def tables(length, taps):
    return (
        jnp.asarray(lane_matrix(-1.0, 1.0)),
        jnp.asarray(lane_matrix(1.0, 1.0 / length)),
        jnp.asarray(twiddles(length, taps)),
    )


def scratch():
    return [
        pltpu.VMEM((RADIX * RADIX, ROWS, LANES), jnp.float32),
        pltpu.VMEM((2 * KEEP * ROWS, 6 * LANES), jnp.bfloat16),
        pltpu.VMEM((2 * KEEP * ROWS, 2 * LANES), jnp.float32),
    ]


def gathered(raw_traces, filter_index, channel_order, wavelets, damping):
    rows, length = raw_traces.shape
    own, taps = wavelets.shape
    n = lax.axis_size("traces")
    me = lax.axis_index("traces")
    each = rows // n
    floor = damping * (jnp.sum(wavelets * wavelets, axis=1) + 1e-6)
    picks = filter_index.reshape(own, rows // own).astype(jnp.float32)
    packed = lax.all_gather(jnp.concatenate([wavelets, floor[:, None], picks], axis=1), "traces", axis=0, tiled=True)
    all_picks = packed[:, taps + 1 :].reshape(n, n, each).astype(jnp.int32)
    came_picks = lax.dynamic_index_in_dim(all_picks, me, 1, keepdims=False)
    bank = jnp.concatenate([packed[:, :taps], jnp.broadcast_to(packed[:, taps : taps + 1], (own * n, LANES))], axis=1)
    fwd, inv, tw = tables(length, taps)
    whole = lambda a: pl.BlockSpec(a.shape, lambda i, *_: (0,) * a.ndim)
    fixed = [pl.BlockSpec((ROWS, taps + LANES), lambda i, *_: (i, 0)), whole(fwd), whole(inv), whole(tw)]
    came = lax.all_to_all(raw_traces.reshape(n, each, length), "traces", 0, 0, tiled=True).reshape(rows, length)
    result = pl.pallas_call(
        functools.partial(block_kernel, taps, ()),
        grid=(rows // ROWS,),
        out_shape=jax.ShapeDtypeStruct((rows, length), jnp.float32),
        in_specs=[pl.BlockSpec((ROWS, length), lambda i: (i, 0))] + fixed,
        out_specs=pl.BlockSpec((ROWS, length), lambda i: (i, 0)),
        scratch_shapes=scratch(),
        compiler_params=pltpu.CompilerParams(vmem_limit_bytes=48 * 1024 * 1024),
    )(came, jnp.take(bank, came_picks.reshape(-1), axis=0), fwd, inv, tw)
    return jnp.take(result, (channel_order % n) * each + channel_order // n, axis=0)


def local(raw_traces, filter_index, channel_order, wavelets, damping):
    rows, length = raw_traces.shape
    own, taps = wavelets.shape
    n = lax.axis_size("traces")
    if n < 4 or n & (n - 1) or rows != n * ROWS or own % SUBLANES or own > LANES or taps % LANES:
        return gathered(raw_traces, filter_index, channel_order, wavelets, damping)

    fwd, inv, tw = tables(length, taps)
    tiles = own // SUBLANES * (taps // LANES)
    outer = split_count(n)[0]
    _, raws, kept = block_order(n)
    raws, kept = len(raws), len(kept)
    dma = pltpu.SemaphoreType.DMA
    came = pl.pallas_call(
        functools.partial(exchange_kernel, n, taps),
        in_specs=[pl.BlockSpec(memory_space=pltpu.HBM)] * 7,
        out_specs=pl.BlockSpec(memory_space=pltpu.VMEM),
        out_shape=pltpu.VMEM((2 * n, ROWS, length), jnp.float32),
        scratch_shapes=scratch()
        + [pltpu.VMEM(a.shape, a.dtype) for a in (fwd, inv, tw)]
        + [
            pltpu.VMEM((n, tiles + 1, SUBLANES, LANES), jnp.float32),
            pltpu.VMEM((ROWS, taps + LANES), jnp.float32),
            pltpu.SMEM(((1 + raws) * rows,), jnp.int32),
            pltpu.SMEM((own,), jnp.float32),
            dma((n,)),
            dma((5 + tiles,)),
            dma((2, raws, 2)),
            dma((2, raws)),
            dma((outer * outer - 1 + n - outer,)),
            dma((n,)),
            pltpu.SemaphoreType.REGULAR((n,)),
            dma((n,)),
            dma((n,)),
        ],
        compiler_params=pltpu.CompilerParams(
            collective_id=0, has_side_effects=True, vmem_limit_bytes=40 * 1024 * 1024
        ),
        cost_estimate=pl.CostEstimate(flops=rows * length * 1500, bytes_accessed=8 * rows * length, transcendentals=0),
    )(raw_traces, filter_index, wavelets, damping, fwd, inv, tw)
    came = pltpu.with_memory_space_constraint(came, pltpu.VMEM)
    smem, vmem, hbm = (pl.BlockSpec(memory_space=m) for m in (pltpu.SMEM, pltpu.VMEM, pltpu.HBM))
    params = pltpu.CompilerParams(vmem_limit_bytes=20 * 1024 * 1024)
    settled, late_rows = pl.pallas_call(
        functools.partial(settle_kernel, n),
        in_specs=[smem, vmem],
        out_specs=[hbm, smem],
        out_shape=[
            jax.ShapeDtypeStruct((rows, length), jnp.float32),
            jax.ShapeDtypeStruct((kept * ROWS,), jnp.int32),
        ],
        scratch_shapes=[dma],
        compiler_params=params,
    )(channel_order, came)
    late = pl.pallas_call(
        functools.partial(late_kernel, n),
        in_specs=[vmem, pl.BlockSpec(memory_space=pl.ANY)],
        out_specs=vmem,
        out_shape=pltpu.VMEM((kept, ROWS, length), jnp.float32),
        scratch_shapes=[dma((kept,)), dma((kept,))],
        compiler_params=pltpu.CompilerParams(
            collective_id=1, has_side_effects=True, vmem_limit_bytes=20 * 1024 * 1024
        ),
    )(came, late_rows)
    late = pltpu.with_memory_space_constraint(late, pltpu.VMEM)
    return pl.pallas_call(
        functools.partial(last_kernel, n),
        in_specs=[smem, vmem, hbm],
        out_specs=hbm,
        out_shape=jax.ShapeDtypeStruct((rows, length), jnp.float32),
        scratch_shapes=[dma],
        input_output_aliases={2: 0},
        compiler_params=params,
    )(late_rows, late, settled)


def solution(mesh):
    placed = (
        P(("groups", "traces"), None),
        P(("groups", "traces")),
        P("groups"),
        P("traces", None),
        P("traces"),
    )
    return jax.shard_map(
        local, mesh=mesh, in_specs=placed, out_specs=P(("groups", "traces"), None), check_vma=False
    )
```

```python
import functools
import math

import jax
import jax.numpy as jnp
import numpy as np
from jax import lax
from jax.experimental import pallas as pl
from jax.experimental.pallas import tpu as pltpu
from jax.sharding import PartitionSpec as P

LANES = 128
RADIX = 8
ROWS = 16
SUBLANES = 8

KEPT = (
    [RADIX * b for b in range(RADIX // 2 + 1)]
    + [a + RADIX * b for a in range(1, RADIX // 2) for b in range(RADIX)]
    + [RADIX // 2 + RADIX * b for b in range(RADIX // 2)]
)
SLOT = {k: s for s, k in enumerate(KEPT)}
KEEP = len(KEPT)


def lane_matrix(sign, scale):
    ids = np.arange(LANES)
    angle = 2.0 * np.pi * (np.outer(ids, ids) % LANES) / LANES
    c, s = np.cos(angle) * scale, sign * np.sin(angle) * scale
    full = np.block([[c, s], [-s, c]])
    import ml_dtypes

    high = full.astype(np.float32).astype(ml_dtypes.bfloat16)
    low = (full.astype(np.float32) - high.astype(np.float32)).astype(ml_dtypes.bfloat16)
    return np.concatenate([high, high, low], axis=0)


def twiddles(length, taps):
    m = np.arange(LANES)
    rows = []
    for k in KEPT:
        angle = 2.0 * np.pi * k * m / length
        row = [np.cos(angle), -np.sin(angle)]
        weight = 1.0 if k in (0, RADIX * RADIX // 2) else 2.0
        row += [weight * np.cos(angle), weight * np.sin(angle)]
        for piece in range(taps // LANES):
            shifted = 2.0 * np.pi * k * (m + LANES * piece) / length
            row += [np.cos(shifted), -np.sin(shifted)]
        rows.append(np.stack(row))
    return np.stack(rows).astype(np.float32)


def cadd(a, b):
    return (a[0] + b[0], a[1] + b[1])


def csub(a, b):
    return (a[0] - b[0], a[1] - b[1])


def turn(a, num, den):
    num %= den
    if num == 0:
        return a
    if 4 * num == den:
        return (-a[1], a[0])
    if 2 * num == den:
        return (-a[0], -a[1])
    if 4 * num == 3 * den:
        return (a[1], -a[0])
    c, s = math.cos(2 * math.pi * num / den), math.sin(2 * math.pi * num / den)
    return (a[0] * c - a[1] * s, a[0] * s + a[1] * c)


def fourier(items, sign):
    n = len(items)
    if n == 1:
        return items
    even, odd = fourier(items[0::2], sign), fourier(items[1::2], sign)
    turned = [turn(o, sign * k, n) for k, o in enumerate(odd)]
    return [cadd(e, t) for e, t in zip(even, turned)] + [csub(e, t) for e, t in zip(even, turned)]


def real_eight(v):
    h = math.sqrt(0.5)
    s0, d0, s1, d1 = v[0] + v[4], v[0] - v[4], v[1] + v[5], v[1] - v[5]
    s2, d2, s3, d3 = v[2] + v[6], v[2] - v[6], v[3] + v[7], v[3] - v[7]
    p, q = s0 + s2, s1 + s3
    r, t = (d1 - d3) * h, (d1 + d3) * h
    return [p + q, (d0 + r, -(d2 + t)), (s0 - s2, s3 - s1), (d0 - r, d2 - t), p - q]


def eight_real(u0, u1, u2, u3, u4):
    h = math.sqrt(0.5)
    p, q = u0 + u4, u0 - u4
    e = [p + u2[0], q - u2[1], p - u2[0], q + u2[1]]
    f, g = u1[0] - u3[0], u1[1] + u3[1]
    o = [u1[0] + u3[0], (f - g) * h, u3[1] - u1[1], -(f + g) * h]
    return [a + b for a, b in zip(e, o)] + [a - b for a, b in zip(e, o)]


def put_split(ref, base, re, im):
    rows = pl.ds(base, ROWS)
    for part, value in enumerate((re, im)):
        high = value.astype(jnp.bfloat16)
        low = (value - high.astype(jnp.float32)).astype(jnp.bfloat16)
        at = part * LANES
        ref[rows, at : at + LANES] = high
        ref[rows, 2 * LANES + at : 2 * LANES + at + LANES] = low
        ref[rows, 4 * LANES + at : 4 * LANES + at + LANES] = high


def deconvolve(read, write, wave, floor, fwd_ref, inv_ref, tw_ref, mid_ref, cut_ref, spec_ref):
    half, wide = RADIX // 2, RADIX * RADIX
    for j2 in range(RADIX):
        out = real_eight([read(RADIX * j1 + j2) for j1 in range(RADIX)])
        mid_ref[2 * j2] = out[0]
        mid_ref[2 * j2 + 1] = out[half]
        for a in range(1, half):
            mid_ref[2 * RADIX * a + 2 * j2] = out[a][0]
            mid_ref[2 * RADIX * a + 2 * j2 + 1] = out[a][1]

    def emit(k, value):
        s = SLOT[k]
        c, n = tw_ref[s, 0:1, :], tw_ref[s, 1:2, :]
        put_split(cut_ref, s * ROWS, value[0] * c - value[1] * n, value[0] * n + value[1] * c)

    zero = real_eight([mid_ref[2 * j2] for j2 in range(RADIX)])
    c, n = tw_ref[0, 0:1, :], tw_ref[0, 1:2, :]
    for b in range(half + 1):
        s = SLOT[RADIX * b]
        c, n = tw_ref[s, 0:1, :], tw_ref[s, 1:2, :]
        if b in (0, half):
            put_split(cut_ref, s * ROWS, zero[b] * c, zero[b] * n)
        else:
            emit(RADIX * b, zero[b])
    for a in range(1, half):
        base = 2 * RADIX * a
        items = [turn((mid_ref[base + 2 * j2], mid_ref[base + 2 * j2 + 1]), -a * j2, wide) for j2 in range(RADIX)]
        for b, value in enumerate(fourier(items, -1)):
            emit(a + RADIX * b, value)
    four = [mid_ref[2 * j2 + 1] for j2 in range(RADIX)]
    for b in range(half):
        k = half + RADIX * b
        re, im = four[0], None
        for j2 in range(1, RADIX):
            angle = 2 * math.pi * (k * j2 % wide) / wide
            re = re + four[j2] * math.cos(angle)
            term = four[j2] * -math.sin(angle)
            im = term if im is None else im + term
        emit(k, (re, im))

    for s in range(KEEP):
        re = im = None
        for piece, taps in enumerate(wave):
            c, n = tw_ref[s, 4 + 2 * piece : 5 + 2 * piece, :], tw_ref[s, 5 + 2 * piece : 6 + 2 * piece, :]
            re = taps * c if re is None else re + taps * c
            im = taps * n if im is None else im + taps * n
        put_split(cut_ref, (KEEP + s) * ROWS, re, im)

    spec_ref[...] = jnp.dot(cut_ref[...], fwd_ref[...], preferred_element_type=jnp.float32)

    def apply(s, carry):
        at = pl.multiple_of(s * ROWS, ROWS)
        other = pl.multiple_of((KEEP + s) * ROWS, ROWS)
        xr, xi = spec_ref[pl.ds(at, ROWS), 0:LANES], spec_ref[pl.ds(at, ROWS), LANES:]
        hr, hi = spec_ref[pl.ds(other, ROWS), 0:LANES], spec_ref[pl.ds(other, ROWS), LANES:]
        scale = 1.0 / (hr * hr + hi * hi + floor)
        put_split(cut_ref, at, (xr * hr + xi * hi) * scale, (xi * hr - xr * hi) * scale)
        return carry

    lax.fori_loop(0, KEEP, apply, 0, unroll=3)
    rows = KEEP * ROWS
    spec_ref[0:rows] = jnp.dot(cut_ref[0:rows], inv_ref[...], preferred_element_type=jnp.float32)

    def fetch(k):
        s = SLOT[k]
        re, im = spec_ref[s * ROWS : (s + 1) * ROWS, 0:LANES], spec_ref[s * ROWS : (s + 1) * ROWS, LANES:]
        c, n = tw_ref[s, 2:3, :], tw_ref[s, 3:4, :]
        if k in (0, wide // 2):
            return re * c - im * n
        return (re * c - im * n, re * n + im * c)

    for a in range(1, half):
        base = 2 * RADIX * a
        for j2, value in enumerate(fourier([fetch(a + RADIX * b) for b in range(RADIX)], 1)):
            value = turn(value, a * j2, wide)
            mid_ref[base + 2 * j2] = value[0]
            mid_ref[base + 2 * j2 + 1] = value[1]
    for j2, value in enumerate(eight_real(*[fetch(RADIX * b) for b in range(half + 1)])):
        mid_ref[2 * j2] = value
    four = [fetch(half + RADIX * b) for b in range(half)]
    for j2 in range(RADIX):
        total = None
        for b, value in enumerate(four):
            angle = 2 * math.pi * ((half + RADIX * b) * j2 % wide) / wide
            term = value[0] * math.cos(angle)
            if j2:
                term = term - value[1] * math.sin(angle)
            total = term if total is None else total + term
        mid_ref[2 * j2 + 1] = total
    for j2 in range(RADIX):
        parts = [mid_ref[2 * j2]]
        for a in range(1, half):
            base = 2 * RADIX * a
            parts.append((mid_ref[base + 2 * j2], mid_ref[base + 2 * j2 + 1]))
        parts.append(mid_ref[2 * j2 + 1])
        for j1, value in enumerate(eight_real(*parts)):
            write(RADIX * j1 + j2, value)


def slabs(ref, lead):
    def at(j):
        return lead + (slice(None), slice(j * LANES, (j + 1) * LANES))

    def read(j):
        value = ref[at(j)]
        return value.reshape(ROWS, LANES)

    def write(j, value):
        ref[at(j)] = value.reshape(ref[at(j)].shape)

    return read, write


def block_kernel(taps, lead, x_ref, w_ref, fwd_ref, inv_ref, tw_ref, o_ref, mid_ref, cut_ref, spec_ref):
    read, _ = slabs(x_ref, lead)
    _, write = slabs(o_ref, (slice(None),) * (len(o_ref.shape) - 2))
    wave = [w_ref[:, p * LANES : (p + 1) * LANES] for p in range(taps // LANES)]
    deconvolve(read, write, wave, w_ref[:, taps : taps + LANES], fwd_ref, inv_ref, tw_ref, mid_ref, cut_ref, spec_ref)


def split_count(n):
    inner = 1
    while inner * inner < n:
        inner *= 2
    return (n // inner, inner) if n % inner == 0 else (1, n)


def block_order(n):
    inner = split_count(n)[1]
    raws = list(range(n - inner + 1, n, 2))[:2]
    kept = list(range(n - inner, n, 2))[1::-1]
    near = sorted(range(1, n // 2), key=lambda k: (k < inner, k))
    cross = [k for k in range(n // 2, n) if k not in raws + kept]
    lead, rest = cross[:inner], cross[inner:]
    mixed = lead[:1] + [k for pair in zip(lead[1:], near) for k in pair]
    return mixed + near[max(len(lead) - 1, 0) :] + rest + kept + raws + [0], raws, kept


def keeps_blocks(me, n):
    outer, inner = split_count(n)
    far = lax.div(me, inner)
    return jnp.logical_and(me % 2 == 0, jnp.logical_or(far == outer // 2 - 1, far == outer // 2))


def exchange_kernel(
    n,
    taps,
    x_ref,
    pick_ref,
    wave_ref,
    damp_ref,
    fwd_hbm,
    inv_hbm,
    tw_hbm,
    buf_ref,
    mid_ref,
    cut_ref,
    spec_ref,
    fwd_ref,
    inv_ref,
    tw_ref,
    bank_ref,
    rows_ref,
    stage_ref,
    pick_smem,
    damp_smem,
    stage_sem,
    load_sems,
    near_sems,
    raw_sems,
    pick_sems,
    bank_sends,
    bank_recvs,
    ready_sems,
    sends,
    recvs,
):
    me = lax.axis_index("traces")
    own, each = wave_ref.shape[0], x_ref.shape[0] // n
    outer, inner = split_count(n)
    far, near = lax.div(me, inner), lax.rem(me, inner)
    halves, pieces = own // SUBLANES, taps // LANES
    last = halves * pieces

    def remote(src, dst, send_sem, recv_sem, device):
        return pltpu.make_async_remote_copy(
            src_ref=src,
            dst_ref=dst,
            send_sem=send_sem,
            recv_sem=recv_sem,
            device_id={"traces": device},
            device_id_type=pl.DeviceIdType.MESH,
        )

    def block_of(e):
        return x_ref.at[pl.ds(pl.multiple_of(e * each, each), each)]

    turns, raws, kept = block_order(n)
    partner = me ^ raws[0]
    made = n - 1 - len(raws)
    sent_here = made - jnp.where(keeps_blocks(me, n), len(kept), 0)

    def turn_of(s):
        k = 0
        for i, turn in enumerate(turns):
            k = jnp.where(s == i, turn, k)
        return k

    barrier = pltpu.get_barrier_semaphore()

    def tell(sem, other):
        pl.semaphore_signal(sem, inc=1, device_id={"traces": other}, device_id_type=pl.DeviceIdType.MESH)

    def greet(other, carry):
        tell(barrier, other)
        return carry

    def answer(other, carry):
        @pl.when(other != partner)
        def _():
            tell(ready_sems.at[me], other)

        return carry

    def meet(other, carry):
        @pl.when(other != partner)
        def _():
            pl.semaphore_wait(ready_sems.at[other], 1)

        return carry

    def raw(i, part, here):
        first, count, other = part * (each // 2), each // 2, me ^ raws[i]
        rows = x_ref.at[pl.ds(pl.multiple_of(other * each + first, count), count)]
        there = buf_ref.at[n + jnp.where(here, other, me), pl.ds(first, count)]
        return remote(rows, there, raw_sems.at[0, i, part], raw_sems.at[1, i, part], other)

    def raw_staged():
        there = buf_ref.at[n + me, pl.ds(0, each // 2)]
        return remote(stage_ref, there, raw_sems.at[0, 0, 0], raw_sems.at[1, 0, 0], partner)

    stage = pl.ds(pl.multiple_of(partner * each, each // 2), each // 2)
    stage_in = pltpu.make_async_copy(x_ref.at[stage], stage_ref, stage_sem)

    @pl.when(partner > me)
    def _():
        stage_in.start()

    lax.fori_loop(me + 1, n, greet, 0)

    @pl.when(me > 0)
    def _():
        pl.semaphore_wait(barrier, me)

    @pl.when(partner < me)
    def _():
        tell(ready_sems.at[me], partner)
        raw(0, 0, False).start()

    damp_in = pltpu.make_async_copy(damp_ref, damp_smem, near_sems.at[0])
    pick_in = pltpu.make_async_copy(pick_ref, pick_smem.at[pl.ds(0, n * each)], near_sems.at[1])
    tables_in = [
        pltpu.make_async_copy(there, here, near_sems.at[2 + i])
        for i, (there, here) in enumerate(((fwd_hbm, fwd_ref), (inv_hbm, inv_ref), (tw_hbm, tw_ref)))
    ]
    tiles_in = [
        pltpu.make_async_copy(
            wave_ref.at[pl.ds(h * SUBLANES, SUBLANES), pl.ds(p * LANES, LANES)],
            bank_ref.at[me, h * pieces + p],
            near_sems.at[5 + h * pieces + p],
        )
        for h in range(halves)
        for p in range(pieces)
    ]
    for copy in [damp_in] + tiles_in + [pick_in] + tables_in:
        copy.start()

    def load(e):
        return pltpu.make_async_copy(block_of(e), buf_ref.at[n + e], load_sems.at[e])

    def load_start(s, carry):
        @pl.when(jnp.logical_or(s < made, s == n - 1))
        def _():
            load(me ^ turn_of(s)).start()

        return carry

    def picks(i):
        count = n * each
        there = pick_smem.at[pl.ds((1 + i) * count, count)]
        return remote(pick_ref, there, pick_sems.at[0, i], pick_sems.at[1, i], me ^ raws[i])

    @pl.when(partner > me)
    def _():
        stage_in.wait()
        pl.semaphore_wait(ready_sems.at[partner], 1)
        raw_staged().start()

    lax.fori_loop(0, me, answer, 0)
    damp_in.wait()
    lane = lax.broadcasted_iota(jnp.int32, (SUBLANES, LANES), 1)
    levels = jnp.zeros((SUBLANES, LANES), jnp.float32)
    for f in range(own):
        levels = jnp.where(lane == f, damp_smem[f], levels)
    bank_ref[me, last] = levels
    lax.fori_loop(me + 1, n, meet, 0)
    for copy in tiles_in:
        copy.wait()

    def bank_copy(block, slot, there):
        return remote(bank_ref.at[block], bank_ref.at[block], bank_sends.at[slot], bank_recvs.at[block], there)

    def block_at(f):
        return f * inner + near

    middle = outer // 2
    upper = far >= middle
    gate = jnp.where(upper, middle, middle - 1)

    def across(t, act):
        there = lax.rem(far + t, outer)
        direct = jnp.logical_or((there >= middle) == upper, there == outer - 1 - gate)

        @pl.when(direct)
        def _():
            act(bank_copy(me, t - 1, block_at(there)))

    def onward(t, act):
        block = lax.rem(far + t, outer)
        for there in range(outer):
            slot = outer - 1 + (t - 1) * outer + there
            near_side = (there >= middle) == upper
            foreign = (block >= middle) != upper
            go = jnp.logical_and(jnp.logical_and(far == gate, far != there), jnp.logical_and(near_side, foreign))

            @pl.when(go)
            def _():
                act(bank_copy(block_at(block), slot, block_at(there)))

    def spread(f, act):
        for d in range(1, inner):
            slot = outer * outer - 1 + f * (inner - 1) + d - 1
            act(bank_copy(block_at(f), slot, far * inner + (near ^ d)))

    def bank_came(block):
        bank_copy(block, 0, partner).wait_recv()

    start, sent = (lambda copy: copy.start()), (lambda copy: copy.wait_send())
    for t in range(1, outer):
        across(t, start)
    spread(far, start)
    raw(0, 1, False).start()
    for i in range(1, len(raws)):
        raw(i, 0, False).start()
        raw(i, 1, False).start()
    for i in range(len(raws)):
        picks(i).start()
    lax.fori_loop(0, n, load_start, 0)
    for t in range(1, outer):
        block = lax.rem(far + t, outer)
        bank_came(block_at(block))
        onward(t, start)
        spread(block, start)
    for f in range(outer):
        for d in range(1, inner):
            bank_came(f * inner + (near ^ d))
    pick_in.wait()
    for copy in tables_in:
        copy.wait()

    def send(e):
        return remote(buf_ref.at[n + e], buf_ref.at[me], sends.at[e], recvs.at[me], e)

    row_lane = lax.broadcasted_iota(jnp.int32, (1, LANES), 1)

    def step(s, carry):
        e = me ^ turn_of(s)
        theirs = jnp.logical_and(s >= made, s < n - 1)
        for i in range(len(raws)):

            @pl.when(s == made + i)
            def _():
                raw(i, 0, True).wait_recv()
                raw(i, 1, True).wait_recv()
                picks(i).wait_recv()

        @pl.when(jnp.logical_not(theirs))
        def _():
            load(e).wait()

        table = jnp.where(theirs, s - made + 1, 0)
        base = (table * n + jnp.where(theirs, me, e)) * each
        for r in range(ROWS):
            pick = pick_smem[base + r]
            block, inside = lax.div(pick, own), lax.rem(pick, own)
            tile, sub = lax.div(inside, SUBLANES) * pieces, lax.rem(inside, SUBLANES)
            for p in range(pieces):
                rows_ref[r : r + 1, p * LANES : (p + 1) * LANES] = bank_ref[block, tile + p, pl.ds(sub, 1), :]
            level = bank_ref[block, last, 0:1, :]
            rows_ref[r : r + 1, taps : taps + LANES] = jnp.where(row_lane == inside, level, 0.0)

        @pl.when(jnp.logical_and(s >= 1, s <= sent_here))
        def _():
            send(me ^ turn_of(s - 1)).start()

        slot = jnp.where(s >= made, e, n + e)
        wave = [rows_ref[:, p * LANES : (p + 1) * LANES] for p in range(pieces)]
        power = sum(jnp.sum(w * w, axis=1, keepdims=True) for w in wave)
        damp = jnp.sum(rows_ref[:, taps : taps + LANES], axis=1, keepdims=True)
        floor = jnp.broadcast_to(damp * (power + 1e-6), (ROWS, LANES))

        def read(j):
            return buf_ref[n + e, :, j * LANES : (j + 1) * LANES]

        def write(j, value):
            buf_ref[slot, :, j * LANES : (j + 1) * LANES] = value

        deconvolve(read, write, wave, floor, fwd_ref, inv_ref, tw_ref, mid_ref, cut_ref, spec_ref)
        return carry

    lax.fori_loop(0, n, step, 0)

    for i in range(len(raws)):
        raw(i, 0, False).wait_send()
        raw(i, 1, False).wait_send()
        picks(i).wait_send()
    for t in range(1, outer):
        across(t, sent)
        onward(t, sent)
    for f in range(outer):
        spread(f, sent)

    def finish(s, carry):
        e = me ^ turn_of(s)
        send(e).wait_send()
        remote(buf_ref.at[e], buf_ref.at[e], sends.at[e], recvs.at[e], e).wait_recv()
        return carry

    lax.fori_loop(0, sent_here, finish, 0)


def late_kernel(n, buf_ref, after_ref, late_ref, sends, recvs):
    del after_ref
    me = lax.axis_index("traces")
    kept = block_order(n)[2]

    @pl.when(keeps_blocks(me, n))
    def _():
        barrier = pltpu.get_barrier_semaphore()
        for k in kept:
            pl.semaphore_signal(barrier, inc=1, device_id={"traces": me ^ k}, device_id_type=pl.DeviceIdType.MESH)
        pl.semaphore_wait(barrier, len(kept))
        copies = [
            pltpu.make_async_remote_copy(
                src_ref=buf_ref.at[n + (me ^ k)],
                dst_ref=late_ref.at[i],
                send_sem=sends.at[i],
                recv_sem=recvs.at[i],
                device_id={"traces": me ^ k},
                device_id_type=pl.DeviceIdType.MESH,
            )
            for i, k in enumerate(kept)
        ]
        for copy in copies:
            copy.start()
        for copy in copies:
            copy.wait()


def settle_kernel(n, order_ref, came_ref, o_ref, late_rows_ref, sem):
    rows = o_ref.shape[0]
    each = rows // n
    shift = n.bit_length() - 1
    me = lax.axis_index("traces")
    kept = block_order(n)[2]
    keeps = keeps_blocks(me, n)

    def put(d, carry):
        for r in range(each):
            q = d * each + r
            place = order_ref[q]
            source, row = place & (n - 1), place >> shift
            turn = source ^ me
            late = jnp.logical_and(keeps, functools.reduce(jnp.logical_or, [turn == k for k in kept]))

            @pl.when(late)
            def _():
                index = functools.reduce(lambda at, ik: jnp.where(turn == ik[1], ik[0], at), enumerate(kept), 0)
                late_rows_ref[index * each + row] = q

            @pl.when(jnp.logical_not(late))
            def _():
                pltpu.make_async_copy(came_ref.at[source, pl.ds(row, 1)], o_ref.at[pl.ds(q, 1)], sem).start()

        return carry

    lax.fori_loop(0, n, put, 0)

    def finish(count):
        pltpu.make_async_copy(o_ref.at[pl.ds(0, count)], o_ref.at[pl.ds(0, count)], sem).wait()

    @pl.when(keeps)
    def _():
        finish(rows - len(kept) * each)

    @pl.when(jnp.logical_not(keeps))
    def _():
        finish(rows)


def last_kernel(n, late_rows_ref, late_ref, settled_ref, o_ref, sem):
    del settled_ref
    count, each, _ = late_ref.shape

    @pl.when(keeps_blocks(lax.axis_index("traces"), n))
    def _():
        for i in range(count):
            for r in range(each):
                q = late_rows_ref[i * each + r]
                pltpu.make_async_copy(late_ref.at[i, pl.ds(r, 1)], o_ref.at[pl.ds(q, 1)], sem).start()
        part = o_ref.at[pl.ds(0, count * each)]
        pltpu.make_async_copy(part, part, sem).wait()


def tables(length, taps):
    return (
        jnp.asarray(lane_matrix(-1.0, 1.0)),
        jnp.asarray(lane_matrix(1.0, 1.0 / length)),
        jnp.asarray(twiddles(length, taps)),
    )


def scratch():
    return [
        pltpu.VMEM((RADIX * RADIX, ROWS, LANES), jnp.float32),
        pltpu.VMEM((2 * KEEP * ROWS, 6 * LANES), jnp.bfloat16),
        pltpu.VMEM((2 * KEEP * ROWS, 2 * LANES), jnp.float32),
    ]


def gathered(raw_traces, filter_index, channel_order, wavelets, damping):
    rows, length = raw_traces.shape
    own, taps = wavelets.shape
    n = lax.axis_size("traces")
    me = lax.axis_index("traces")
    each = rows // n
    floor = damping * (jnp.sum(wavelets * wavelets, axis=1) + 1e-6)
    picks = filter_index.reshape(own, rows // own).astype(jnp.float32)
    packed = lax.all_gather(jnp.concatenate([wavelets, floor[:, None], picks], axis=1), "traces", axis=0, tiled=True)
    all_picks = packed[:, taps + 1 :].reshape(n, n, each).astype(jnp.int32)
    came_picks = lax.dynamic_index_in_dim(all_picks, me, 1, keepdims=False)
    bank = jnp.concatenate([packed[:, :taps], jnp.broadcast_to(packed[:, taps : taps + 1], (own * n, LANES))], axis=1)
    fwd, inv, tw = tables(length, taps)
    whole = lambda a: pl.BlockSpec(a.shape, lambda i, *_: (0,) * a.ndim)
    fixed = [pl.BlockSpec((ROWS, taps + LANES), lambda i, *_: (i, 0)), whole(fwd), whole(inv), whole(tw)]
    came = lax.all_to_all(raw_traces.reshape(n, each, length), "traces", 0, 0, tiled=True).reshape(rows, length)
    result = pl.pallas_call(
        functools.partial(block_kernel, taps, ()),
        grid=(rows // ROWS,),
        out_shape=jax.ShapeDtypeStruct((rows, length), jnp.float32),
        in_specs=[pl.BlockSpec((ROWS, length), lambda i: (i, 0))] + fixed,
        out_specs=pl.BlockSpec((ROWS, length), lambda i: (i, 0)),
        scratch_shapes=scratch(),
        compiler_params=pltpu.CompilerParams(vmem_limit_bytes=48 * 1024 * 1024),
    )(came, jnp.take(bank, came_picks.reshape(-1), axis=0), fwd, inv, tw)
    return jnp.take(result, (channel_order % n) * each + channel_order // n, axis=0)


def local(raw_traces, filter_index, channel_order, wavelets, damping):
    rows, length = raw_traces.shape
    own, taps = wavelets.shape
    n = lax.axis_size("traces")
    if n < 4 or n & (n - 1) or rows != n * ROWS or own % SUBLANES or own > LANES or taps % LANES:
        return gathered(raw_traces, filter_index, channel_order, wavelets, damping)

    fwd, inv, tw = tables(length, taps)
    tiles = own // SUBLANES * (taps // LANES)
    outer = split_count(n)[0]
    _, raws, kept = block_order(n)
    raws, kept = len(raws), len(kept)
    dma = pltpu.SemaphoreType.DMA
    came = pl.pallas_call(
        functools.partial(exchange_kernel, n, taps),
        in_specs=[pl.BlockSpec(memory_space=pltpu.HBM)] * 7,
        out_specs=pl.BlockSpec(memory_space=pltpu.VMEM),
        out_shape=pltpu.VMEM((2 * n, ROWS, length), jnp.float32),
        scratch_shapes=scratch()
        + [pltpu.VMEM(a.shape, a.dtype) for a in (fwd, inv, tw)]
        + [
            pltpu.VMEM((n, tiles + 1, SUBLANES, LANES), jnp.float32),
            pltpu.VMEM((ROWS, taps + LANES), jnp.float32),
            pltpu.VMEM((ROWS // 2, length), jnp.float32),
            pltpu.SMEM(((1 + raws) * rows,), jnp.int32),
            pltpu.SMEM((own,), jnp.float32),
            dma,
            dma((n,)),
            dma((5 + tiles,)),
            dma((2, raws, 2)),
            dma((2, raws)),
            dma((outer * outer - 1 + n - outer,)),
            dma((n,)),
            pltpu.SemaphoreType.REGULAR((n,)),
            dma((n,)),
            dma((n,)),
        ],
        compiler_params=pltpu.CompilerParams(
            collective_id=0, has_side_effects=True, vmem_limit_bytes=40 * 1024 * 1024
        ),
        cost_estimate=pl.CostEstimate(flops=rows * length * 1500, bytes_accessed=8 * rows * length, transcendentals=0),
    )(raw_traces, filter_index, wavelets, damping, fwd, inv, tw)
    came = pltpu.with_memory_space_constraint(came, pltpu.VMEM)
    smem, vmem, hbm = (pl.BlockSpec(memory_space=m) for m in (pltpu.SMEM, pltpu.VMEM, pltpu.HBM))
    params = pltpu.CompilerParams(vmem_limit_bytes=20 * 1024 * 1024)
    settled, late_rows = pl.pallas_call(
        functools.partial(settle_kernel, n),
        in_specs=[smem, vmem],
        out_specs=[hbm, smem],
        out_shape=[
            jax.ShapeDtypeStruct((rows, length), jnp.float32),
            jax.ShapeDtypeStruct((kept * ROWS,), jnp.int32),
        ],
        scratch_shapes=[dma],
        compiler_params=params,
    )(channel_order, came)
    late = pl.pallas_call(
        functools.partial(late_kernel, n),
        in_specs=[vmem, pl.BlockSpec(memory_space=pl.ANY)],
        out_specs=vmem,
        out_shape=pltpu.VMEM((kept, ROWS, length), jnp.float32),
        scratch_shapes=[dma((kept,)), dma((kept,))],
        compiler_params=pltpu.CompilerParams(
            collective_id=1, has_side_effects=True, vmem_limit_bytes=20 * 1024 * 1024
        ),
    )(came, late_rows)
    late = pltpu.with_memory_space_constraint(late, pltpu.VMEM)
    return pl.pallas_call(
        functools.partial(last_kernel, n),
        in_specs=[smem, vmem, hbm],
        out_specs=hbm,
        out_shape=jax.ShapeDtypeStruct((rows, length), jnp.float32),
        scratch_shapes=[dma],
        input_output_aliases={2: 0},
        compiler_params=params,
    )(late_rows, late, settled)


def solution(mesh):
    placed = (
        P(("groups", "traces"), None),
        P(("groups", "traces")),
        P("groups"),
        P("traces", None),
        P("traces"),
    )
    return jax.shard_map(
        local, mesh=mesh, in_specs=placed, out_specs=P(("groups", "traces"), None), check_vma=False
    )
```

```python
import functools
import math

import jax
import jax.numpy as jnp
import numpy as np
from jax import lax
from jax.experimental import pallas as pl
from jax.experimental.pallas import tpu as pltpu
from jax.sharding import PartitionSpec as P

LANES = 128
RADIX = 8
ROWS = 16
SUBLANES = 8

KEPT = (
    [RADIX * b for b in range(RADIX // 2 + 1)]
    + [a + RADIX * b for a in range(1, RADIX // 2) for b in range(RADIX)]
    + [RADIX // 2 + RADIX * b for b in range(RADIX // 2)]
)
SLOT = {k: s for s, k in enumerate(KEPT)}
KEEP = len(KEPT)


def lane_matrix(sign, scale):
    ids = np.arange(LANES)
    angle = 2.0 * np.pi * (np.outer(ids, ids) % LANES) / LANES
    c, s = np.cos(angle) * scale, sign * np.sin(angle) * scale
    full = np.block([[c, s], [-s, c]])
    import ml_dtypes

    high = full.astype(np.float32).astype(ml_dtypes.bfloat16)
    low = (full.astype(np.float32) - high.astype(np.float32)).astype(ml_dtypes.bfloat16)
    return np.concatenate([high, high, low], axis=0)


def twiddles(length, taps):
    m = np.arange(LANES)
    rows = []
    for k in KEPT:
        angle = 2.0 * np.pi * k * m / length
        row = [np.cos(angle), -np.sin(angle)]
        weight = 1.0 if k in (0, RADIX * RADIX // 2) else 2.0
        row += [weight * np.cos(angle), weight * np.sin(angle)]
        for piece in range(taps // LANES):
            shifted = 2.0 * np.pi * k * (m + LANES * piece) / length
            row += [np.cos(shifted), -np.sin(shifted)]
        rows.append(np.stack(row))
    return np.stack(rows).astype(np.float32)


def cadd(a, b):
    return (a[0] + b[0], a[1] + b[1])


def csub(a, b):
    return (a[0] - b[0], a[1] - b[1])


def turn(a, num, den):
    num %= den
    if num == 0:
        return a
    if 4 * num == den:
        return (-a[1], a[0])
    if 2 * num == den:
        return (-a[0], -a[1])
    if 4 * num == 3 * den:
        return (a[1], -a[0])
    c, s = math.cos(2 * math.pi * num / den), math.sin(2 * math.pi * num / den)
    return (a[0] * c - a[1] * s, a[0] * s + a[1] * c)


def fourier(items, sign):
    n = len(items)
    if n == 1:
        return items
    even, odd = fourier(items[0::2], sign), fourier(items[1::2], sign)
    turned = [turn(o, sign * k, n) for k, o in enumerate(odd)]
    return [cadd(e, t) for e, t in zip(even, turned)] + [csub(e, t) for e, t in zip(even, turned)]


def real_eight(v):
    h = math.sqrt(0.5)
    s0, d0, s1, d1 = v[0] + v[4], v[0] - v[4], v[1] + v[5], v[1] - v[5]
    s2, d2, s3, d3 = v[2] + v[6], v[2] - v[6], v[3] + v[7], v[3] - v[7]
    p, q = s0 + s2, s1 + s3
    r, t = (d1 - d3) * h, (d1 + d3) * h
    return [p + q, (d0 + r, -(d2 + t)), (s0 - s2, s3 - s1), (d0 - r, d2 - t), p - q]


def eight_real(u0, u1, u2, u3, u4):
    h = math.sqrt(0.5)
    p, q = u0 + u4, u0 - u4
    e = [p + u2[0], q - u2[1], p - u2[0], q + u2[1]]
    f, g = u1[0] - u3[0], u1[1] + u3[1]
    o = [u1[0] + u3[0], (f - g) * h, u3[1] - u1[1], -(f + g) * h]
    return [a + b for a, b in zip(e, o)] + [a - b for a, b in zip(e, o)]


def put_split(ref, base, re, im):
    rows = pl.ds(base, ROWS)
    for part, value in enumerate((re, im)):
        high = value.astype(jnp.bfloat16)
        low = (value - high.astype(jnp.float32)).astype(jnp.bfloat16)
        at = part * LANES
        ref[rows, at : at + LANES] = high
        ref[rows, 2 * LANES + at : 2 * LANES + at + LANES] = low
        ref[rows, 4 * LANES + at : 4 * LANES + at + LANES] = high


def deconvolve(read, write, wave, floor, fwd_ref, inv_ref, tw_ref, mid_ref, cut_ref, spec_ref):
    half, wide = RADIX // 2, RADIX * RADIX
    for j2 in range(RADIX):
        out = real_eight([read(RADIX * j1 + j2) for j1 in range(RADIX)])
        mid_ref[2 * j2] = out[0]
        mid_ref[2 * j2 + 1] = out[half]
        for a in range(1, half):
            mid_ref[2 * RADIX * a + 2 * j2] = out[a][0]
            mid_ref[2 * RADIX * a + 2 * j2 + 1] = out[a][1]

    def emit(k, value):
        s = SLOT[k]
        c, n = tw_ref[s, 0:1, :], tw_ref[s, 1:2, :]
        put_split(cut_ref, s * ROWS, value[0] * c - value[1] * n, value[0] * n + value[1] * c)

    zero = real_eight([mid_ref[2 * j2] for j2 in range(RADIX)])
    c, n = tw_ref[0, 0:1, :], tw_ref[0, 1:2, :]
    for b in range(half + 1):
        s = SLOT[RADIX * b]
        c, n = tw_ref[s, 0:1, :], tw_ref[s, 1:2, :]
        if b in (0, half):
            put_split(cut_ref, s * ROWS, zero[b] * c, zero[b] * n)
        else:
            emit(RADIX * b, zero[b])
    for a in range(1, half):
        base = 2 * RADIX * a
        items = [turn((mid_ref[base + 2 * j2], mid_ref[base + 2 * j2 + 1]), -a * j2, wide) for j2 in range(RADIX)]
        for b, value in enumerate(fourier(items, -1)):
            emit(a + RADIX * b, value)
    four = [mid_ref[2 * j2 + 1] for j2 in range(RADIX)]
    for b in range(half):
        k = half + RADIX * b
        re, im = four[0], None
        for j2 in range(1, RADIX):
            angle = 2 * math.pi * (k * j2 % wide) / wide
            re = re + four[j2] * math.cos(angle)
            term = four[j2] * -math.sin(angle)
            im = term if im is None else im + term
        emit(k, (re, im))

    for s in range(KEEP):
        re = im = None
        for piece, taps in enumerate(wave):
            c, n = tw_ref[s, 4 + 2 * piece : 5 + 2 * piece, :], tw_ref[s, 5 + 2 * piece : 6 + 2 * piece, :]
            re = taps * c if re is None else re + taps * c
            im = taps * n if im is None else im + taps * n
        put_split(cut_ref, (KEEP + s) * ROWS, re, im)

    spec_ref[...] = jnp.dot(cut_ref[...], fwd_ref[...], preferred_element_type=jnp.float32)

    def apply(s, carry):
        at = pl.multiple_of(s * ROWS, ROWS)
        other = pl.multiple_of((KEEP + s) * ROWS, ROWS)
        xr, xi = spec_ref[pl.ds(at, ROWS), 0:LANES], spec_ref[pl.ds(at, ROWS), LANES:]
        hr, hi = spec_ref[pl.ds(other, ROWS), 0:LANES], spec_ref[pl.ds(other, ROWS), LANES:]
        scale = 1.0 / (hr * hr + hi * hi + floor)
        put_split(cut_ref, at, (xr * hr + xi * hi) * scale, (xi * hr - xr * hi) * scale)
        return carry

    lax.fori_loop(0, KEEP, apply, 0, unroll=3)
    rows = KEEP * ROWS
    spec_ref[0:rows] = jnp.dot(cut_ref[0:rows], inv_ref[...], preferred_element_type=jnp.float32)

    def fetch(k):
        s = SLOT[k]
        re, im = spec_ref[s * ROWS : (s + 1) * ROWS, 0:LANES], spec_ref[s * ROWS : (s + 1) * ROWS, LANES:]
        c, n = tw_ref[s, 2:3, :], tw_ref[s, 3:4, :]
        if k in (0, wide // 2):
            return re * c - im * n
        return (re * c - im * n, re * n + im * c)

    for a in range(1, half):
        base = 2 * RADIX * a
        for j2, value in enumerate(fourier([fetch(a + RADIX * b) for b in range(RADIX)], 1)):
            value = turn(value, a * j2, wide)
            mid_ref[base + 2 * j2] = value[0]
            mid_ref[base + 2 * j2 + 1] = value[1]
    for j2, value in enumerate(eight_real(*[fetch(RADIX * b) for b in range(half + 1)])):
        mid_ref[2 * j2] = value
    four = [fetch(half + RADIX * b) for b in range(half)]
    for j2 in range(RADIX):
        total = None
        for b, value in enumerate(four):
            angle = 2 * math.pi * ((half + RADIX * b) * j2 % wide) / wide
            term = value[0] * math.cos(angle)
            if j2:
                term = term - value[1] * math.sin(angle)
            total = term if total is None else total + term
        mid_ref[2 * j2 + 1] = total
    for j2 in range(RADIX):
        parts = [mid_ref[2 * j2]]
        for a in range(1, half):
            base = 2 * RADIX * a
            parts.append((mid_ref[base + 2 * j2], mid_ref[base + 2 * j2 + 1]))
        parts.append(mid_ref[2 * j2 + 1])
        for j1, value in enumerate(eight_real(*parts)):
            write(RADIX * j1 + j2, value)


def slabs(ref, lead):
    def at(j):
        return lead + (slice(None), slice(j * LANES, (j + 1) * LANES))

    def read(j):
        value = ref[at(j)]
        return value.reshape(ROWS, LANES)

    def write(j, value):
        ref[at(j)] = value.reshape(ref[at(j)].shape)

    return read, write


def block_kernel(taps, lead, x_ref, w_ref, fwd_ref, inv_ref, tw_ref, o_ref, mid_ref, cut_ref, spec_ref):
    read, _ = slabs(x_ref, lead)
    _, write = slabs(o_ref, (slice(None),) * (len(o_ref.shape) - 2))
    wave = [w_ref[:, p * LANES : (p + 1) * LANES] for p in range(taps // LANES)]
    deconvolve(read, write, wave, w_ref[:, taps : taps + LANES], fwd_ref, inv_ref, tw_ref, mid_ref, cut_ref, spec_ref)


def split_count(n):
    inner = 1
    while inner * inner < n:
        inner *= 2
    return (n // inner, inner) if n % inner == 0 else (1, n)


def block_order(n):
    inner = split_count(n)[1]
    raws = list(range(n - inner + 1, n, 2))[:2]
    kept = list(range(n - inner, n, 2))[1::-1]
    near = sorted(range(1, n // 2), key=lambda k: (k < inner, k))
    cross = [k for k in range(n // 2, n) if k not in raws + kept]
    lead, rest = cross[:inner], cross[inner:]
    mixed = lead[:1] + [k for pair in zip(lead[1:], near) for k in pair]
    return mixed + near[max(len(lead) - 1, 0) :] + rest + kept + raws + [0], raws, kept


def keeps_blocks(me, n):
    outer, inner = split_count(n)
    far = lax.div(me, inner)
    return jnp.logical_and(me % 2 == 0, jnp.logical_or(far == outer // 2 - 1, far == outer // 2))


def exchange_kernel(
    n,
    taps,
    x_ref,
    pick_ref,
    wave_ref,
    damp_ref,
    fwd_hbm,
    inv_hbm,
    tw_hbm,
    buf_ref,
    mid_ref,
    cut_ref,
    spec_ref,
    fwd_ref,
    inv_ref,
    tw_ref,
    bank_ref,
    rows_ref,
    stage_ref,
    pick_smem,
    damp_smem,
    stage_sem,
    load_sems,
    near_sems,
    raw_sems,
    pick_sems,
    bank_sends,
    bank_recvs,
    ready_sems,
    sends,
    recvs,
):
    me = lax.axis_index("traces")
    own, each = wave_ref.shape[0], x_ref.shape[0] // n
    outer, inner = split_count(n)
    far, near = lax.div(me, inner), lax.rem(me, inner)
    halves, pieces = own // SUBLANES, taps // LANES
    last = halves * pieces

    def remote(src, dst, send_sem, recv_sem, device):
        return pltpu.make_async_remote_copy(
            src_ref=src,
            dst_ref=dst,
            send_sem=send_sem,
            recv_sem=recv_sem,
            device_id={"traces": device},
            device_id_type=pl.DeviceIdType.MESH,
        )

    def block_of(e):
        return x_ref.at[pl.ds(pl.multiple_of(e * each, each), each)]

    turns, raws, kept = block_order(n)
    partner = me ^ raws[0]
    made = n - 1 - len(raws)
    sent_here = made - jnp.where(keeps_blocks(me, n), len(kept), 0)

    def turn_of(s):
        k = 0
        for i, turn in enumerate(turns):
            k = jnp.where(s == i, turn, k)
        return k

    barrier = pltpu.get_barrier_semaphore()

    def tell(sem, other):
        pl.semaphore_signal(sem, inc=1, device_id={"traces": other}, device_id_type=pl.DeviceIdType.MESH)

    def greet(other, carry):
        tell(barrier, other)
        return carry

    def answer(other, carry):
        @pl.when(other != partner)
        def _():
            tell(ready_sems.at[me], other)

        return carry

    def meet(other, carry):
        @pl.when(other != partner)
        def _():
            pl.semaphore_wait(ready_sems.at[other], 1)

        return carry

    def raw(i, part, here):
        first, count, other = part * (each // 2), each // 2, me ^ raws[i]
        rows = x_ref.at[pl.ds(pl.multiple_of(other * each + first, count), count)]
        there = buf_ref.at[n + jnp.where(here, other, me), pl.ds(first, count)]
        return remote(rows, there, raw_sems.at[0, i, part], raw_sems.at[1, i, part], other)

    def raw_staged():
        there = buf_ref.at[n + me, pl.ds(0, each // 2)]
        return remote(stage_ref, there, raw_sems.at[0, 0, 0], raw_sems.at[1, 0, 0], partner)

    stage = pl.ds(pl.multiple_of(partner * each, each // 2), each // 2)
    stage_in = pltpu.make_async_copy(x_ref.at[stage], stage_ref, stage_sem)

    @pl.when(partner > me)
    def _():
        stage_in.start()

    lax.fori_loop(me + 1, n, greet, 0)

    @pl.when(me > 0)
    def _():
        pl.semaphore_wait(barrier, me)

    @pl.when(partner < me)
    def _():
        tell(ready_sems.at[me], partner)
        raw(0, 0, False).start()

    damp_in = pltpu.make_async_copy(damp_ref, damp_smem, near_sems.at[0])
    pick_in = pltpu.make_async_copy(pick_ref, pick_smem.at[pl.ds(0, n * each)], near_sems.at[1])
    tables_in = [
        pltpu.make_async_copy(there, here, near_sems.at[2 + i])
        for i, (there, here) in enumerate(((fwd_hbm, fwd_ref), (inv_hbm, inv_ref), (tw_hbm, tw_ref)))
    ]
    tiles_in = [
        pltpu.make_async_copy(
            wave_ref.at[pl.ds(h * SUBLANES, SUBLANES), pl.ds(p * LANES, LANES)],
            bank_ref.at[me, pl.ds((h * pieces + p) * SUBLANES, SUBLANES)],
            near_sems.at[5 + h * pieces + p],
        )
        for h in range(halves)
        for p in range(pieces)
    ]
    for copy in [damp_in] + tiles_in + [pick_in] + tables_in:
        copy.start()

    def load(e):
        return pltpu.make_async_copy(block_of(e), buf_ref.at[n + e], load_sems.at[e])

    def load_start(s, carry):
        @pl.when(jnp.logical_or(s < made, s == n - 1))
        def _():
            load(me ^ turn_of(s)).start()

        return carry

    def picks(i):
        count = n * each
        there = pick_smem.at[pl.ds((1 + i) * count, count)]
        return remote(pick_ref, there, pick_sems.at[0, i], pick_sems.at[1, i], me ^ raws[i])

    @pl.when(partner > me)
    def _():
        stage_in.wait()
        pl.semaphore_wait(ready_sems.at[partner], 1)
        raw_staged().start()

    lax.fori_loop(0, me, answer, 0)
    damp_in.wait()
    lane = lax.broadcasted_iota(jnp.int32, (SUBLANES, LANES), 1)
    levels = jnp.zeros((SUBLANES, LANES), jnp.float32)
    for f in range(own):
        levels = jnp.where(lane == f, damp_smem[f], levels)
    bank_ref[me, last * SUBLANES : (last + 1) * SUBLANES, :] = levels
    lax.fori_loop(me + 1, n, meet, 0)
    for copy in tiles_in:
        copy.wait()

    def bank_copy(block, slot, there):
        used = bank_ref.at[block, pl.ds(0, last * SUBLANES + 1)]
        return remote(used, used, bank_sends.at[slot], bank_recvs.at[block], there)

    def block_at(f):
        return f * inner + near

    middle = outer // 2
    upper = far >= middle
    gate = jnp.where(upper, middle, middle - 1)

    def across(t, act):
        there = lax.rem(far + t, outer)
        direct = jnp.logical_or((there >= middle) == upper, there == outer - 1 - gate)

        @pl.when(direct)
        def _():
            act(bank_copy(me, t - 1, block_at(there)))

    def onward(t, act):
        block = lax.rem(far + t, outer)
        for there in range(outer):
            slot = outer - 1 + (t - 1) * outer + there
            near_side = (there >= middle) == upper
            foreign = (block >= middle) != upper
            go = jnp.logical_and(jnp.logical_and(far == gate, far != there), jnp.logical_and(near_side, foreign))

            @pl.when(go)
            def _():
                act(bank_copy(block_at(block), slot, block_at(there)))

    def spread(f, act):
        for d in range(1, inner):
            slot = outer * outer - 1 + f * (inner - 1) + d - 1
            act(bank_copy(block_at(f), slot, far * inner + (near ^ d)))

    def bank_came(block):
        bank_copy(block, 0, partner).wait_recv()

    start, sent = (lambda copy: copy.start()), (lambda copy: copy.wait_send())
    for t in range(1, outer):
        across(t, start)
    spread(far, start)
    raw(0, 1, False).start()
    for i in range(1, len(raws)):
        raw(i, 0, False).start()
        raw(i, 1, False).start()
    for i in range(len(raws)):
        picks(i).start()
    lax.fori_loop(0, n, load_start, 0)
    for t in range(1, outer):
        block = lax.rem(far + t, outer)
        bank_came(block_at(block))
        onward(t, start)
        spread(block, start)
    for f in range(outer):
        for d in range(1, inner):
            bank_came(f * inner + (near ^ d))
    pick_in.wait()
    for copy in tables_in:
        copy.wait()

    def send(e):
        return remote(buf_ref.at[n + e], buf_ref.at[me], sends.at[e], recvs.at[me], e)

    row_lane = lax.broadcasted_iota(jnp.int32, (1, LANES), 1)

    def step(s, carry):
        e = me ^ turn_of(s)
        theirs = jnp.logical_and(s >= made, s < n - 1)
        for i in range(len(raws)):

            @pl.when(s == made + i)
            def _():
                raw(i, 0, True).wait_recv()
                raw(i, 1, True).wait_recv()
                picks(i).wait_recv()

        @pl.when(jnp.logical_not(theirs))
        def _():
            load(e).wait()

        table = jnp.where(theirs, s - made + 1, 0)
        base = (table * n + jnp.where(theirs, me, e)) * each
        for r in range(ROWS):
            pick = pick_smem[base + r]
            block, inside = lax.div(pick, own), lax.rem(pick, own)
            at = lax.div(inside, SUBLANES) * (pieces * SUBLANES) + lax.rem(inside, SUBLANES)
            for p in range(pieces):
                rows_ref[r : r + 1, p * LANES : (p + 1) * LANES] = bank_ref[block, pl.ds(at + p * SUBLANES, 1), :]
            level = bank_ref[block, last * SUBLANES : last * SUBLANES + 1, :]
            rows_ref[r : r + 1, taps : taps + LANES] = jnp.where(row_lane == inside, level, 0.0)

        @pl.when(jnp.logical_and(s >= 1, s <= sent_here))
        def _():
            send(me ^ turn_of(s - 1)).start()

        slot = jnp.where(s >= made, e, n + e)
        wave = [rows_ref[:, p * LANES : (p + 1) * LANES] for p in range(pieces)]
        power = sum(jnp.sum(w * w, axis=1, keepdims=True) for w in wave)
        damp = jnp.sum(rows_ref[:, taps : taps + LANES], axis=1, keepdims=True)
        floor = jnp.broadcast_to(damp * (power + 1e-6), (ROWS, LANES))

        def read(j):
            return buf_ref[n + e, :, j * LANES : (j + 1) * LANES]

        def write(j, value):
            buf_ref[slot, :, j * LANES : (j + 1) * LANES] = value

        deconvolve(read, write, wave, floor, fwd_ref, inv_ref, tw_ref, mid_ref, cut_ref, spec_ref)
        return carry

    lax.fori_loop(0, n, step, 0)

    for i in range(len(raws)):
        raw(i, 0, False).wait_send()
        raw(i, 1, False).wait_send()
        picks(i).wait_send()
    for t in range(1, outer):
        across(t, sent)
        onward(t, sent)
    for f in range(outer):
        spread(f, sent)

    def finish(s, carry):
        e = me ^ turn_of(s)
        send(e).wait_send()
        remote(buf_ref.at[e], buf_ref.at[e], sends.at[e], recvs.at[e], e).wait_recv()
        return carry

    lax.fori_loop(0, sent_here, finish, 0)


def late_kernel(n, buf_ref, after_ref, late_ref, sends, recvs):
    del after_ref
    me = lax.axis_index("traces")
    kept = block_order(n)[2]

    @pl.when(keeps_blocks(me, n))
    def _():
        barrier = pltpu.get_barrier_semaphore()
        for k in kept:
            pl.semaphore_signal(barrier, inc=1, device_id={"traces": me ^ k}, device_id_type=pl.DeviceIdType.MESH)
        pl.semaphore_wait(barrier, len(kept))
        copies = [
            pltpu.make_async_remote_copy(
                src_ref=buf_ref.at[n + (me ^ k)],
                dst_ref=late_ref.at[i],
                send_sem=sends.at[i],
                recv_sem=recvs.at[i],
                device_id={"traces": me ^ k},
                device_id_type=pl.DeviceIdType.MESH,
            )
            for i, k in enumerate(kept)
        ]
        for copy in copies:
            copy.start()
        for copy in copies:
            copy.wait()


def settle_kernel(n, order_ref, came_ref, o_ref, late_rows_ref, sem):
    rows = o_ref.shape[0]
    each = rows // n
    shift = n.bit_length() - 1
    me = lax.axis_index("traces")
    kept = block_order(n)[2]
    keeps = keeps_blocks(me, n)

    def put(d, carry):
        for r in range(each):
            q = d * each + r
            place = order_ref[q]
            source, row = place & (n - 1), place >> shift
            turn = source ^ me
            late = jnp.logical_and(keeps, functools.reduce(jnp.logical_or, [turn == k for k in kept]))

            @pl.when(late)
            def _():
                index = functools.reduce(lambda at, ik: jnp.where(turn == ik[1], ik[0], at), enumerate(kept), 0)
                late_rows_ref[index * each + row] = q

            @pl.when(jnp.logical_not(late))
            def _():
                pltpu.make_async_copy(came_ref.at[source, pl.ds(row, 1)], o_ref.at[pl.ds(q, 1)], sem).start()

        return carry

    lax.fori_loop(0, n, put, 0)

    def finish(count):
        pltpu.make_async_copy(o_ref.at[pl.ds(0, count)], o_ref.at[pl.ds(0, count)], sem).wait()

    @pl.when(keeps)
    def _():
        finish(rows - len(kept) * each)

    @pl.when(jnp.logical_not(keeps))
    def _():
        finish(rows)


def last_kernel(n, late_rows_ref, late_ref, settled_ref, o_ref, sem):
    del settled_ref
    count, each, _ = late_ref.shape

    @pl.when(keeps_blocks(lax.axis_index("traces"), n))
    def _():
        for i in range(count):
            for r in range(each):
                q = late_rows_ref[i * each + r]
                pltpu.make_async_copy(late_ref.at[i, pl.ds(r, 1)], o_ref.at[pl.ds(q, 1)], sem).start()
        part = o_ref.at[pl.ds(0, count * each)]
        pltpu.make_async_copy(part, part, sem).wait()


def tables(length, taps):
    return (
        jnp.asarray(lane_matrix(-1.0, 1.0)),
        jnp.asarray(lane_matrix(1.0, 1.0 / length)),
        jnp.asarray(twiddles(length, taps)),
    )


def scratch():
    return [
        pltpu.VMEM((RADIX * RADIX, ROWS, LANES), jnp.float32),
        pltpu.VMEM((2 * KEEP * ROWS, 6 * LANES), jnp.bfloat16),
        pltpu.VMEM((2 * KEEP * ROWS, 2 * LANES), jnp.float32),
    ]


def gathered(raw_traces, filter_index, channel_order, wavelets, damping):
    rows, length = raw_traces.shape
    own, taps = wavelets.shape
    n = lax.axis_size("traces")
    me = lax.axis_index("traces")
    each = rows // n
    floor = damping * (jnp.sum(wavelets * wavelets, axis=1) + 1e-6)
    picks = filter_index.reshape(own, rows // own).astype(jnp.float32)
    packed = lax.all_gather(jnp.concatenate([wavelets, floor[:, None], picks], axis=1), "traces", axis=0, tiled=True)
    all_picks = packed[:, taps + 1 :].reshape(n, n, each).astype(jnp.int32)
    came_picks = lax.dynamic_index_in_dim(all_picks, me, 1, keepdims=False)
    bank = jnp.concatenate([packed[:, :taps], jnp.broadcast_to(packed[:, taps : taps + 1], (own * n, LANES))], axis=1)
    fwd, inv, tw = tables(length, taps)
    whole = lambda a: pl.BlockSpec(a.shape, lambda i, *_: (0,) * a.ndim)
    fixed = [pl.BlockSpec((ROWS, taps + LANES), lambda i, *_: (i, 0)), whole(fwd), whole(inv), whole(tw)]
    came = lax.all_to_all(raw_traces.reshape(n, each, length), "traces", 0, 0, tiled=True).reshape(rows, length)
    result = pl.pallas_call(
        functools.partial(block_kernel, taps, ()),
        grid=(rows // ROWS,),
        out_shape=jax.ShapeDtypeStruct((rows, length), jnp.float32),
        in_specs=[pl.BlockSpec((ROWS, length), lambda i: (i, 0))] + fixed,
        out_specs=pl.BlockSpec((ROWS, length), lambda i: (i, 0)),
        scratch_shapes=scratch(),
        compiler_params=pltpu.CompilerParams(vmem_limit_bytes=48 * 1024 * 1024),
    )(came, jnp.take(bank, came_picks.reshape(-1), axis=0), fwd, inv, tw)
    return jnp.take(result, (channel_order % n) * each + channel_order // n, axis=0)


def local(raw_traces, filter_index, channel_order, wavelets, damping):
    rows, length = raw_traces.shape
    own, taps = wavelets.shape
    n = lax.axis_size("traces")
    if n < 4 or n & (n - 1) or rows != n * ROWS or own % SUBLANES or own > LANES or taps % LANES:
        return gathered(raw_traces, filter_index, channel_order, wavelets, damping)

    fwd, inv, tw = tables(length, taps)
    tiles = own // SUBLANES * (taps // LANES)
    outer = split_count(n)[0]
    _, raws, kept = block_order(n)
    raws, kept = len(raws), len(kept)
    dma = pltpu.SemaphoreType.DMA
    came = pl.pallas_call(
        functools.partial(exchange_kernel, n, taps),
        in_specs=[pl.BlockSpec(memory_space=pltpu.HBM)] * 7,
        out_specs=pl.BlockSpec(memory_space=pltpu.VMEM),
        out_shape=pltpu.VMEM((2 * n, ROWS, length), jnp.float32),
        scratch_shapes=scratch()
        + [pltpu.VMEM(a.shape, a.dtype) for a in (fwd, inv, tw)]
        + [
            pltpu.VMEM((n, (tiles + 1) * SUBLANES, LANES), jnp.float32),
            pltpu.VMEM((ROWS, taps + LANES), jnp.float32),
            pltpu.VMEM((ROWS // 2, length), jnp.float32),
            pltpu.SMEM(((1 + raws) * rows,), jnp.int32),
            pltpu.SMEM((own,), jnp.float32),
            dma,
            dma((n,)),
            dma((5 + tiles,)),
            dma((2, raws, 2)),
            dma((2, raws)),
            dma((outer * outer - 1 + n - outer,)),
            dma((n,)),
            pltpu.SemaphoreType.REGULAR((n,)),
            dma((n,)),
            dma((n,)),
        ],
        compiler_params=pltpu.CompilerParams(
            collective_id=0, has_side_effects=True, vmem_limit_bytes=40 * 1024 * 1024
        ),
        cost_estimate=pl.CostEstimate(flops=rows * length * 1500, bytes_accessed=8 * rows * length, transcendentals=0),
    )(raw_traces, filter_index, wavelets, damping, fwd, inv, tw)
    came = pltpu.with_memory_space_constraint(came, pltpu.VMEM)
    smem, vmem, hbm = (pl.BlockSpec(memory_space=m) for m in (pltpu.SMEM, pltpu.VMEM, pltpu.HBM))
    params = pltpu.CompilerParams(vmem_limit_bytes=20 * 1024 * 1024)
    settled, late_rows = pl.pallas_call(
        functools.partial(settle_kernel, n),
        in_specs=[smem, vmem],
        out_specs=[hbm, smem],
        out_shape=[
            jax.ShapeDtypeStruct((rows, length), jnp.float32),
            pltpu.SMEM((kept * ROWS,), jnp.int32),
        ],
        scratch_shapes=[dma],
        compiler_params=params,
    )(channel_order, came)
    late_rows = pltpu.with_memory_space_constraint(late_rows, pltpu.SMEM)
    late = pl.pallas_call(
        functools.partial(late_kernel, n),
        in_specs=[vmem, smem],
        out_specs=vmem,
        out_shape=pltpu.VMEM((kept, ROWS, length), jnp.float32),
        scratch_shapes=[dma((kept,)), dma((kept,))],
        compiler_params=pltpu.CompilerParams(
            collective_id=1, has_side_effects=True, vmem_limit_bytes=20 * 1024 * 1024
        ),
    )(came, late_rows)
    late = pltpu.with_memory_space_constraint(late, pltpu.VMEM)
    return pl.pallas_call(
        functools.partial(last_kernel, n),
        in_specs=[smem, vmem, hbm],
        out_specs=hbm,
        out_shape=jax.ShapeDtypeStruct((rows, length), jnp.float32),
        scratch_shapes=[dma],
        input_output_aliases={2: 0},
        compiler_params=params,
    )(late_rows, late, settled)


def solution(mesh):
    placed = (
        P(("groups", "traces"), None),
        P(("groups", "traces")),
        P("groups"),
        P("traces", None),
        P("traces"),
    )
    return jax.shard_map(
        local, mesh=mesh, in_specs=placed, out_specs=P(("groups", "traces"), None), check_vma=False
    )
```

```python
import functools
import math

import jax
import jax.numpy as jnp
import numpy as np
from jax import lax
from jax.experimental import pallas as pl
from jax.experimental.pallas import tpu as pltpu
from jax.sharding import PartitionSpec as P

LANES = 128
RADIX = 8
ROWS = 16
SUBLANES = 8

KEPT = (
    [RADIX * b for b in range(RADIX // 2 + 1)]
    + [a + RADIX * b for a in range(1, RADIX // 2) for b in range(RADIX)]
    + [RADIX // 2 + RADIX * b for b in range(RADIX // 2)]
)
SLOT = {k: s for s, k in enumerate(KEPT)}
KEEP = len(KEPT)


def lane_matrix(sign, scale):
    ids = np.arange(LANES)
    angle = 2.0 * np.pi * (np.outer(ids, ids) % LANES) / LANES
    c, s = np.cos(angle) * scale, sign * np.sin(angle) * scale
    full = np.block([[c, s], [-s, c]])
    import ml_dtypes

    high = full.astype(np.float32).astype(ml_dtypes.bfloat16)
    low = (full.astype(np.float32) - high.astype(np.float32)).astype(ml_dtypes.bfloat16)
    return np.concatenate([high, high, low], axis=0)


def twiddles(length, taps):
    m = np.arange(LANES)
    rows = []
    for k in KEPT:
        angle = 2.0 * np.pi * k * m / length
        row = [np.cos(angle), -np.sin(angle)]
        weight = 1.0 if k in (0, RADIX * RADIX // 2) else 2.0
        row += [weight * np.cos(angle), weight * np.sin(angle)]
        for piece in range(taps // LANES):
            shifted = 2.0 * np.pi * k * (m + LANES * piece) / length
            row += [np.cos(shifted), -np.sin(shifted)]
        rows.append(np.stack(row))
    return np.stack(rows).astype(np.float32)


def cadd(a, b):
    return (a[0] + b[0], a[1] + b[1])


def csub(a, b):
    return (a[0] - b[0], a[1] - b[1])


def turn(a, num, den):
    num %= den
    if num == 0:
        return a
    if 4 * num == den:
        return (-a[1], a[0])
    if 2 * num == den:
        return (-a[0], -a[1])
    if 4 * num == 3 * den:
        return (a[1], -a[0])
    c, s = math.cos(2 * math.pi * num / den), math.sin(2 * math.pi * num / den)
    return (a[0] * c - a[1] * s, a[0] * s + a[1] * c)


def fourier(items, sign):
    n = len(items)
    if n == 1:
        return items
    even, odd = fourier(items[0::2], sign), fourier(items[1::2], sign)
    turned = [turn(o, sign * k, n) for k, o in enumerate(odd)]
    return [cadd(e, t) for e, t in zip(even, turned)] + [csub(e, t) for e, t in zip(even, turned)]


def real_eight(v):
    h = math.sqrt(0.5)
    s0, d0, s1, d1 = v[0] + v[4], v[0] - v[4], v[1] + v[5], v[1] - v[5]
    s2, d2, s3, d3 = v[2] + v[6], v[2] - v[6], v[3] + v[7], v[3] - v[7]
    p, q = s0 + s2, s1 + s3
    r, t = (d1 - d3) * h, (d1 + d3) * h
    return [p + q, (d0 + r, -(d2 + t)), (s0 - s2, s3 - s1), (d0 - r, d2 - t), p - q]


def eight_real(u0, u1, u2, u3, u4):
    h = math.sqrt(0.5)
    p, q = u0 + u4, u0 - u4
    e = [p + u2[0], q - u2[1], p - u2[0], q + u2[1]]
    f, g = u1[0] - u3[0], u1[1] + u3[1]
    o = [u1[0] + u3[0], (f - g) * h, u3[1] - u1[1], -(f + g) * h]
    return [a + b for a, b in zip(e, o)] + [a - b for a, b in zip(e, o)]


def put_split(ref, base, re, im):
    rows = pl.ds(base, ROWS)
    for part, value in enumerate((re, im)):
        high = value.astype(jnp.bfloat16)
        low = (value - high.astype(jnp.float32)).astype(jnp.bfloat16)
        at = part * LANES
        ref[rows, at : at + LANES] = high
        ref[rows, 2 * LANES + at : 2 * LANES + at + LANES] = low
        ref[rows, 4 * LANES + at : 4 * LANES + at + LANES] = high


def deconvolve(read, write, wave, floor, fwd_ref, inv_ref, tw_ref, mid_ref, cut_ref, spec_ref):
    half, wide = RADIX // 2, RADIX * RADIX
    for j2 in range(RADIX):
        out = real_eight([read(RADIX * j1 + j2) for j1 in range(RADIX)])
        mid_ref[2 * j2] = out[0]
        mid_ref[2 * j2 + 1] = out[half]
        for a in range(1, half):
            mid_ref[2 * RADIX * a + 2 * j2] = out[a][0]
            mid_ref[2 * RADIX * a + 2 * j2 + 1] = out[a][1]

    def emit(k, value):
        s = SLOT[k]
        c, n = tw_ref[s, 0:1, :], tw_ref[s, 1:2, :]
        put_split(cut_ref, s * ROWS, value[0] * c - value[1] * n, value[0] * n + value[1] * c)

    zero = real_eight([mid_ref[2 * j2] for j2 in range(RADIX)])
    c, n = tw_ref[0, 0:1, :], tw_ref[0, 1:2, :]
    for b in range(half + 1):
        s = SLOT[RADIX * b]
        c, n = tw_ref[s, 0:1, :], tw_ref[s, 1:2, :]
        if b in (0, half):
            put_split(cut_ref, s * ROWS, zero[b] * c, zero[b] * n)
        else:
            emit(RADIX * b, zero[b])
    for a in range(1, half):
        base = 2 * RADIX * a
        items = [turn((mid_ref[base + 2 * j2], mid_ref[base + 2 * j2 + 1]), -a * j2, wide) for j2 in range(RADIX)]
        for b, value in enumerate(fourier(items, -1)):
            emit(a + RADIX * b, value)
    four = [mid_ref[2 * j2 + 1] for j2 in range(RADIX)]
    for b in range(half):
        k = half + RADIX * b
        re, im = four[0], None
        for j2 in range(1, RADIX):
            angle = 2 * math.pi * (k * j2 % wide) / wide
            re = re + four[j2] * math.cos(angle)
            term = four[j2] * -math.sin(angle)
            im = term if im is None else im + term
        emit(k, (re, im))

    for s in range(KEEP):
        re = im = None
        for piece, taps in enumerate(wave):
            c, n = tw_ref[s, 4 + 2 * piece : 5 + 2 * piece, :], tw_ref[s, 5 + 2 * piece : 6 + 2 * piece, :]
            re = taps * c if re is None else re + taps * c
            im = taps * n if im is None else im + taps * n
        put_split(cut_ref, (KEEP + s) * ROWS, re, im)

    spec_ref[...] = jnp.dot(cut_ref[...], fwd_ref[...], preferred_element_type=jnp.float32)

    def apply(s, carry):
        at = pl.multiple_of(s * ROWS, ROWS)
        other = pl.multiple_of((KEEP + s) * ROWS, ROWS)
        xr, xi = spec_ref[pl.ds(at, ROWS), 0:LANES], spec_ref[pl.ds(at, ROWS), LANES:]
        hr, hi = spec_ref[pl.ds(other, ROWS), 0:LANES], spec_ref[pl.ds(other, ROWS), LANES:]
        scale = 1.0 / (hr * hr + hi * hi + floor)
        put_split(cut_ref, at, (xr * hr + xi * hi) * scale, (xi * hr - xr * hi) * scale)
        return carry

    lax.fori_loop(0, KEEP, apply, 0, unroll=3)
    rows = KEEP * ROWS
    spec_ref[0:rows] = jnp.dot(cut_ref[0:rows], inv_ref[...], preferred_element_type=jnp.float32)

    def fetch(k):
        s = SLOT[k]
        re, im = spec_ref[s * ROWS : (s + 1) * ROWS, 0:LANES], spec_ref[s * ROWS : (s + 1) * ROWS, LANES:]
        c, n = tw_ref[s, 2:3, :], tw_ref[s, 3:4, :]
        if k in (0, wide // 2):
            return re * c - im * n
        return (re * c - im * n, re * n + im * c)

    for a in range(1, half):
        base = 2 * RADIX * a
        for j2, value in enumerate(fourier([fetch(a + RADIX * b) for b in range(RADIX)], 1)):
            value = turn(value, a * j2, wide)
            mid_ref[base + 2 * j2] = value[0]
            mid_ref[base + 2 * j2 + 1] = value[1]
    for j2, value in enumerate(eight_real(*[fetch(RADIX * b) for b in range(half + 1)])):
        mid_ref[2 * j2] = value
    four = [fetch(half + RADIX * b) for b in range(half)]
    for j2 in range(RADIX):
        total = None
        for b, value in enumerate(four):
            angle = 2 * math.pi * ((half + RADIX * b) * j2 % wide) / wide
            term = value[0] * math.cos(angle)
            if j2:
                term = term - value[1] * math.sin(angle)
            total = term if total is None else total + term
        mid_ref[2 * j2 + 1] = total
    for j2 in range(RADIX):
        parts = [mid_ref[2 * j2]]
        for a in range(1, half):
            base = 2 * RADIX * a
            parts.append((mid_ref[base + 2 * j2], mid_ref[base + 2 * j2 + 1]))
        parts.append(mid_ref[2 * j2 + 1])
        for j1, value in enumerate(eight_real(*parts)):
            write(RADIX * j1 + j2, value)


def slabs(ref, lead):
    def at(j):
        return lead + (slice(None), slice(j * LANES, (j + 1) * LANES))

    def read(j):
        value = ref[at(j)]
        return value.reshape(ROWS, LANES)

    def write(j, value):
        ref[at(j)] = value.reshape(ref[at(j)].shape)

    return read, write


def block_kernel(taps, lead, x_ref, w_ref, fwd_ref, inv_ref, tw_ref, o_ref, mid_ref, cut_ref, spec_ref):
    read, _ = slabs(x_ref, lead)
    _, write = slabs(o_ref, (slice(None),) * (len(o_ref.shape) - 2))
    wave = [w_ref[:, p * LANES : (p + 1) * LANES] for p in range(taps // LANES)]
    deconvolve(read, write, wave, w_ref[:, taps : taps + LANES], fwd_ref, inv_ref, tw_ref, mid_ref, cut_ref, spec_ref)


def split_count(n):
    inner = 1
    while inner * inner < n:
        inner *= 2
    return (n // inner, inner) if n % inner == 0 else (1, n)


def block_order(n):
    inner = split_count(n)[1]
    raws = list(range(n - inner + 1, n, 2))[:2]
    kept = list(range(n - inner, n, 2))[1::-1]
    near = sorted(range(1, n // 2), key=lambda k: (k < inner, k))
    cross = [k for k in range(n // 2, n) if k not in raws + kept]
    return cross + near + kept + raws + [0], raws, kept


def keeps_blocks(me, n):
    outer, inner = split_count(n)
    far = lax.div(me, inner)
    return jnp.logical_and(me % 2 == 0, jnp.logical_or(far == outer // 2 - 1, far == outer // 2))


def exchange_kernel(
    n,
    taps,
    x_ref,
    pick_ref,
    wave_ref,
    damp_ref,
    fwd_hbm,
    inv_hbm,
    tw_hbm,
    buf_ref,
    mid_ref,
    cut_ref,
    spec_ref,
    fwd_ref,
    inv_ref,
    tw_ref,
    bank_ref,
    rows_ref,
    stage_ref,
    pick_smem,
    damp_smem,
    stage_sem,
    load_sems,
    near_sems,
    raw_sems,
    pick_sems,
    bank_sends,
    bank_recvs,
    ready_sems,
    sends,
    recvs,
):
    me = lax.axis_index("traces")
    own, each = wave_ref.shape[0], x_ref.shape[0] // n
    outer, inner = split_count(n)
    far, near = lax.div(me, inner), lax.rem(me, inner)
    halves, pieces = own // SUBLANES, taps // LANES
    last = halves * pieces

    def remote(src, dst, send_sem, recv_sem, device):
        return pltpu.make_async_remote_copy(
            src_ref=src,
            dst_ref=dst,
            send_sem=send_sem,
            recv_sem=recv_sem,
            device_id={"traces": device},
            device_id_type=pl.DeviceIdType.MESH,
        )

    def block_of(e):
        return x_ref.at[pl.ds(pl.multiple_of(e * each, each), each)]

    turns, raws, kept = block_order(n)
    partner = me ^ raws[0]
    made = n - 1 - len(raws)
    sent_here = made - jnp.where(keeps_blocks(me, n), len(kept), 0)

    def turn_of(s):
        k = 0
        for i, turn in enumerate(turns):
            k = jnp.where(s == i, turn, k)
        return k

    barrier = pltpu.get_barrier_semaphore()

    def tell(sem, other):
        pl.semaphore_signal(sem, inc=1, device_id={"traces": other}, device_id_type=pl.DeviceIdType.MESH)

    def greet(other, carry):
        tell(barrier, other)
        return carry

    def answer(other, carry):
        @pl.when(other != partner)
        def _():
            tell(ready_sems.at[me], other)

        return carry

    def meet(other, carry):
        @pl.when(other != partner)
        def _():
            pl.semaphore_wait(ready_sems.at[other], 1)

        return carry

    def raw(i, part, here):
        first, count, other = part * (each // 2), each // 2, me ^ raws[i]
        rows = x_ref.at[pl.ds(pl.multiple_of(other * each + first, count), count)]
        there = buf_ref.at[n + jnp.where(here, other, me), pl.ds(first, count)]
        return remote(rows, there, raw_sems.at[0, i, part], raw_sems.at[1, i, part], other)

    def raw_staged():
        there = buf_ref.at[n + me, pl.ds(0, each // 2)]
        return remote(stage_ref, there, raw_sems.at[0, 0, 0], raw_sems.at[1, 0, 0], partner)

    stage = pl.ds(pl.multiple_of(partner * each, each // 2), each // 2)
    stage_in = pltpu.make_async_copy(x_ref.at[stage], stage_ref, stage_sem)

    @pl.when(partner > me)
    def _():
        stage_in.start()

    lax.fori_loop(me + 1, n, greet, 0)

    @pl.when(me > 0)
    def _():
        pl.semaphore_wait(barrier, me)

    @pl.when(partner < me)
    def _():
        tell(ready_sems.at[me], partner)
        raw(0, 0, False).start()

    damp_in = pltpu.make_async_copy(damp_ref, damp_smem, near_sems.at[0])
    pick_in = pltpu.make_async_copy(pick_ref, pick_smem.at[pl.ds(0, n * each)], near_sems.at[1])
    tables_in = [
        pltpu.make_async_copy(there, here, near_sems.at[2 + i])
        for i, (there, here) in enumerate(((fwd_hbm, fwd_ref), (inv_hbm, inv_ref), (tw_hbm, tw_ref)))
    ]
    tiles_in = [
        pltpu.make_async_copy(
            wave_ref.at[pl.ds(h * SUBLANES, SUBLANES), pl.ds(p * LANES, LANES)],
            bank_ref.at[me, pl.ds((h * pieces + p) * SUBLANES, SUBLANES)],
            near_sems.at[5 + h * pieces + p],
        )
        for h in range(halves)
        for p in range(pieces)
    ]
    for copy in [damp_in] + tiles_in + [pick_in] + tables_in:
        copy.start()

    def load(e):
        return pltpu.make_async_copy(block_of(e), buf_ref.at[n + e], load_sems.at[e])

    def load_start(s, carry):
        @pl.when(jnp.logical_or(s < made, s == n - 1))
        def _():
            load(me ^ turn_of(s)).start()

        return carry

    def picks(i):
        count = n * each
        there = pick_smem.at[pl.ds((1 + i) * count, count)]
        return remote(pick_ref, there, pick_sems.at[0, i], pick_sems.at[1, i], me ^ raws[i])

    @pl.when(partner > me)
    def _():
        stage_in.wait()
        pl.semaphore_wait(ready_sems.at[partner], 1)
        raw_staged().start()

    lax.fori_loop(0, me, answer, 0)
    damp_in.wait()
    lane = lax.broadcasted_iota(jnp.int32, (SUBLANES, LANES), 1)
    levels = jnp.zeros((SUBLANES, LANES), jnp.float32)
    for f in range(own):
        levels = jnp.where(lane == f, damp_smem[f], levels)
    bank_ref[me, last * SUBLANES : (last + 1) * SUBLANES, :] = levels
    lax.fori_loop(me + 1, n, meet, 0)
    for copy in tiles_in:
        copy.wait()

    def bank_copy(block, slot, there):
        used = bank_ref.at[block, pl.ds(0, last * SUBLANES + 1)]
        return remote(used, used, bank_sends.at[slot], bank_recvs.at[block], there)

    def block_at(f):
        return f * inner + near

    middle = outer // 2
    upper = far >= middle
    gate = jnp.where(upper, middle, middle - 1)

    def across(t, act):
        there = lax.rem(far + t, outer)
        direct = jnp.logical_or((there >= middle) == upper, there == outer - 1 - gate)

        @pl.when(direct)
        def _():
            act(bank_copy(me, t - 1, block_at(there)))

    def onward(t, act):
        block = lax.rem(far + t, outer)
        for there in range(outer):
            slot = outer - 1 + (t - 1) * outer + there
            near_side = (there >= middle) == upper
            foreign = (block >= middle) != upper
            go = jnp.logical_and(jnp.logical_and(far == gate, far != there), jnp.logical_and(near_side, foreign))

            @pl.when(go)
            def _():
                act(bank_copy(block_at(block), slot, block_at(there)))

    def spread(f, act):
        for d in range(1, inner):
            slot = outer * outer - 1 + f * (inner - 1) + d - 1
            act(bank_copy(block_at(f), slot, far * inner + (near ^ d)))

    def bank_came(block):
        bank_copy(block, 0, partner).wait_recv()

    start, sent = (lambda copy: copy.start()), (lambda copy: copy.wait_send())
    for t in range(1, outer):
        across(t, start)
    spread(far, start)
    raw(0, 1, False).start()
    for i in range(1, len(raws)):
        raw(i, 0, False).start()
        raw(i, 1, False).start()
    for i in range(len(raws)):
        picks(i).start()
    lax.fori_loop(0, n, load_start, 0)
    for t in range(1, outer):
        block = lax.rem(far + t, outer)
        bank_came(block_at(block))
        onward(t, start)
        spread(block, start)
    for f in range(outer):
        for d in range(1, inner):
            bank_came(f * inner + (near ^ d))
    pick_in.wait()
    for copy in tables_in:
        copy.wait()

    def send(e):
        return remote(buf_ref.at[n + e], buf_ref.at[me], sends.at[e], recvs.at[me], e)

    row_lane = lax.broadcasted_iota(jnp.int32, (1, LANES), 1)

    def step(s, carry):
        e = me ^ turn_of(s)
        theirs = jnp.logical_and(s >= made, s < n - 1)
        for i in range(len(raws)):

            @pl.when(s == made + i)
            def _():
                raw(i, 0, True).wait_recv()
                raw(i, 1, True).wait_recv()
                picks(i).wait_recv()

        @pl.when(jnp.logical_not(theirs))
        def _():
            load(e).wait()

        table = jnp.where(theirs, s - made + 1, 0)
        base = (table * n + jnp.where(theirs, me, e)) * each
        for r in range(ROWS):
            pick = pick_smem[base + r]
            block, inside = lax.div(pick, own), lax.rem(pick, own)
            at = lax.div(inside, SUBLANES) * (pieces * SUBLANES) + lax.rem(inside, SUBLANES)
            for p in range(pieces):
                rows_ref[r : r + 1, p * LANES : (p + 1) * LANES] = bank_ref[block, pl.ds(at + p * SUBLANES, 1), :]
            level = bank_ref[block, last * SUBLANES : last * SUBLANES + 1, :]
            rows_ref[r : r + 1, taps : taps + LANES] = jnp.where(row_lane == inside, level, 0.0)

        @pl.when(jnp.logical_and(s >= 1, s <= sent_here))
        def _():
            send(me ^ turn_of(s - 1)).start()

        slot = jnp.where(s >= made, e, n + e)
        wave = [rows_ref[:, p * LANES : (p + 1) * LANES] for p in range(pieces)]
        power = sum(jnp.sum(w * w, axis=1, keepdims=True) for w in wave)
        damp = jnp.sum(rows_ref[:, taps : taps + LANES], axis=1, keepdims=True)
        floor = jnp.broadcast_to(damp * (power + 1e-6), (ROWS, LANES))

        def read(j):
            return buf_ref[n + e, :, j * LANES : (j + 1) * LANES]

        def write(j, value):
            buf_ref[slot, :, j * LANES : (j + 1) * LANES] = value

        deconvolve(read, write, wave, floor, fwd_ref, inv_ref, tw_ref, mid_ref, cut_ref, spec_ref)
        return carry

    lax.fori_loop(0, n, step, 0)

    for i in range(len(raws)):
        raw(i, 0, False).wait_send()
        raw(i, 1, False).wait_send()
        picks(i).wait_send()
    for t in range(1, outer):
        across(t, sent)
        onward(t, sent)
    for f in range(outer):
        spread(f, sent)

    def finish(s, carry):
        e = me ^ turn_of(s)
        send(e).wait_send()
        remote(buf_ref.at[e], buf_ref.at[e], sends.at[e], recvs.at[e], e).wait_recv()
        return carry

    lax.fori_loop(0, sent_here, finish, 0)


def late_kernel(n, buf_ref, after_ref, late_ref, sends, recvs):
    del after_ref
    me = lax.axis_index("traces")
    kept = block_order(n)[2]

    @pl.when(keeps_blocks(me, n))
    def _():
        barrier = pltpu.get_barrier_semaphore()
        for k in kept:
            pl.semaphore_signal(barrier, inc=1, device_id={"traces": me ^ k}, device_id_type=pl.DeviceIdType.MESH)
        pl.semaphore_wait(barrier, len(kept))
        copies = [
            pltpu.make_async_remote_copy(
                src_ref=buf_ref.at[n + (me ^ k)],
                dst_ref=late_ref.at[i],
                send_sem=sends.at[i],
                recv_sem=recvs.at[i],
                device_id={"traces": me ^ k},
                device_id_type=pl.DeviceIdType.MESH,
            )
            for i, k in enumerate(kept)
        ]
        for copy in copies:
            copy.start()
        for copy in copies:
            copy.wait()


def settle_kernel(n, order_ref, came_ref, o_ref, late_rows_ref, sem):
    rows = o_ref.shape[0]
    each = rows // n
    shift = n.bit_length() - 1
    me = lax.axis_index("traces")
    kept = block_order(n)[2]
    keeps = keeps_blocks(me, n)

    def put(d, carry):
        for r in range(each):
            q = d * each + r
            place = order_ref[q]
            source, row = place & (n - 1), place >> shift
            turn = source ^ me
            late = jnp.logical_and(keeps, functools.reduce(jnp.logical_or, [turn == k for k in kept]))

            @pl.when(late)
            def _():
                index = functools.reduce(lambda at, ik: jnp.where(turn == ik[1], ik[0], at), enumerate(kept), 0)
                late_rows_ref[index * each + row] = q

            @pl.when(jnp.logical_not(late))
            def _():
                pltpu.make_async_copy(came_ref.at[source, pl.ds(row, 1)], o_ref.at[pl.ds(q, 1)], sem).start()

        return carry

    lax.fori_loop(0, n, put, 0)

    def finish(count):
        pltpu.make_async_copy(o_ref.at[pl.ds(0, count)], o_ref.at[pl.ds(0, count)], sem).wait()

    @pl.when(keeps)
    def _():
        finish(rows - len(kept) * each)

    @pl.when(jnp.logical_not(keeps))
    def _():
        finish(rows)


def last_kernel(n, late_rows_ref, late_ref, settled_ref, o_ref, sem):
    del settled_ref
    count, each, _ = late_ref.shape

    @pl.when(keeps_blocks(lax.axis_index("traces"), n))
    def _():
        for i in range(count):
            for r in range(each):
                q = late_rows_ref[i * each + r]
                pltpu.make_async_copy(late_ref.at[i, pl.ds(r, 1)], o_ref.at[pl.ds(q, 1)], sem).start()
        part = o_ref.at[pl.ds(0, count * each)]
        pltpu.make_async_copy(part, part, sem).wait()


def tables(length, taps):
    return (
        jnp.asarray(lane_matrix(-1.0, 1.0)),
        jnp.asarray(lane_matrix(1.0, 1.0 / length)),
        jnp.asarray(twiddles(length, taps)),
    )


def scratch():
    return [
        pltpu.VMEM((RADIX * RADIX, ROWS, LANES), jnp.float32),
        pltpu.VMEM((2 * KEEP * ROWS, 6 * LANES), jnp.bfloat16),
        pltpu.VMEM((2 * KEEP * ROWS, 2 * LANES), jnp.float32),
    ]


def gathered(raw_traces, filter_index, channel_order, wavelets, damping):
    rows, length = raw_traces.shape
    own, taps = wavelets.shape
    n = lax.axis_size("traces")
    me = lax.axis_index("traces")
    each = rows // n
    floor = damping * (jnp.sum(wavelets * wavelets, axis=1) + 1e-6)
    picks = filter_index.reshape(own, rows // own).astype(jnp.float32)
    packed = lax.all_gather(jnp.concatenate([wavelets, floor[:, None], picks], axis=1), "traces", axis=0, tiled=True)
    all_picks = packed[:, taps + 1 :].reshape(n, n, each).astype(jnp.int32)
    came_picks = lax.dynamic_index_in_dim(all_picks, me, 1, keepdims=False)
    bank = jnp.concatenate([packed[:, :taps], jnp.broadcast_to(packed[:, taps : taps + 1], (own * n, LANES))], axis=1)
    fwd, inv, tw = tables(length, taps)
    whole = lambda a: pl.BlockSpec(a.shape, lambda i, *_: (0,) * a.ndim)
    fixed = [pl.BlockSpec((ROWS, taps + LANES), lambda i, *_: (i, 0)), whole(fwd), whole(inv), whole(tw)]
    came = lax.all_to_all(raw_traces.reshape(n, each, length), "traces", 0, 0, tiled=True).reshape(rows, length)
    result = pl.pallas_call(
        functools.partial(block_kernel, taps, ()),
        grid=(rows // ROWS,),
        out_shape=jax.ShapeDtypeStruct((rows, length), jnp.float32),
        in_specs=[pl.BlockSpec((ROWS, length), lambda i: (i, 0))] + fixed,
        out_specs=pl.BlockSpec((ROWS, length), lambda i: (i, 0)),
        scratch_shapes=scratch(),
        compiler_params=pltpu.CompilerParams(vmem_limit_bytes=48 * 1024 * 1024),
    )(came, jnp.take(bank, came_picks.reshape(-1), axis=0), fwd, inv, tw)
    return jnp.take(result, (channel_order % n) * each + channel_order // n, axis=0)


def local(raw_traces, filter_index, channel_order, wavelets, damping):
    rows, length = raw_traces.shape
    own, taps = wavelets.shape
    n = lax.axis_size("traces")
    if n < 4 or n & (n - 1) or rows != n * ROWS or own % SUBLANES or own > LANES or taps % LANES:
        return gathered(raw_traces, filter_index, channel_order, wavelets, damping)

    fwd, inv, tw = tables(length, taps)
    tiles = own // SUBLANES * (taps // LANES)
    outer = split_count(n)[0]
    _, raws, kept = block_order(n)
    raws, kept = len(raws), len(kept)
    dma = pltpu.SemaphoreType.DMA
    came = pl.pallas_call(
        functools.partial(exchange_kernel, n, taps),
        in_specs=[pl.BlockSpec(memory_space=pltpu.HBM)] * 7,
        out_specs=pl.BlockSpec(memory_space=pltpu.VMEM),
        out_shape=pltpu.VMEM((2 * n, ROWS, length), jnp.float32),
        scratch_shapes=scratch()
        + [pltpu.VMEM(a.shape, a.dtype) for a in (fwd, inv, tw)]
        + [
            pltpu.VMEM((n, (tiles + 1) * SUBLANES, LANES), jnp.float32),
            pltpu.VMEM((ROWS, taps + LANES), jnp.float32),
            pltpu.VMEM((ROWS // 2, length), jnp.float32),
            pltpu.SMEM(((1 + raws) * rows,), jnp.int32),
            pltpu.SMEM((own,), jnp.float32),
            dma,
            dma((n,)),
            dma((5 + tiles,)),
            dma((2, raws, 2)),
            dma((2, raws)),
            dma((outer * outer - 1 + n - outer,)),
            dma((n,)),
            pltpu.SemaphoreType.REGULAR((n,)),
            dma((n,)),
            dma((n,)),
        ],
        compiler_params=pltpu.CompilerParams(
            collective_id=0, has_side_effects=True, vmem_limit_bytes=40 * 1024 * 1024
        ),
        cost_estimate=pl.CostEstimate(flops=rows * length * 1500, bytes_accessed=8 * rows * length, transcendentals=0),
    )(raw_traces, filter_index, wavelets, damping, fwd, inv, tw)
    came = pltpu.with_memory_space_constraint(came, pltpu.VMEM)
    smem, vmem, hbm = (pl.BlockSpec(memory_space=m) for m in (pltpu.SMEM, pltpu.VMEM, pltpu.HBM))
    params = pltpu.CompilerParams(vmem_limit_bytes=20 * 1024 * 1024)
    settled, late_rows = pl.pallas_call(
        functools.partial(settle_kernel, n),
        in_specs=[smem, vmem],
        out_specs=[hbm, smem],
        out_shape=[
            jax.ShapeDtypeStruct((rows, length), jnp.float32),
            pltpu.SMEM((kept * ROWS,), jnp.int32),
        ],
        scratch_shapes=[dma],
        compiler_params=params,
    )(channel_order, came)
    late_rows = pltpu.with_memory_space_constraint(late_rows, pltpu.SMEM)
    late = pl.pallas_call(
        functools.partial(late_kernel, n),
        in_specs=[vmem, smem],
        out_specs=vmem,
        out_shape=pltpu.VMEM((kept, ROWS, length), jnp.float32),
        scratch_shapes=[dma((kept,)), dma((kept,))],
        compiler_params=pltpu.CompilerParams(
            collective_id=1, has_side_effects=True, vmem_limit_bytes=20 * 1024 * 1024
        ),
    )(came, late_rows)
    late = pltpu.with_memory_space_constraint(late, pltpu.VMEM)
    return pl.pallas_call(
        functools.partial(last_kernel, n),
        in_specs=[smem, vmem, hbm],
        out_specs=hbm,
        out_shape=jax.ShapeDtypeStruct((rows, length), jnp.float32),
        scratch_shapes=[dma],
        input_output_aliases={2: 0},
        compiler_params=params,
    )(late_rows, late, settled)


def solution(mesh):
    placed = (
        P(("groups", "traces"), None),
        P(("groups", "traces")),
        P("groups"),
        P("traces", None),
        P("traces"),
    )
    return jax.shard_map(
        local, mesh=mesh, in_specs=placed, out_specs=P(("groups", "traces"), None), check_vma=False
    )
```

```python
import functools
import math

import jax
import jax.numpy as jnp
import numpy as np
from jax import lax
from jax.experimental import pallas as pl
from jax.experimental.pallas import tpu as pltpu
from jax.sharding import PartitionSpec as P

LANES = 128
RADIX = 8
ROWS = 16
SUBLANES = 8

KEPT = (
    [RADIX * b for b in range(RADIX // 2 + 1)]
    + [a + RADIX * b for a in range(1, RADIX // 2) for b in range(RADIX)]
    + [RADIX // 2 + RADIX * b for b in range(RADIX // 2)]
)
SLOT = {k: s for s, k in enumerate(KEPT)}
KEEP = len(KEPT)


def lane_matrix(sign, scale):
    ids = np.arange(LANES)
    angle = 2.0 * np.pi * (np.outer(ids, ids) % LANES) / LANES
    c, s = np.cos(angle) * scale, sign * np.sin(angle) * scale
    full = np.block([[c, s], [-s, c]])
    import ml_dtypes

    high = full.astype(np.float32).astype(ml_dtypes.bfloat16)
    low = (full.astype(np.float32) - high.astype(np.float32)).astype(ml_dtypes.bfloat16)
    return np.concatenate([high, high, low], axis=0)


def twiddles(length, taps):
    m = np.arange(LANES)
    rows = []
    for k in KEPT:
        angle = 2.0 * np.pi * k * m / length
        row = [np.cos(angle), -np.sin(angle)]
        weight = 1.0 if k in (0, RADIX * RADIX // 2) else 2.0
        row += [weight * np.cos(angle), weight * np.sin(angle)]
        for piece in range(taps // LANES):
            shifted = 2.0 * np.pi * k * (m + LANES * piece) / length
            row += [np.cos(shifted), -np.sin(shifted)]
        rows.append(np.stack(row))
    return np.stack(rows).astype(np.float32)


def cadd(a, b):
    return (a[0] + b[0], a[1] + b[1])


def csub(a, b):
    return (a[0] - b[0], a[1] - b[1])


def turn(a, num, den):
    num %= den
    if num == 0:
        return a
    if 4 * num == den:
        return (-a[1], a[0])
    if 2 * num == den:
        return (-a[0], -a[1])
    if 4 * num == 3 * den:
        return (a[1], -a[0])
    c, s = math.cos(2 * math.pi * num / den), math.sin(2 * math.pi * num / den)
    return (a[0] * c - a[1] * s, a[0] * s + a[1] * c)


def fourier(items, sign):
    n = len(items)
    if n == 1:
        return items
    even, odd = fourier(items[0::2], sign), fourier(items[1::2], sign)
    turned = [turn(o, sign * k, n) for k, o in enumerate(odd)]
    return [cadd(e, t) for e, t in zip(even, turned)] + [csub(e, t) for e, t in zip(even, turned)]


def real_eight(v):
    h = math.sqrt(0.5)
    s0, d0, s1, d1 = v[0] + v[4], v[0] - v[4], v[1] + v[5], v[1] - v[5]
    s2, d2, s3, d3 = v[2] + v[6], v[2] - v[6], v[3] + v[7], v[3] - v[7]
    p, q = s0 + s2, s1 + s3
    r, t = (d1 - d3) * h, (d1 + d3) * h
    return [p + q, (d0 + r, -(d2 + t)), (s0 - s2, s3 - s1), (d0 - r, d2 - t), p - q]


def eight_real(u0, u1, u2, u3, u4):
    h = math.sqrt(0.5)
    p, q = u0 + u4, u0 - u4
    e = [p + u2[0], q - u2[1], p - u2[0], q + u2[1]]
    f, g = u1[0] - u3[0], u1[1] + u3[1]
    o = [u1[0] + u3[0], (f - g) * h, u3[1] - u1[1], -(f + g) * h]
    return [a + b for a, b in zip(e, o)] + [a - b for a, b in zip(e, o)]


def put_split(ref, base, re, im):
    rows = pl.ds(base, ROWS)
    for part, value in enumerate((re, im)):
        high = value.astype(jnp.bfloat16)
        low = (value - high.astype(jnp.float32)).astype(jnp.bfloat16)
        at = part * LANES
        ref[rows, at : at + LANES] = high
        ref[rows, 2 * LANES + at : 2 * LANES + at + LANES] = low
        ref[rows, 4 * LANES + at : 4 * LANES + at + LANES] = high


def deconvolve(read, write, wave, floor, fwd_ref, inv_ref, tw_ref, mid_ref, cut_ref, spec_ref):
    half, wide = RADIX // 2, RADIX * RADIX
    for j2 in range(RADIX):
        out = real_eight([read(RADIX * j1 + j2) for j1 in range(RADIX)])
        mid_ref[2 * j2] = out[0]
        mid_ref[2 * j2 + 1] = out[half]
        for a in range(1, half):
            mid_ref[2 * RADIX * a + 2 * j2] = out[a][0]
            mid_ref[2 * RADIX * a + 2 * j2 + 1] = out[a][1]

    def emit(k, value):
        s = SLOT[k]
        c, n = tw_ref[s, 0:1, :], tw_ref[s, 1:2, :]
        put_split(cut_ref, s * ROWS, value[0] * c - value[1] * n, value[0] * n + value[1] * c)

    zero = real_eight([mid_ref[2 * j2] for j2 in range(RADIX)])
    c, n = tw_ref[0, 0:1, :], tw_ref[0, 1:2, :]
    for b in range(half + 1):
        s = SLOT[RADIX * b]
        c, n = tw_ref[s, 0:1, :], tw_ref[s, 1:2, :]
        if b in (0, half):
            put_split(cut_ref, s * ROWS, zero[b] * c, zero[b] * n)
        else:
            emit(RADIX * b, zero[b])
    for a in range(1, half):
        base = 2 * RADIX * a
        items = [turn((mid_ref[base + 2 * j2], mid_ref[base + 2 * j2 + 1]), -a * j2, wide) for j2 in range(RADIX)]
        for b, value in enumerate(fourier(items, -1)):
            emit(a + RADIX * b, value)
    four = [mid_ref[2 * j2 + 1] for j2 in range(RADIX)]
    for b in range(half):
        k = half + RADIX * b
        re, im = four[0], None
        for j2 in range(1, RADIX):
            angle = 2 * math.pi * (k * j2 % wide) / wide
            re = re + four[j2] * math.cos(angle)
            term = four[j2] * -math.sin(angle)
            im = term if im is None else im + term
        emit(k, (re, im))

    for s in range(KEEP):
        re = im = None
        for piece, taps in enumerate(wave):
            c, n = tw_ref[s, 4 + 2 * piece : 5 + 2 * piece, :], tw_ref[s, 5 + 2 * piece : 6 + 2 * piece, :]
            re = taps * c if re is None else re + taps * c
            im = taps * n if im is None else im + taps * n
        put_split(cut_ref, (KEEP + s) * ROWS, re, im)

    spec_ref[...] = jnp.dot(cut_ref[...], fwd_ref[...], preferred_element_type=jnp.float32)

    def apply(s, carry):
        at = pl.multiple_of(s * ROWS, ROWS)
        other = pl.multiple_of((KEEP + s) * ROWS, ROWS)
        xr, xi = spec_ref[pl.ds(at, ROWS), 0:LANES], spec_ref[pl.ds(at, ROWS), LANES:]
        hr, hi = spec_ref[pl.ds(other, ROWS), 0:LANES], spec_ref[pl.ds(other, ROWS), LANES:]
        scale = 1.0 / (hr * hr + hi * hi + floor)
        put_split(cut_ref, at, (xr * hr + xi * hi) * scale, (xi * hr - xr * hi) * scale)
        return carry

    lax.fori_loop(0, KEEP, apply, 0, unroll=3)
    rows = KEEP * ROWS
    spec_ref[0:rows] = jnp.dot(cut_ref[0:rows], inv_ref[...], preferred_element_type=jnp.float32)

    def fetch(k):
        s = SLOT[k]
        re, im = spec_ref[s * ROWS : (s + 1) * ROWS, 0:LANES], spec_ref[s * ROWS : (s + 1) * ROWS, LANES:]
        c, n = tw_ref[s, 2:3, :], tw_ref[s, 3:4, :]
        if k in (0, wide // 2):
            return re * c - im * n
        return (re * c - im * n, re * n + im * c)

    for a in range(1, half):
        base = 2 * RADIX * a
        for j2, value in enumerate(fourier([fetch(a + RADIX * b) for b in range(RADIX)], 1)):
            value = turn(value, a * j2, wide)
            mid_ref[base + 2 * j2] = value[0]
            mid_ref[base + 2 * j2 + 1] = value[1]
    for j2, value in enumerate(eight_real(*[fetch(RADIX * b) for b in range(half + 1)])):
        mid_ref[2 * j2] = value
    four = [fetch(half + RADIX * b) for b in range(half)]
    for j2 in range(RADIX):
        total = None
        for b, value in enumerate(four):
            angle = 2 * math.pi * ((half + RADIX * b) * j2 % wide) / wide
            term = value[0] * math.cos(angle)
            if j2:
                term = term - value[1] * math.sin(angle)
            total = term if total is None else total + term
        mid_ref[2 * j2 + 1] = total
    for j2 in range(RADIX):
        parts = [mid_ref[2 * j2]]
        for a in range(1, half):
            base = 2 * RADIX * a
            parts.append((mid_ref[base + 2 * j2], mid_ref[base + 2 * j2 + 1]))
        parts.append(mid_ref[2 * j2 + 1])
        for j1, value in enumerate(eight_real(*parts)):
            write(RADIX * j1 + j2, value)


def slabs(ref, lead):
    def at(j):
        return lead + (slice(None), slice(j * LANES, (j + 1) * LANES))

    def read(j):
        value = ref[at(j)]
        return value.reshape(ROWS, LANES)

    def write(j, value):
        ref[at(j)] = value.reshape(ref[at(j)].shape)

    return read, write


def block_kernel(taps, lead, x_ref, w_ref, fwd_ref, inv_ref, tw_ref, o_ref, mid_ref, cut_ref, spec_ref):
    read, _ = slabs(x_ref, lead)
    _, write = slabs(o_ref, (slice(None),) * (len(o_ref.shape) - 2))
    wave = [w_ref[:, p * LANES : (p + 1) * LANES] for p in range(taps // LANES)]
    deconvolve(read, write, wave, w_ref[:, taps : taps + LANES], fwd_ref, inv_ref, tw_ref, mid_ref, cut_ref, spec_ref)


def split_count(n):
    inner = 1
    while inner * inner < n:
        inner *= 2
    return (n // inner, inner) if n % inner == 0 else (1, n)


def block_order(n):
    inner = split_count(n)[1]
    raws = list(range(n - inner + 1, n, 2))[:2]
    kept = list(range(n - inner, n, 2))[1::-1]
    near = sorted(range(1, n // 2), key=lambda k: (k < inner, k))
    cross = [k for k in range(n // 2, n) if k not in raws + kept]
    return cross + near + kept + raws + [0], raws, kept


def keeps_blocks(me, n):
    outer, inner = split_count(n)
    far = lax.div(me, inner)
    return jnp.logical_and(me % 2 == 0, jnp.logical_or(far == outer // 2 - 1, far == outer // 2))


def exchange_kernel(
    n,
    taps,
    x_ref,
    pick_ref,
    wave_ref,
    damp_ref,
    fwd_hbm,
    inv_hbm,
    tw_hbm,
    buf_ref,
    mid_ref,
    cut_ref,
    spec_ref,
    fwd_ref,
    inv_ref,
    tw_ref,
    bank_ref,
    rows_ref,
    stage_ref,
    pick_smem,
    damp_smem,
    stage_sem,
    load_sems,
    near_sems,
    raw_sems,
    pick_sems,
    bank_sends,
    bank_recvs,
    ready_sems,
    sends,
    recvs,
):
    me = lax.axis_index("traces")
    own, each = wave_ref.shape[0], x_ref.shape[0] // n
    outer, inner = split_count(n)
    far, near = lax.div(me, inner), lax.rem(me, inner)
    halves, pieces = own // SUBLANES, taps // LANES
    last = halves * pieces

    def remote(src, dst, send_sem, recv_sem, device):
        return pltpu.make_async_remote_copy(
            src_ref=src,
            dst_ref=dst,
            send_sem=send_sem,
            recv_sem=recv_sem,
            device_id={"traces": device},
            device_id_type=pl.DeviceIdType.MESH,
        )

    def block_of(e):
        return x_ref.at[pl.ds(pl.multiple_of(e * each, each), each)]

    turns, raws, kept = block_order(n)
    partner = me ^ raws[0]
    made = n - 1 - len(raws)
    sent_here = made - jnp.where(keeps_blocks(me, n), len(kept), 0)

    def turn_of(s):
        k = 0
        for i, turn in enumerate(turns):
            k = jnp.where(s == i, turn, k)
        return k

    barrier = pltpu.get_barrier_semaphore()

    def tell(sem, other):
        pl.semaphore_signal(sem, inc=1, device_id={"traces": other}, device_id_type=pl.DeviceIdType.MESH)

    def greet(other, carry):
        tell(barrier, other)
        return carry

    def answer(other, carry):
        @pl.when(other != partner)
        def _():
            tell(ready_sems.at[me], other)

        return carry

    def meet(other, carry):
        @pl.when(other != partner)
        def _():
            pl.semaphore_wait(ready_sems.at[other], 1)

        return carry

    def raw(i, part, here):
        first, count, other = part * (each // 2), each // 2, me ^ raws[i]
        rows = x_ref.at[pl.ds(pl.multiple_of(other * each + first, count), count)]
        there = buf_ref.at[n + jnp.where(here, other, me), pl.ds(first, count)]
        return remote(rows, there, raw_sems.at[0, i, part], raw_sems.at[1, i, part], other)

    def raw_staged():
        there = buf_ref.at[n + me, pl.ds(0, each // 2)]
        return remote(stage_ref, there, raw_sems.at[0, 0, 0], raw_sems.at[1, 0, 0], partner)

    stage = pl.ds(pl.multiple_of(partner * each, each // 2), each // 2)
    stage_in = pltpu.make_async_copy(x_ref.at[stage], stage_ref, stage_sem)

    stage_in.start()
    lax.fori_loop(me + 1, n, greet, 0)

    @pl.when(me > 0)
    def _():
        pl.semaphore_wait(barrier, me)

    @pl.when(partner < me)
    def _():
        tell(ready_sems.at[me], partner)
        stage_in.wait()
        raw_staged().start()

    damp_in = pltpu.make_async_copy(damp_ref, damp_smem, near_sems.at[0])
    pick_in = pltpu.make_async_copy(pick_ref, pick_smem.at[pl.ds(0, n * each)], near_sems.at[1])
    tables_in = [
        pltpu.make_async_copy(there, here, near_sems.at[2 + i])
        for i, (there, here) in enumerate(((fwd_hbm, fwd_ref), (inv_hbm, inv_ref), (tw_hbm, tw_ref)))
    ]
    tiles_in = [
        pltpu.make_async_copy(
            wave_ref.at[pl.ds(h * SUBLANES, SUBLANES), pl.ds(p * LANES, LANES)],
            bank_ref.at[me, pl.ds((h * pieces + p) * SUBLANES, SUBLANES)],
            near_sems.at[5 + h * pieces + p],
        )
        for h in range(halves)
        for p in range(pieces)
    ]
    for copy in [damp_in] + tiles_in + [pick_in] + tables_in:
        copy.start()

    def load(e):
        return pltpu.make_async_copy(block_of(e), buf_ref.at[n + e], load_sems.at[e])

    def load_start(s, carry):
        @pl.when(jnp.logical_or(s < made, s == n - 1))
        def _():
            load(me ^ turn_of(s)).start()

        return carry

    def picks(i):
        count = n * each
        there = pick_smem.at[pl.ds((1 + i) * count, count)]
        return remote(pick_ref, there, pick_sems.at[0, i], pick_sems.at[1, i], me ^ raws[i])

    @pl.when(partner > me)
    def _():
        stage_in.wait()
        pl.semaphore_wait(ready_sems.at[partner], 1)
        raw_staged().start()

    lax.fori_loop(0, me, answer, 0)
    damp_in.wait()
    lane = lax.broadcasted_iota(jnp.int32, (SUBLANES, LANES), 1)
    levels = jnp.zeros((SUBLANES, LANES), jnp.float32)
    for f in range(own):
        levels = jnp.where(lane == f, damp_smem[f], levels)
    bank_ref[me, last * SUBLANES : (last + 1) * SUBLANES, :] = levels
    lax.fori_loop(me + 1, n, meet, 0)
    for copy in tiles_in:
        copy.wait()

    def bank_copy(block, slot, there):
        used = bank_ref.at[block, pl.ds(0, last * SUBLANES + 1)]
        return remote(used, used, bank_sends.at[slot], bank_recvs.at[block], there)

    def block_at(f):
        return f * inner + near

    middle = outer // 2
    upper = far >= middle
    gate = jnp.where(upper, middle, middle - 1)

    def across(t, act):
        there = lax.rem(far + t, outer)
        direct = jnp.logical_or((there >= middle) == upper, there == outer - 1 - gate)

        @pl.when(direct)
        def _():
            act(bank_copy(me, t - 1, block_at(there)))

    def onward(t, act):
        block = lax.rem(far + t, outer)
        for there in range(outer):
            slot = outer - 1 + (t - 1) * outer + there
            near_side = (there >= middle) == upper
            foreign = (block >= middle) != upper
            go = jnp.logical_and(jnp.logical_and(far == gate, far != there), jnp.logical_and(near_side, foreign))

            @pl.when(go)
            def _():
                act(bank_copy(block_at(block), slot, block_at(there)))

    def spread(f, act):
        for d in range(1, inner):
            slot = outer * outer - 1 + f * (inner - 1) + d - 1
            act(bank_copy(block_at(f), slot, far * inner + (near ^ d)))

    def bank_came(block):
        bank_copy(block, 0, partner).wait_recv()

    start, sent = (lambda copy: copy.start()), (lambda copy: copy.wait_send())
    for t in range(1, outer):
        across(t, start)
    spread(far, start)
    raw(0, 1, False).start()
    for i in range(1, len(raws)):
        raw(i, 0, False).start()
        raw(i, 1, False).start()
    for i in range(len(raws)):
        picks(i).start()
    lax.fori_loop(0, n, load_start, 0)
    for t in range(1, outer):
        block = lax.rem(far + t, outer)
        bank_came(block_at(block))
        onward(t, start)
        spread(block, start)
    for f in range(outer):
        for d in range(1, inner):
            bank_came(f * inner + (near ^ d))
    pick_in.wait()
    for copy in tables_in:
        copy.wait()

    def send(e):
        return remote(buf_ref.at[n + e], buf_ref.at[me], sends.at[e], recvs.at[me], e)

    row_lane = lax.broadcasted_iota(jnp.int32, (1, LANES), 1)

    def step(s, carry):
        e = me ^ turn_of(s)
        theirs = jnp.logical_and(s >= made, s < n - 1)
        for i in range(len(raws)):

            @pl.when(s == made + i)
            def _():
                raw(i, 0, True).wait_recv()
                raw(i, 1, True).wait_recv()
                picks(i).wait_recv()

        @pl.when(jnp.logical_not(theirs))
        def _():
            load(e).wait()

        table = jnp.where(theirs, s - made + 1, 0)
        base = (table * n + jnp.where(theirs, me, e)) * each
        for r in range(ROWS):
            pick = pick_smem[base + r]
            block, inside = lax.div(pick, own), lax.rem(pick, own)
            at = lax.div(inside, SUBLANES) * (pieces * SUBLANES) + lax.rem(inside, SUBLANES)
            for p in range(pieces):
                rows_ref[r : r + 1, p * LANES : (p + 1) * LANES] = bank_ref[block, pl.ds(at + p * SUBLANES, 1), :]
            level = bank_ref[block, last * SUBLANES : last * SUBLANES + 1, :]
            rows_ref[r : r + 1, taps : taps + LANES] = jnp.where(row_lane == inside, level, 0.0)

        @pl.when(jnp.logical_and(s >= 1, s <= sent_here))
        def _():
            send(me ^ turn_of(s - 1)).start()

        slot = jnp.where(s >= made, e, n + e)
        wave = [rows_ref[:, p * LANES : (p + 1) * LANES] for p in range(pieces)]
        power = sum(jnp.sum(w * w, axis=1, keepdims=True) for w in wave)
        damp = jnp.sum(rows_ref[:, taps : taps + LANES], axis=1, keepdims=True)
        floor = jnp.broadcast_to(damp * (power + 1e-6), (ROWS, LANES))

        def read(j):
            return buf_ref[n + e, :, j * LANES : (j + 1) * LANES]

        def write(j, value):
            buf_ref[slot, :, j * LANES : (j + 1) * LANES] = value

        deconvolve(read, write, wave, floor, fwd_ref, inv_ref, tw_ref, mid_ref, cut_ref, spec_ref)
        return carry

    lax.fori_loop(0, n, step, 0)

    for i in range(len(raws)):
        raw(i, 0, False).wait_send()
        raw(i, 1, False).wait_send()
        picks(i).wait_send()
    for t in range(1, outer):
        across(t, sent)
        onward(t, sent)
    for f in range(outer):
        spread(f, sent)

    def finish(s, carry):
        e = me ^ turn_of(s)
        send(e).wait_send()
        remote(buf_ref.at[e], buf_ref.at[e], sends.at[e], recvs.at[e], e).wait_recv()
        return carry

    lax.fori_loop(0, sent_here, finish, 0)


def late_kernel(n, buf_ref, after_ref, late_ref, sends, recvs):
    del after_ref
    me = lax.axis_index("traces")
    kept = block_order(n)[2]

    @pl.when(keeps_blocks(me, n))
    def _():
        barrier = pltpu.get_barrier_semaphore()
        for k in kept:
            pl.semaphore_signal(barrier, inc=1, device_id={"traces": me ^ k}, device_id_type=pl.DeviceIdType.MESH)
        pl.semaphore_wait(barrier, len(kept))
        copies = [
            pltpu.make_async_remote_copy(
                src_ref=buf_ref.at[n + (me ^ k)],
                dst_ref=late_ref.at[i],
                send_sem=sends.at[i],
                recv_sem=recvs.at[i],
                device_id={"traces": me ^ k},
                device_id_type=pl.DeviceIdType.MESH,
            )
            for i, k in enumerate(kept)
        ]
        for copy in copies:
            copy.start()
        for copy in copies:
            copy.wait()


def settle_kernel(n, order_ref, came_ref, o_ref, late_rows_ref, sem):
    rows = o_ref.shape[0]
    each = rows // n
    shift = n.bit_length() - 1
    me = lax.axis_index("traces")
    kept = block_order(n)[2]
    keeps = keeps_blocks(me, n)

    def put(d, carry):
        for r in range(each):
            q = d * each + r
            place = order_ref[q]
            source, row = place & (n - 1), place >> shift
            turn = source ^ me
            late = jnp.logical_and(keeps, functools.reduce(jnp.logical_or, [turn == k for k in kept]))

            @pl.when(late)
            def _():
                index = functools.reduce(lambda at, ik: jnp.where(turn == ik[1], ik[0], at), enumerate(kept), 0)
                late_rows_ref[index * each + row] = q

            @pl.when(jnp.logical_not(late))
            def _():
                pltpu.make_async_copy(came_ref.at[source, pl.ds(row, 1)], o_ref.at[pl.ds(q, 1)], sem).start()

        return carry

    lax.fori_loop(0, n, put, 0)

    def finish(count):
        pltpu.make_async_copy(o_ref.at[pl.ds(0, count)], o_ref.at[pl.ds(0, count)], sem).wait()

    @pl.when(keeps)
    def _():
        finish(rows - len(kept) * each)

    @pl.when(jnp.logical_not(keeps))
    def _():
        finish(rows)


def last_kernel(n, late_rows_ref, late_ref, settled_ref, o_ref, sem):
    del settled_ref
    count, each, _ = late_ref.shape

    @pl.when(keeps_blocks(lax.axis_index("traces"), n))
    def _():
        for i in range(count):
            for r in range(each):
                q = late_rows_ref[i * each + r]
                pltpu.make_async_copy(late_ref.at[i, pl.ds(r, 1)], o_ref.at[pl.ds(q, 1)], sem).start()
        part = o_ref.at[pl.ds(0, count * each)]
        pltpu.make_async_copy(part, part, sem).wait()


def tables(length, taps):
    return (
        jnp.asarray(lane_matrix(-1.0, 1.0)),
        jnp.asarray(lane_matrix(1.0, 1.0 / length)),
        jnp.asarray(twiddles(length, taps)),
    )


def scratch():
    return [
        pltpu.VMEM((RADIX * RADIX, ROWS, LANES), jnp.float32),
        pltpu.VMEM((2 * KEEP * ROWS, 6 * LANES), jnp.bfloat16),
        pltpu.VMEM((2 * KEEP * ROWS, 2 * LANES), jnp.float32),
    ]


def gathered(raw_traces, filter_index, channel_order, wavelets, damping):
    rows, length = raw_traces.shape
    own, taps = wavelets.shape
    n = lax.axis_size("traces")
    me = lax.axis_index("traces")
    each = rows // n
    floor = damping * (jnp.sum(wavelets * wavelets, axis=1) + 1e-6)
    picks = filter_index.reshape(own, rows // own).astype(jnp.float32)
    packed = lax.all_gather(jnp.concatenate([wavelets, floor[:, None], picks], axis=1), "traces", axis=0, tiled=True)
    all_picks = packed[:, taps + 1 :].reshape(n, n, each).astype(jnp.int32)
    came_picks = lax.dynamic_index_in_dim(all_picks, me, 1, keepdims=False)
    bank = jnp.concatenate([packed[:, :taps], jnp.broadcast_to(packed[:, taps : taps + 1], (own * n, LANES))], axis=1)
    fwd, inv, tw = tables(length, taps)
    whole = lambda a: pl.BlockSpec(a.shape, lambda i, *_: (0,) * a.ndim)
    fixed = [pl.BlockSpec((ROWS, taps + LANES), lambda i, *_: (i, 0)), whole(fwd), whole(inv), whole(tw)]
    came = lax.all_to_all(raw_traces.reshape(n, each, length), "traces", 0, 0, tiled=True).reshape(rows, length)
    result = pl.pallas_call(
        functools.partial(block_kernel, taps, ()),
        grid=(rows // ROWS,),
        out_shape=jax.ShapeDtypeStruct((rows, length), jnp.float32),
        in_specs=[pl.BlockSpec((ROWS, length), lambda i: (i, 0))] + fixed,
        out_specs=pl.BlockSpec((ROWS, length), lambda i: (i, 0)),
        scratch_shapes=scratch(),
        compiler_params=pltpu.CompilerParams(vmem_limit_bytes=48 * 1024 * 1024),
    )(came, jnp.take(bank, came_picks.reshape(-1), axis=0), fwd, inv, tw)
    return jnp.take(result, (channel_order % n) * each + channel_order // n, axis=0)


def local(raw_traces, filter_index, channel_order, wavelets, damping):
    rows, length = raw_traces.shape
    own, taps = wavelets.shape
    n = lax.axis_size("traces")
    if n < 4 or n & (n - 1) or rows != n * ROWS or own % SUBLANES or own > LANES or taps % LANES:
        return gathered(raw_traces, filter_index, channel_order, wavelets, damping)

    fwd, inv, tw = tables(length, taps)
    tiles = own // SUBLANES * (taps // LANES)
    outer = split_count(n)[0]
    _, raws, kept = block_order(n)
    raws, kept = len(raws), len(kept)
    dma = pltpu.SemaphoreType.DMA
    came = pl.pallas_call(
        functools.partial(exchange_kernel, n, taps),
        in_specs=[pl.BlockSpec(memory_space=pltpu.HBM)] * 7,
        out_specs=pl.BlockSpec(memory_space=pltpu.VMEM),
        out_shape=pltpu.VMEM((2 * n, ROWS, length), jnp.float32),
        scratch_shapes=scratch()
        + [pltpu.VMEM(a.shape, a.dtype) for a in (fwd, inv, tw)]
        + [
            pltpu.VMEM((n, (tiles + 1) * SUBLANES, LANES), jnp.float32),
            pltpu.VMEM((ROWS, taps + LANES), jnp.float32),
            pltpu.VMEM((ROWS // 2, length), jnp.float32),
            pltpu.SMEM(((1 + raws) * rows,), jnp.int32),
            pltpu.SMEM((own,), jnp.float32),
            dma,
            dma((n,)),
            dma((5 + tiles,)),
            dma((2, raws, 2)),
            dma((2, raws)),
            dma((outer * outer - 1 + n - outer,)),
            dma((n,)),
            pltpu.SemaphoreType.REGULAR((n,)),
            dma((n,)),
            dma((n,)),
        ],
        compiler_params=pltpu.CompilerParams(
            collective_id=0, has_side_effects=True, vmem_limit_bytes=40 * 1024 * 1024
        ),
        cost_estimate=pl.CostEstimate(flops=rows * length * 1500, bytes_accessed=8 * rows * length, transcendentals=0),
    )(raw_traces, filter_index, wavelets, damping, fwd, inv, tw)
    came = pltpu.with_memory_space_constraint(came, pltpu.VMEM)
    smem, vmem, hbm = (pl.BlockSpec(memory_space=m) for m in (pltpu.SMEM, pltpu.VMEM, pltpu.HBM))
    params = pltpu.CompilerParams(vmem_limit_bytes=20 * 1024 * 1024)
    settled, late_rows = pl.pallas_call(
        functools.partial(settle_kernel, n),
        in_specs=[smem, vmem],
        out_specs=[hbm, smem],
        out_shape=[
            jax.ShapeDtypeStruct((rows, length), jnp.float32),
            pltpu.SMEM((kept * ROWS,), jnp.int32),
        ],
        scratch_shapes=[dma],
        compiler_params=params,
    )(channel_order, came)
    late_rows = pltpu.with_memory_space_constraint(late_rows, pltpu.SMEM)
    late = pl.pallas_call(
        functools.partial(late_kernel, n),
        in_specs=[vmem, smem],
        out_specs=vmem,
        out_shape=pltpu.VMEM((kept, ROWS, length), jnp.float32),
        scratch_shapes=[dma((kept,)), dma((kept,))],
        compiler_params=pltpu.CompilerParams(
            collective_id=1, has_side_effects=True, vmem_limit_bytes=20 * 1024 * 1024
        ),
    )(came, late_rows)
    late = pltpu.with_memory_space_constraint(late, pltpu.VMEM)
    return pl.pallas_call(
        functools.partial(last_kernel, n),
        in_specs=[smem, vmem, hbm],
        out_specs=hbm,
        out_shape=jax.ShapeDtypeStruct((rows, length), jnp.float32),
        scratch_shapes=[dma],
        input_output_aliases={2: 0},
        compiler_params=params,
    )(late_rows, late, settled)


def solution(mesh):
    placed = (
        P(("groups", "traces"), None),
        P(("groups", "traces")),
        P("groups"),
        P("traces", None),
        P("traces"),
    )
    return jax.shard_map(
        local, mesh=mesh, in_specs=placed, out_specs=P(("groups", "traces"), None), check_vma=False
    )
```

```python
import functools
import math

import jax
import jax.numpy as jnp
import numpy as np
from jax import lax
from jax.experimental import pallas as pl
from jax.experimental.pallas import tpu as pltpu
from jax.sharding import PartitionSpec as P

LANES = 128
RADIX = 8
ROWS = 16
SUBLANES = 8

KEPT = (
    [RADIX * b for b in range(RADIX // 2 + 1)]
    + [a + RADIX * b for a in range(1, RADIX // 2) for b in range(RADIX)]
    + [RADIX // 2 + RADIX * b for b in range(RADIX // 2)]
)
SLOT = {k: s for s, k in enumerate(KEPT)}
KEEP = len(KEPT)


def lane_matrix(sign, scale):
    ids = np.arange(LANES)
    angle = 2.0 * np.pi * (np.outer(ids, ids) % LANES) / LANES
    c, s = np.cos(angle) * scale, sign * np.sin(angle) * scale
    full = np.block([[c, s], [-s, c]])
    import ml_dtypes

    high = full.astype(np.float32).astype(ml_dtypes.bfloat16)
    low = (full.astype(np.float32) - high.astype(np.float32)).astype(ml_dtypes.bfloat16)
    return np.concatenate([high, high, low], axis=0)


def twiddles(length, taps):
    m = np.arange(LANES)
    rows = []
    for k in KEPT:
        angle = 2.0 * np.pi * k * m / length
        row = [np.cos(angle), -np.sin(angle)]
        weight = 1.0 if k in (0, RADIX * RADIX // 2) else 2.0
        row += [weight * np.cos(angle), weight * np.sin(angle)]
        for piece in range(taps // LANES):
            shifted = 2.0 * np.pi * k * (m + LANES * piece) / length
            row += [np.cos(shifted), -np.sin(shifted)]
        rows.append(np.stack(row))
    return np.stack(rows).astype(np.float32)


def cadd(a, b):
    return (a[0] + b[0], a[1] + b[1])


def csub(a, b):
    return (a[0] - b[0], a[1] - b[1])


def turn(a, num, den):
    num %= den
    if num == 0:
        return a
    if 4 * num == den:
        return (-a[1], a[0])
    if 2 * num == den:
        return (-a[0], -a[1])
    if 4 * num == 3 * den:
        return (a[1], -a[0])
    c, s = math.cos(2 * math.pi * num / den), math.sin(2 * math.pi * num / den)
    return (a[0] * c - a[1] * s, a[0] * s + a[1] * c)


def fourier(items, sign):
    n = len(items)
    if n == 1:
        return items
    even, odd = fourier(items[0::2], sign), fourier(items[1::2], sign)
    turned = [turn(o, sign * k, n) for k, o in enumerate(odd)]
    return [cadd(e, t) for e, t in zip(even, turned)] + [csub(e, t) for e, t in zip(even, turned)]


def real_eight(v):
    h = math.sqrt(0.5)
    s0, d0, s1, d1 = v[0] + v[4], v[0] - v[4], v[1] + v[5], v[1] - v[5]
    s2, d2, s3, d3 = v[2] + v[6], v[2] - v[6], v[3] + v[7], v[3] - v[7]
    p, q = s0 + s2, s1 + s3
    r, t = (d1 - d3) * h, (d1 + d3) * h
    return [p + q, (d0 + r, -(d2 + t)), (s0 - s2, s3 - s1), (d0 - r, d2 - t), p - q]


def eight_real(u0, u1, u2, u3, u4):
    h = math.sqrt(0.5)
    p, q = u0 + u4, u0 - u4
    e = [p + u2[0], q - u2[1], p - u2[0], q + u2[1]]
    f, g = u1[0] - u3[0], u1[1] + u3[1]
    o = [u1[0] + u3[0], (f - g) * h, u3[1] - u1[1], -(f + g) * h]
    return [a + b for a, b in zip(e, o)] + [a - b for a, b in zip(e, o)]


def put_split(ref, base, re, im):
    rows = pl.ds(base, ROWS)
    for part, value in enumerate((re, im)):
        high = value.astype(jnp.bfloat16)
        low = (value - high.astype(jnp.float32)).astype(jnp.bfloat16)
        at = part * LANES
        ref[rows, at : at + LANES] = high
        ref[rows, 2 * LANES + at : 2 * LANES + at + LANES] = low
        ref[rows, 4 * LANES + at : 4 * LANES + at + LANES] = high


def deconvolve(read, write, wave, floor, fwd_ref, inv_ref, tw_ref, mid_ref, cut_ref, spec_ref):
    half, wide = RADIX // 2, RADIX * RADIX
    for j2 in range(RADIX):
        out = real_eight([read(RADIX * j1 + j2) for j1 in range(RADIX)])
        mid_ref[2 * j2] = out[0]
        mid_ref[2 * j2 + 1] = out[half]
        for a in range(1, half):
            mid_ref[2 * RADIX * a + 2 * j2] = out[a][0]
            mid_ref[2 * RADIX * a + 2 * j2 + 1] = out[a][1]

    def emit(k, value):
        s = SLOT[k]
        c, n = tw_ref[s, 0:1, :], tw_ref[s, 1:2, :]
        put_split(cut_ref, s * ROWS, value[0] * c - value[1] * n, value[0] * n + value[1] * c)

    zero = real_eight([mid_ref[2 * j2] for j2 in range(RADIX)])
    c, n = tw_ref[0, 0:1, :], tw_ref[0, 1:2, :]
    for b in range(half + 1):
        s = SLOT[RADIX * b]
        c, n = tw_ref[s, 0:1, :], tw_ref[s, 1:2, :]
        if b in (0, half):
            put_split(cut_ref, s * ROWS, zero[b] * c, zero[b] * n)
        else:
            emit(RADIX * b, zero[b])
    for a in range(1, half):
        base = 2 * RADIX * a
        items = [turn((mid_ref[base + 2 * j2], mid_ref[base + 2 * j2 + 1]), -a * j2, wide) for j2 in range(RADIX)]
        for b, value in enumerate(fourier(items, -1)):
            emit(a + RADIX * b, value)
    four = [mid_ref[2 * j2 + 1] for j2 in range(RADIX)]
    for b in range(half):
        k = half + RADIX * b
        re, im = four[0], None
        for j2 in range(1, RADIX):
            angle = 2 * math.pi * (k * j2 % wide) / wide
            re = re + four[j2] * math.cos(angle)
            term = four[j2] * -math.sin(angle)
            im = term if im is None else im + term
        emit(k, (re, im))

    for s in range(KEEP):
        re = im = None
        for piece, taps in enumerate(wave):
            c, n = tw_ref[s, 4 + 2 * piece : 5 + 2 * piece, :], tw_ref[s, 5 + 2 * piece : 6 + 2 * piece, :]
            re = taps * c if re is None else re + taps * c
            im = taps * n if im is None else im + taps * n
        put_split(cut_ref, (KEEP + s) * ROWS, re, im)

    spec_ref[...] = jnp.dot(cut_ref[...], fwd_ref[...], preferred_element_type=jnp.float32)

    def apply(s, carry):
        at = pl.multiple_of(s * ROWS, ROWS)
        other = pl.multiple_of((KEEP + s) * ROWS, ROWS)
        xr, xi = spec_ref[pl.ds(at, ROWS), 0:LANES], spec_ref[pl.ds(at, ROWS), LANES:]
        hr, hi = spec_ref[pl.ds(other, ROWS), 0:LANES], spec_ref[pl.ds(other, ROWS), LANES:]
        scale = 1.0 / (hr * hr + hi * hi + floor)
        put_split(cut_ref, at, (xr * hr + xi * hi) * scale, (xi * hr - xr * hi) * scale)
        return carry

    lax.fori_loop(0, KEEP, apply, 0, unroll=3)
    rows = KEEP * ROWS
    spec_ref[0:rows] = jnp.dot(cut_ref[0:rows], inv_ref[...], preferred_element_type=jnp.float32)

    def fetch(k):
        s = SLOT[k]
        re, im = spec_ref[s * ROWS : (s + 1) * ROWS, 0:LANES], spec_ref[s * ROWS : (s + 1) * ROWS, LANES:]
        c, n = tw_ref[s, 2:3, :], tw_ref[s, 3:4, :]
        if k in (0, wide // 2):
            return re * c - im * n
        return (re * c - im * n, re * n + im * c)

    for a in range(1, half):
        base = 2 * RADIX * a
        for j2, value in enumerate(fourier([fetch(a + RADIX * b) for b in range(RADIX)], 1)):
            value = turn(value, a * j2, wide)
            mid_ref[base + 2 * j2] = value[0]
            mid_ref[base + 2 * j2 + 1] = value[1]
    for j2, value in enumerate(eight_real(*[fetch(RADIX * b) for b in range(half + 1)])):
        mid_ref[2 * j2] = value
    four = [fetch(half + RADIX * b) for b in range(half)]
    for j2 in range(RADIX):
        total = None
        for b, value in enumerate(four):
            angle = 2 * math.pi * ((half + RADIX * b) * j2 % wide) / wide
            term = value[0] * math.cos(angle)
            if j2:
                term = term - value[1] * math.sin(angle)
            total = term if total is None else total + term
        mid_ref[2 * j2 + 1] = total
    for j2 in range(RADIX):
        parts = [mid_ref[2 * j2]]
        for a in range(1, half):
            base = 2 * RADIX * a
            parts.append((mid_ref[base + 2 * j2], mid_ref[base + 2 * j2 + 1]))
        parts.append(mid_ref[2 * j2 + 1])
        for j1, value in enumerate(eight_real(*parts)):
            write(RADIX * j1 + j2, value)


def slabs(ref, lead):
    def at(j):
        return lead + (slice(None), slice(j * LANES, (j + 1) * LANES))

    def read(j):
        value = ref[at(j)]
        return value.reshape(ROWS, LANES)

    def write(j, value):
        ref[at(j)] = value.reshape(ref[at(j)].shape)

    return read, write


def block_kernel(taps, lead, x_ref, w_ref, fwd_ref, inv_ref, tw_ref, o_ref, mid_ref, cut_ref, spec_ref):
    read, _ = slabs(x_ref, lead)
    _, write = slabs(o_ref, (slice(None),) * (len(o_ref.shape) - 2))
    wave = [w_ref[:, p * LANES : (p + 1) * LANES] for p in range(taps // LANES)]
    deconvolve(read, write, wave, w_ref[:, taps : taps + LANES], fwd_ref, inv_ref, tw_ref, mid_ref, cut_ref, spec_ref)


def split_count(n):
    inner = 1
    while inner * inner < n:
        inner *= 2
    return (n // inner, inner) if n % inner == 0 else (1, n)


def block_order(n):
    inner = split_count(n)[1]
    raws = list(range(n - inner + 1, n, 2))[:2]
    kept = list(range(n - inner, n, 2))[:2]
    near = sorted(range(1, n // 2), key=lambda k: (k < inner, k))
    cross = [k for k in range(n // 2, n) if k not in raws + kept]
    return cross + near + kept + raws + [0], raws, kept


def keeps_blocks(me, n):
    outer, inner = split_count(n)
    far = lax.div(me, inner)
    return jnp.logical_and(me % 2 == 0, jnp.logical_or(far == outer // 2 - 1, far == outer // 2))


def exchange_kernel(
    n,
    taps,
    x_ref,
    pick_ref,
    wave_ref,
    damp_ref,
    fwd_hbm,
    inv_hbm,
    tw_hbm,
    buf_ref,
    mid_ref,
    cut_ref,
    spec_ref,
    fwd_ref,
    inv_ref,
    tw_ref,
    bank_ref,
    rows_ref,
    stage_ref,
    pick_smem,
    damp_smem,
    stage_sem,
    load_sems,
    near_sems,
    raw_sems,
    pick_sems,
    bank_sends,
    bank_recvs,
    ready_sems,
    sends,
    recvs,
):
    me = lax.axis_index("traces")
    own, each = wave_ref.shape[0], x_ref.shape[0] // n
    outer, inner = split_count(n)
    far, near = lax.div(me, inner), lax.rem(me, inner)
    halves, pieces = own // SUBLANES, taps // LANES
    last = halves * pieces

    def remote(src, dst, send_sem, recv_sem, device):
        return pltpu.make_async_remote_copy(
            src_ref=src,
            dst_ref=dst,
            send_sem=send_sem,
            recv_sem=recv_sem,
            device_id={"traces": device},
            device_id_type=pl.DeviceIdType.MESH,
        )

    def block_of(e):
        return x_ref.at[pl.ds(pl.multiple_of(e * each, each), each)]

    turns, raws, kept = block_order(n)
    partner = me ^ raws[0]
    made = n - 1 - len(raws)
    sent_here = made - jnp.where(keeps_blocks(me, n), len(kept), 0)

    def turn_of(s):
        k = 0
        for i, turn in enumerate(turns):
            k = jnp.where(s == i, turn, k)
        return k

    barrier = pltpu.get_barrier_semaphore()

    def tell(sem, other):
        pl.semaphore_signal(sem, inc=1, device_id={"traces": other}, device_id_type=pl.DeviceIdType.MESH)

    def greet(other, carry):
        tell(barrier, other)
        return carry

    def answer(other, carry):
        @pl.when(other != partner)
        def _():
            tell(ready_sems.at[me], other)

        return carry

    def meet(other, carry):
        @pl.when(other != partner)
        def _():
            pl.semaphore_wait(ready_sems.at[other], 1)

        return carry

    def raw(i, part, here):
        first, count, other = part * (each // 2), each // 2, me ^ raws[i]
        rows = x_ref.at[pl.ds(pl.multiple_of(other * each + first, count), count)]
        there = buf_ref.at[n + jnp.where(here, other, me), pl.ds(first, count)]
        return remote(rows, there, raw_sems.at[0, i, part], raw_sems.at[1, i, part], other)

    def raw_staged():
        there = buf_ref.at[n + me, pl.ds(0, each // 2)]
        return remote(stage_ref, there, raw_sems.at[0, 0, 0], raw_sems.at[1, 0, 0], partner)

    stage = pl.ds(pl.multiple_of(partner * each, each // 2), each // 2)
    stage_in = pltpu.make_async_copy(x_ref.at[stage], stage_ref, stage_sem)

    stage_in.start()
    lax.fori_loop(me + 1, n, greet, 0)

    @pl.when(me > 0)
    def _():
        pl.semaphore_wait(barrier, me)

    @pl.when(partner < me)
    def _():
        tell(ready_sems.at[me], partner)
        stage_in.wait()
        raw_staged().start()

    damp_in = pltpu.make_async_copy(damp_ref, damp_smem, near_sems.at[0])
    pick_in = pltpu.make_async_copy(pick_ref, pick_smem.at[pl.ds(0, n * each)], near_sems.at[1])
    tables_in = [
        pltpu.make_async_copy(there, here, near_sems.at[2 + i])
        for i, (there, here) in enumerate(((fwd_hbm, fwd_ref), (inv_hbm, inv_ref), (tw_hbm, tw_ref)))
    ]
    tiles_in = [
        pltpu.make_async_copy(
            wave_ref.at[pl.ds(h * SUBLANES, SUBLANES), pl.ds(p * LANES, LANES)],
            bank_ref.at[me, pl.ds((h * pieces + p) * SUBLANES, SUBLANES)],
            near_sems.at[5 + h * pieces + p],
        )
        for h in range(halves)
        for p in range(pieces)
    ]
    for copy in [damp_in] + tiles_in + [pick_in] + tables_in:
        copy.start()

    def load(e):
        return pltpu.make_async_copy(block_of(e), buf_ref.at[n + e], load_sems.at[e])

    def load_start(s, carry):
        @pl.when(jnp.logical_or(s < made, s == n - 1))
        def _():
            load(me ^ turn_of(s)).start()

        return carry

    def picks(i):
        count = n * each
        there = pick_smem.at[pl.ds((1 + i) * count, count)]
        return remote(pick_ref, there, pick_sems.at[0, i], pick_sems.at[1, i], me ^ raws[i])

    @pl.when(partner > me)
    def _():
        stage_in.wait()
        pl.semaphore_wait(ready_sems.at[partner], 1)
        raw_staged().start()

    lax.fori_loop(0, me, answer, 0)
    damp_in.wait()
    lane = lax.broadcasted_iota(jnp.int32, (SUBLANES, LANES), 1)
    levels = jnp.zeros((SUBLANES, LANES), jnp.float32)
    for f in range(own):
        levels = jnp.where(lane == f, damp_smem[f], levels)
    bank_ref[me, last * SUBLANES : (last + 1) * SUBLANES, :] = levels
    lax.fori_loop(me + 1, n, meet, 0)
    for copy in tiles_in:
        copy.wait()

    def bank_copy(block, slot, there):
        used = bank_ref.at[block, pl.ds(0, last * SUBLANES + 1)]
        return remote(used, used, bank_sends.at[slot], bank_recvs.at[block], there)

    def block_at(f):
        return f * inner + near

    middle = outer // 2
    upper = far >= middle
    gate = jnp.where(upper, middle, middle - 1)

    def across(t, act):
        there = lax.rem(far + t, outer)
        direct = jnp.logical_or((there >= middle) == upper, there == outer - 1 - gate)

        @pl.when(direct)
        def _():
            act(bank_copy(me, t - 1, block_at(there)))

    def onward(t, act):
        block = lax.rem(far + t, outer)
        for there in range(outer):
            slot = outer - 1 + (t - 1) * outer + there
            near_side = (there >= middle) == upper
            foreign = (block >= middle) != upper
            go = jnp.logical_and(jnp.logical_and(far == gate, far != there), jnp.logical_and(near_side, foreign))

            @pl.when(go)
            def _():
                act(bank_copy(block_at(block), slot, block_at(there)))

    def spread(f, act):
        for d in range(1, inner):
            slot = outer * outer - 1 + f * (inner - 1) + d - 1
            act(bank_copy(block_at(f), slot, far * inner + (near ^ d)))

    def bank_came(block):
        bank_copy(block, 0, partner).wait_recv()

    start, sent = (lambda copy: copy.start()), (lambda copy: copy.wait_send())
    for t in range(1, outer):
        across(t, start)
    spread(far, start)
    raw(0, 1, False).start()
    for i in range(1, len(raws)):
        raw(i, 0, False).start()
        raw(i, 1, False).start()
    for i in range(len(raws)):
        picks(i).start()
    lax.fori_loop(0, n, load_start, 0)
    for t in range(1, outer):
        block = lax.rem(far + t, outer)
        bank_came(block_at(block))
        onward(t, start)
        spread(block, start)
    for f in range(outer):
        for d in range(1, inner):
            bank_came(f * inner + (near ^ d))
    pick_in.wait()
    for copy in tables_in:
        copy.wait()

    def send(e):
        return remote(buf_ref.at[n + e], buf_ref.at[me], sends.at[e], recvs.at[me], e)

    row_lane = lax.broadcasted_iota(jnp.int32, (1, LANES), 1)

    def step(s, carry):
        e = me ^ turn_of(s)
        theirs = jnp.logical_and(s >= made, s < n - 1)
        for i in range(len(raws)):

            @pl.when(s == made + i)
            def _():
                raw(i, 0, True).wait_recv()
                raw(i, 1, True).wait_recv()
                picks(i).wait_recv()

        @pl.when(jnp.logical_not(theirs))
        def _():
            load(e).wait()

        table = jnp.where(theirs, s - made + 1, 0)
        base = (table * n + jnp.where(theirs, me, e)) * each
        for r in range(ROWS):
            pick = pick_smem[base + r]
            block, inside = lax.div(pick, own), lax.rem(pick, own)
            at = lax.div(inside, SUBLANES) * (pieces * SUBLANES) + lax.rem(inside, SUBLANES)
            for p in range(pieces):
                rows_ref[r : r + 1, p * LANES : (p + 1) * LANES] = bank_ref[block, pl.ds(at + p * SUBLANES, 1), :]
            level = bank_ref[block, last * SUBLANES : last * SUBLANES + 1, :]
            rows_ref[r : r + 1, taps : taps + LANES] = jnp.where(row_lane == inside, level, 0.0)

        @pl.when(jnp.logical_and(s >= 1, s <= sent_here))
        def _():
            send(me ^ turn_of(s - 1)).start()

        slot = jnp.where(s >= made, e, n + e)
        wave = [rows_ref[:, p * LANES : (p + 1) * LANES] for p in range(pieces)]
        power = sum(jnp.sum(w * w, axis=1, keepdims=True) for w in wave)
        damp = jnp.sum(rows_ref[:, taps : taps + LANES], axis=1, keepdims=True)
        floor = jnp.broadcast_to(damp * (power + 1e-6), (ROWS, LANES))

        def read(j):
            return buf_ref[n + e, :, j * LANES : (j + 1) * LANES]

        def write(j, value):
            buf_ref[slot, :, j * LANES : (j + 1) * LANES] = value

        deconvolve(read, write, wave, floor, fwd_ref, inv_ref, tw_ref, mid_ref, cut_ref, spec_ref)
        return carry

    lax.fori_loop(0, n, step, 0)

    for i in range(len(raws)):
        raw(i, 0, False).wait_send()
        raw(i, 1, False).wait_send()
        picks(i).wait_send()
    for t in range(1, outer):
        across(t, sent)
        onward(t, sent)
    for f in range(outer):
        spread(f, sent)

    def finish(s, carry):
        e = me ^ turn_of(s)
        send(e).wait_send()
        remote(buf_ref.at[e], buf_ref.at[e], sends.at[e], recvs.at[e], e).wait_recv()
        return carry

    lax.fori_loop(0, sent_here, finish, 0)


def late_kernel(n, buf_ref, after_ref, late_ref, sends, recvs):
    del after_ref
    me = lax.axis_index("traces")
    kept = block_order(n)[2]

    @pl.when(keeps_blocks(me, n))
    def _():
        barrier = pltpu.get_barrier_semaphore()
        for k in kept:
            pl.semaphore_signal(barrier, inc=1, device_id={"traces": me ^ k}, device_id_type=pl.DeviceIdType.MESH)
        pl.semaphore_wait(barrier, len(kept))
        copies = [
            pltpu.make_async_remote_copy(
                src_ref=buf_ref.at[n + (me ^ k)],
                dst_ref=late_ref.at[i],
                send_sem=sends.at[i],
                recv_sem=recvs.at[i],
                device_id={"traces": me ^ k},
                device_id_type=pl.DeviceIdType.MESH,
            )
            for i, k in enumerate(kept)
        ]
        for copy in copies:
            copy.start()
        for copy in copies:
            copy.wait()


def settle_kernel(n, order_ref, came_ref, o_ref, late_rows_ref, sem):
    rows = o_ref.shape[0]
    each = rows // n
    shift = n.bit_length() - 1
    me = lax.axis_index("traces")
    kept = block_order(n)[2]
    keeps = keeps_blocks(me, n)

    def put(d, carry):
        for r in range(each):
            q = d * each + r
            place = order_ref[q]
            source, row = place & (n - 1), place >> shift
            turn = source ^ me
            late = jnp.logical_and(keeps, functools.reduce(jnp.logical_or, [turn == k for k in kept]))

            @pl.when(late)
            def _():
                index = functools.reduce(lambda at, ik: jnp.where(turn == ik[1], ik[0], at), enumerate(kept), 0)
                late_rows_ref[index * each + row] = q

            @pl.when(jnp.logical_not(late))
            def _():
                pltpu.make_async_copy(came_ref.at[source, pl.ds(row, 1)], o_ref.at[pl.ds(q, 1)], sem).start()

        return carry

    lax.fori_loop(0, n, put, 0)

    def finish(count):
        pltpu.make_async_copy(o_ref.at[pl.ds(0, count)], o_ref.at[pl.ds(0, count)], sem).wait()

    @pl.when(keeps)
    def _():
        finish(rows - len(kept) * each)

    @pl.when(jnp.logical_not(keeps))
    def _():
        finish(rows)


def last_kernel(n, late_rows_ref, late_ref, settled_ref, o_ref, sem):
    del settled_ref
    count, each, _ = late_ref.shape

    @pl.when(keeps_blocks(lax.axis_index("traces"), n))
    def _():
        for i in range(count):
            for r in range(each):
                q = late_rows_ref[i * each + r]
                pltpu.make_async_copy(late_ref.at[i, pl.ds(r, 1)], o_ref.at[pl.ds(q, 1)], sem).start()
        part = o_ref.at[pl.ds(0, count * each)]
        pltpu.make_async_copy(part, part, sem).wait()


def tables(length, taps):
    return (
        jnp.asarray(lane_matrix(-1.0, 1.0)),
        jnp.asarray(lane_matrix(1.0, 1.0 / length)),
        jnp.asarray(twiddles(length, taps)),
    )


def scratch():
    return [
        pltpu.VMEM((RADIX * RADIX, ROWS, LANES), jnp.float32),
        pltpu.VMEM((2 * KEEP * ROWS, 6 * LANES), jnp.bfloat16),
        pltpu.VMEM((2 * KEEP * ROWS, 2 * LANES), jnp.float32),
    ]


def gathered(raw_traces, filter_index, channel_order, wavelets, damping):
    rows, length = raw_traces.shape
    own, taps = wavelets.shape
    n = lax.axis_size("traces")
    me = lax.axis_index("traces")
    each = rows // n
    floor = damping * (jnp.sum(wavelets * wavelets, axis=1) + 1e-6)
    picks = filter_index.reshape(own, rows // own).astype(jnp.float32)
    packed = lax.all_gather(jnp.concatenate([wavelets, floor[:, None], picks], axis=1), "traces", axis=0, tiled=True)
    all_picks = packed[:, taps + 1 :].reshape(n, n, each).astype(jnp.int32)
    came_picks = lax.dynamic_index_in_dim(all_picks, me, 1, keepdims=False)
    bank = jnp.concatenate([packed[:, :taps], jnp.broadcast_to(packed[:, taps : taps + 1], (own * n, LANES))], axis=1)
    fwd, inv, tw = tables(length, taps)
    whole = lambda a: pl.BlockSpec(a.shape, lambda i, *_: (0,) * a.ndim)
    fixed = [pl.BlockSpec((ROWS, taps + LANES), lambda i, *_: (i, 0)), whole(fwd), whole(inv), whole(tw)]
    came = lax.all_to_all(raw_traces.reshape(n, each, length), "traces", 0, 0, tiled=True).reshape(rows, length)
    result = pl.pallas_call(
        functools.partial(block_kernel, taps, ()),
        grid=(rows // ROWS,),
        out_shape=jax.ShapeDtypeStruct((rows, length), jnp.float32),
        in_specs=[pl.BlockSpec((ROWS, length), lambda i: (i, 0))] + fixed,
        out_specs=pl.BlockSpec((ROWS, length), lambda i: (i, 0)),
        scratch_shapes=scratch(),
        compiler_params=pltpu.CompilerParams(vmem_limit_bytes=48 * 1024 * 1024),
    )(came, jnp.take(bank, came_picks.reshape(-1), axis=0), fwd, inv, tw)
    return jnp.take(result, (channel_order % n) * each + channel_order // n, axis=0)


def local(raw_traces, filter_index, channel_order, wavelets, damping):
    rows, length = raw_traces.shape
    own, taps = wavelets.shape
    n = lax.axis_size("traces")
    if n < 4 or n & (n - 1) or rows != n * ROWS or own % SUBLANES or own > LANES or taps % LANES:
        return gathered(raw_traces, filter_index, channel_order, wavelets, damping)

    fwd, inv, tw = tables(length, taps)
    tiles = own // SUBLANES * (taps // LANES)
    outer = split_count(n)[0]
    _, raws, kept = block_order(n)
    raws, kept = len(raws), len(kept)
    dma = pltpu.SemaphoreType.DMA
    came = pl.pallas_call(
        functools.partial(exchange_kernel, n, taps),
        in_specs=[pl.BlockSpec(memory_space=pltpu.HBM)] * 7,
        out_specs=pl.BlockSpec(memory_space=pltpu.VMEM),
        out_shape=pltpu.VMEM((2 * n, ROWS, length), jnp.float32),
        scratch_shapes=scratch()
        + [pltpu.VMEM(a.shape, a.dtype) for a in (fwd, inv, tw)]
        + [
            pltpu.VMEM((n, (tiles + 1) * SUBLANES, LANES), jnp.float32),
            pltpu.VMEM((ROWS, taps + LANES), jnp.float32),
            pltpu.VMEM((ROWS // 2, length), jnp.float32),
            pltpu.SMEM(((1 + raws) * rows,), jnp.int32),
            pltpu.SMEM((own,), jnp.float32),
            dma,
            dma((n,)),
            dma((5 + tiles,)),
            dma((2, raws, 2)),
            dma((2, raws)),
            dma((outer * outer - 1 + n - outer,)),
            dma((n,)),
            pltpu.SemaphoreType.REGULAR((n,)),
            dma((n,)),
            dma((n,)),
        ],
        compiler_params=pltpu.CompilerParams(
            collective_id=0, has_side_effects=True, vmem_limit_bytes=40 * 1024 * 1024
        ),
        cost_estimate=pl.CostEstimate(flops=rows * length * 1500, bytes_accessed=8 * rows * length, transcendentals=0),
    )(raw_traces, filter_index, wavelets, damping, fwd, inv, tw)
    came = pltpu.with_memory_space_constraint(came, pltpu.VMEM)
    smem, vmem, hbm = (pl.BlockSpec(memory_space=m) for m in (pltpu.SMEM, pltpu.VMEM, pltpu.HBM))
    params = pltpu.CompilerParams(vmem_limit_bytes=20 * 1024 * 1024)
    settled, late_rows = pl.pallas_call(
        functools.partial(settle_kernel, n),
        in_specs=[smem, vmem],
        out_specs=[hbm, smem],
        out_shape=[
            jax.ShapeDtypeStruct((rows, length), jnp.float32),
            pltpu.SMEM((kept * ROWS,), jnp.int32),
        ],
        scratch_shapes=[dma],
        compiler_params=params,
    )(channel_order, came)
    late_rows = pltpu.with_memory_space_constraint(late_rows, pltpu.SMEM)
    late = pl.pallas_call(
        functools.partial(late_kernel, n),
        in_specs=[vmem, smem],
        out_specs=vmem,
        out_shape=pltpu.VMEM((kept, ROWS, length), jnp.float32),
        scratch_shapes=[dma((kept,)), dma((kept,))],
        compiler_params=pltpu.CompilerParams(
            collective_id=1, has_side_effects=True, vmem_limit_bytes=20 * 1024 * 1024
        ),
    )(came, late_rows)
    late = pltpu.with_memory_space_constraint(late, pltpu.VMEM)
    return pl.pallas_call(
        functools.partial(last_kernel, n),
        in_specs=[smem, vmem, hbm],
        out_specs=hbm,
        out_shape=jax.ShapeDtypeStruct((rows, length), jnp.float32),
        scratch_shapes=[dma],
        input_output_aliases={2: 0},
        compiler_params=params,
    )(late_rows, late, settled)


def solution(mesh):
    placed = (
        P(("groups", "traces"), None),
        P(("groups", "traces")),
        P("groups"),
        P("traces", None),
        P("traces"),
    )
    return jax.shard_map(
        local, mesh=mesh, in_specs=placed, out_specs=P(("groups", "traces"), None), check_vma=False
    )
```
